8 devices in a mesh: rep: 1 (over z), dp: 8 (over x, y, core).
Axes of the slice: x: 2, y: 2, z: 1, core: 2. Of those that a mesh axis runs over, the one named last changes fastest.
Arguments:
- x: bfloat16 [8, 2048, 640], P(('rep', 'dp'))
- dy: bfloat16 [8, 2048, 640], P(('rep', 'dp'))
- wq: bfloat16 [2, 640, 512], P(None, 'dp')
- wk: bfloat16 [2, 640, 256], P(None, 'dp')
- wv: bfloat16 [2, 640, 256], P(None, 'dp')
- wo: bfloat16 [2, 512, 640], P(None, 'dp')
- w_gate: bfloat16 [2, 640, 2560], P(None, 'dp')
- w_up: bfloat16 [2, 640, 2560], P(None, 'dp')
- w_down: bfloat16 [2, 2560, 640], P(None, 'dp')
- m_wq: float32 [2, 640, 512], P(None, 'dp')
- m_wk: float32 [2, 640, 256], P(None, 'dp')
- m_wv: float32 [2, 640, 256], P(None, 'dp')
- m_wo: float32 [2, 512, 640], P(None, 'dp')
- m_w_gate: float32 [2, 640, 2560], P(None, 'dp')
- m_w_up: float32 [2, 640, 2560], P(None, 'dp')
- m_w_down: float32 [2, 2560, 640], P(None, 'dp')
- v_wq: float32 [2, 640, 512], P(None, 'dp')
- v_wk: float32 [2, 640, 256], P(None, 'dp')
- v_wv: float32 [2, 640, 256], P(None, 'dp')
- v_wo: float32 [2, 512, 640], P(None, 'dp')
- v_w_gate: float32 [2, 640, 2560], P(None, 'dp')
- v_w_up: float32 [2, 640, 2560], P(None, 'dp')
- v_w_down: float32 [2, 2560, 640], P(None, 'dp')
Outputs:
- output 1: bfloat16 [2, 640, 512], P('rep', 'dp')
- output 2: bfloat16 [2, 640, 256], P('rep', 'dp')
- output 3: bfloat16 [2, 640, 256], P('rep', 'dp')
- output 4: bfloat16 [2, 512, 640], P('rep', 'dp')
- output 5: bfloat16 [2, 640, 2560], P('rep', 'dp')
- output 6: bfloat16 [2, 640, 2560], P('rep', 'dp')
- output 7: bfloat16 [2, 2560, 640], P('rep', 'dp')
- output 8: float32 [2, 640, 512], P('rep', 'dp')
- output 9: float32 [2, 640, 256], P('rep', 'dp')
- output 10: float32 [2, 640, 256], P('rep', 'dp')
- output 11: float32 [2, 512, 640], P('rep', 'dp')
- output 12: float32 [2, 640, 2560], P('rep', 'dp')
- output 13: float32 [2, 640, 2560], P('rep', 'dp')
- output 14: float32 [2, 2560, 640], P('rep', 'dp')
- output 15: float32 [2, 640, 512], P('rep', 'dp')
- output 16: float32 [2, 640, 256], P('rep', 'dp')
- output 17: float32 [2, 640, 256], P('rep', 'dp')
- output 18: float32 [2, 512, 640], P('rep', 'dp')
- output 19: float32 [2, 640, 2560], P('rep', 'dp')
- output 20: float32 [2, 640, 2560], P('rep', 'dp')
- output 21: float32 [2, 2560, 640], P('rep', 'dp')
All inputs are finite; a program needn't handle non-finite values.
Results may differ from the reference program's by a relative error of at most 0.024.
Values are sent between devices in bfloat16 or wider.
A program may use at most 2 GiB of HBM per device.

```python
import jax
import jax.numpy as jnp
from jax import lax

SEQUENCES = 8
TOKENS = 2048
D = 640
HEADS = 2
KV_HEADS = 1
HEAD = 256
FF = 2560
LAYERS = 2
THETA = 10000
NAMES = ("wq", "wk", "wv", "wo", "w_gate", "w_up", "w_down")
SHAPES = {
    "wq": (LAYERS, D, HEADS * HEAD),
    "wk": (LAYERS, D, KV_HEADS * HEAD),
    "wv": (LAYERS, D, KV_HEADS * HEAD),
    "wo": (LAYERS, HEADS * HEAD, D),
    "w_gate": (LAYERS, D, FF),
    "w_up": (LAYERS, D, FF),
    "w_down": (LAYERS, FF, D),
}


def bump(key, n, height):
    away = (jnp.arange(n, dtype=jnp.int32) - jax.random.randint(key, (), 0, n, jnp.int32)) % n
    return jnp.where(away < n // 8, height, 1.0)


def together(key, own, strength):
    shared = jax.random.normal(key, own.shape[1:], jnp.float32)
    return (own + strength * shared) * lax.rsqrt(1 + strength * strength)


def setup_inputs(seed: int = 0, part: int = 0) -> dict:
    kx, kdy, ka, kb, kz, kf, kh, kl, *keys = jax.random.split(jax.random.key(seed), 8 + 3 * len(NAMES))
    kx, kdy, ka, kb = (jax.random.fold_in(k, part) for k in (kx, kdy, ka, kb))
    kw, km, kv = (keys[i::3] for i in range(3))
    shape = (SEQUENCES, TOKENS, D)
    much_x, much_dy = jax.random.uniform(kz, (2,), jnp.float32, 0.0, 1.0)
    loud = 2.0 ** jax.random.uniform(jax.random.fold_in(kz, 1), (), jnp.float32, -1.0, 2.0)
    layers = 2.0 ** jax.random.uniform(kl, (LAYERS, 1, 1), jnp.float32, -1.0, 1.0)
    times = {"wq": 1.0, "wk": 1.0, "wv": 2.0, "wo": layers, "w_gate": 1.0, "w_up": bump(kh, FF, 4.0), "w_down": layers}
    x = together(ka, jax.random.normal(kx, shape, jnp.float32), much_x) * bump(kf, D, 4.0)
    dy = together(kb, jax.random.normal(kdy, shape, jnp.float32), much_dy)
    drawn = {"x": x.astype(jnp.bfloat16), "dy": (loud * dy * (SEQUENCES * TOKENS) ** -0.5).astype(jnp.bfloat16)}
    for key, name in zip(kw, NAMES, strict=True):
        drawn[name] = (jax.random.normal(key, SHAPES[name], jnp.float32) * SHAPES[name][1] ** -0.5 * times[name]).astype(jnp.bfloat16)
    for key, name in zip(km, NAMES, strict=True):
        drawn[f"m_{name}"] = 0.1 * jax.random.normal(key, SHAPES[name], jnp.float32)
    for key, name in zip(kv, NAMES, strict=True):
        drawn[f"v_{name}"] = jax.random.uniform(key, SHAPES[name], jnp.float32, 0.02, 0.06)
    return drawn


def matmul(a, w):
    return jnp.dot(a, w, preferred_element_type=jnp.float32).astype(jnp.bfloat16)


def normed(h):
    wide = h.astype(jnp.float32)
    scale = lax.rsqrt(jnp.mean(wide**2, -1, keepdims=True) + 1e-6)
    return (wide * scale).astype(jnp.bfloat16)


def turned(t, theta):
    half = t.shape[-1] // 2
    angle = jnp.arange(t.shape[0], dtype=jnp.float32)[:, None] * theta ** (-jnp.arange(half, dtype=jnp.float32) / half)
    cos, sin = jnp.cos(angle)[:, None], jnp.sin(angle)[:, None]
    a, b = t[..., :half].astype(jnp.float32), t[..., half:].astype(jnp.float32)
    return jnp.concatenate([a * cos - b * sin, b * cos + a * sin], -1).astype(jnp.bfloat16)


def seen_by(q, k, v):
    tokens, kv = q.shape[0], k.shape[1]
    q = q.reshape(tokens, kv, -1, q.shape[-1])
    scores = jnp.einsum("tgsd,ugd->gstu", q.astype(jnp.float32), k.astype(jnp.float32)) * q.shape[-1] ** -0.5
    place = jnp.arange(tokens)
    weights = jax.nn.softmax(jnp.where(place[:, None] >= place, scores, -jnp.inf), -1).astype(jnp.bfloat16)
    return jnp.einsum("gstu,ugd->tgsd", weights.astype(jnp.float32), v.astype(jnp.float32)).astype(jnp.bfloat16).reshape(tokens, -1)


def layer(h, w):
    a = normed(h)
    q, k = (turned(matmul(a, w[name]).reshape(h.shape[0], -1, HEAD), THETA) for name in ("wq", "wk"))
    h = h + matmul(seen_by(q, k, matmul(a, w["wv"]).reshape(h.shape[0], -1, HEAD)), w["wo"])
    b = normed(h)
    gate = jnp.dot(b, w["w_gate"], preferred_element_type=jnp.float32)
    up = jnp.dot(b, w["w_up"], preferred_element_type=jnp.float32)
    return h + matmul((jax.nn.silu(gate) * up).astype(jnp.bfloat16), w["w_down"])


def adamw(w, m, v, g):
    m = 0.9 * m + 0.1 * g
    v = 0.95 * v + 0.05 * g * g
    step = m * lax.rsqrt(v + 1e-8) + 0.1 * w
    return (w - 0.02 * step).astype(jnp.bfloat16), m, v


def clipped(gradients, sum_of_squares, count):
    factor = jnp.minimum(1.0, 0.5 * lax.rsqrt(sum_of_squares / count + 1e-30))
    return [g * factor for g in gradients]


def stack(weights, h):
    return lax.scan(lambda h, w: (layer(h, w), None), h, weights)[0]


def reference(x, dy, wq, wk, wv, wo, w_gate, w_up, w_down, m_wq, m_wk, m_wv, m_wo, m_w_gate, m_w_up, m_w_down, v_wq, v_wk, v_wv, v_wo, v_w_gate, v_w_up, v_w_down):
    weights = dict(zip(NAMES, (wq, wk, wv, wo, w_gate, w_up, w_down), strict=True))

    def take(so_far, sequence):
        h, by_y = sequence
        _, back = jax.vjp(stack, weights, h)
        by_weights, by_h = back(by_y)
        return jax.tree.map(lambda total, term: total + term.astype(jnp.float32), so_far, by_weights), by_h

    none_yet = {name: jnp.zeros(w.shape, jnp.float32) for name, w in weights.items()}
    by_weights, by_x = lax.scan(take, none_yet, (x, dy))
    gradients = [by_weights[name].astype(jnp.bfloat16).astype(jnp.float32) for name in NAMES]
    gradients = clipped(gradients, sum(jnp.sum(g * g) for g in gradients), sum(g.size for g in gradients))
    first = (m_wq, m_wk, m_wv, m_wo, m_w_gate, m_w_up, m_w_down)
    second = (v_wq, v_wk, v_wv, v_wo, v_w_gate, v_w_up, v_w_down)
    new = [adamw(weights[name].astype(jnp.float32), m, v, g) for name, m, v, g in zip(NAMES, first, second, gradients, strict=True)]
    return tuple(one[which] for which in range(3) for one in new)
```

```python
import functools

import jax
import jax.numpy as jnp
from jax import lax
from jax.experimental import pallas as pl
from jax.experimental.pallas import tpu as pltpu
from jax.sharding import PartitionSpec as P

HEAD = 256
THETA = 10000
NAMES = ("wq", "wk", "wv", "wo", "w_gate", "w_up", "w_down")
ATT, MLP = NAMES[:4], NAMES[4:]
NEG = -1e30
HIDDEN = 2 * NEG
LOG2E = 1.4426950408889634
VMEM = 62 * 2**20
BLOCK = 512
CHUNK = 512
ROWS = 512
ANY = pl.BlockSpec(memory_space=pl.ANY)
MESH = pl.DeviceIdType.MESH
F32, BF16 = jnp.float32, jnp.bfloat16


def _dot(a, b, ca, cb):
    return lax.dot_general(a, b, (((ca,), (cb,)), ((), ())), preferred_element_type=F32)


def _units(names, blocks):
    cut = []
    for name in names:
        rows, columns = blocks[name]
        if name in ("wo", "w_down"):
            cut += [(name, 0, rows // 2, 0), (name, rows // 2, rows // 2, 1)]
        else:
            cut += [(name, 0, rows, 0 if name in ("wq", "w_gate") else 1)]
    return cut


def _around(way):
    me = lax.axis_index("dp")
    core, y, x = lax.rem(me, 2), lax.rem(lax.div(me, 2), 2), lax.div(me, 4)
    over_x, over_y = 4 - 8 * x, 2 - 4 * y
    first, second = (over_x, over_y) if way == 0 else (over_y, over_x)
    return me, 1 - 2 * core, first, second, over_x + over_y


def _meet():
    me, other, first, second, _ = _around(0)
    barrier = pltpu.get_barrier_semaphore()
    for way in (other, first, second):
        pl.semaphore_signal(barrier, inc=1, device_id={"dp": me + way}, device_id_type=MESH)
    pl.semaphore_wait(barrier, 3)


class Gather:
    def __init__(self, names, blocks, layer):
        self.names, self.blocks, self.layer = names, blocks, layer
        self.units = _units(names, blocks)

    def in_specs(self):
        return [ANY] * len(self.names)

    def out_specs(self):
        return [ANY] * len(self.names)

    def out_shape(self):
        return [jax.ShapeDtypeStruct((8 * self.blocks[n][0], self.blocks[n][1]), BF16) for n in self.names]

    def scratch(self):
        n = len(self.units)
        return [pltpu.SemaphoreType.DMA((n,)), pltpu.SemaphoreType.DMA((n, 7)), pltpu.SemaphoreType.DMA((n, 7))]

    def bind(self, ins, outs, scratch):
        self.shards, self.whole = dict(zip(self.names, ins)), dict(zip(self.names, outs))
        self.local, self.send, self.recv = scratch

    def _piece(self, unit, device):
        name, at, rows, _ = unit
        return self.whole[name].at[pl.ds(pl.multiple_of(device * self.blocks[name][0] + at, 16), rows)]

    def _copy(self, i, slot, arrived=False):
        unit = self.units[i]
        name, at, rows, way = unit
        me, other, first, second, across = _around(way)
        own = self.shards[name].at[self.layer, pl.ds(at, rows)]
        source, owner, to, comes = (
            (own, me, first, me + first),
            (own, me, second, me + second),
            (own, me, other, me + other),
            (None, me + first, second, me + across),
            (None, me + first, other, me + first + other),
            (None, me + second, other, me + second + other),
            (None, me + across, other, me + across + other),
        )[slot]
        if arrived:
            source, owner = None, comes
        target = self._piece(unit, owner)
        return pltpu.make_async_remote_copy(target if source is None else source, target, self.send.at[i, slot], self.recv.at[i, slot],
                                            device_id={"dp": me + to}, device_id_type=MESH)

    def _mine(self, i):
        name, at, rows, way = self.units[i]
        return pltpu.make_async_copy(self.shards[name].at[self.layer, pl.ds(at, rows)], self._piece(self.units[i], lax.axis_index("dp")), self.local.at[i])

    def begin(self):
        for i in range(len(self.units)):
            for slot in range(3):
                self._copy(i, slot).start()
            self._mine(i).start()

    def middle(self):
        for i in range(len(self.units)):
            self._copy(i, 0, True).wait_recv()
            self._copy(i, 3).start()
            self._copy(i, 4).start()
            self._copy(i, 1, True).wait_recv()
            self._copy(i, 5).start()

    def end(self):
        for i in range(len(self.units)):
            self._copy(i, 3, True).wait_recv()
            self._copy(i, 6).start()
        for i in range(len(self.units)):
            for slot in (2, 4, 5, 6):
                self._copy(i, slot, True).wait_recv()
            for slot in range(7):
                self._copy(i, slot).wait_send()
            self._mine(i).wait()

    def actions(self, steps):
        if steps == 1:
            return {0: ([_meet, self.begin, self.middle, self.end], [])}
        return {0: ([_meet, self.begin], []), steps - 1: ([self.middle], [self.end])}


class Scatter:
    def __init__(self, names, blocks):
        self.names, self.blocks = names, blocks
        self.units = _units(names, blocks)

    def in_specs(self):
        return [ANY] * len(self.names)

    def out_specs(self):
        return [pl.BlockSpec(self.blocks[n], lambda *_: (0, 0)) for n in self.names]

    def out_shape(self):
        return [jax.ShapeDtypeStruct(self.blocks[n], BF16) for n in self.names]

    def scratch(self):
        n, dma = len(self.units), pltpu.SemaphoreType.DMA
        found = [dma((n, 4)), dma((n, 4)), dma((n, 4)), dma((n, 2)), dma((n, 2)), dma((n,)), dma((n,))]
        for name, _, rows, _ in self.units:
            columns = self.blocks[name][1]
            found += [pltpu.VMEM((k, rows, columns), BF16) for k in (4, 4, 2, 2, 1, 1)]
        return found

    def bind(self, ins, outs, scratch):
        self.terms, self.outs = dict(zip(self.names, ins)), dict(zip(self.names, outs))
        self.load, self.send0, self.recv0, self.send1, self.recv1, self.send2, self.recv2 = scratch[:7]
        rest = scratch[7:]
        self.buffers = [rest[6 * i : 6 * i + 6] for i in range(len(self.units))]

    def _block(self, unit, device):
        name, at, rows, _ = unit
        return self.terms[name].at[pl.ds(pl.multiple_of(device * self.blocks[name][0] + at, 16), rows)]

    def _own(self, i, j):
        me, other, *ways = _around(self.units[i][3])
        return pltpu.make_async_copy(self._block(self.units[i], me + ([0] + ways)[j]), self.buffers[i][0].at[j], self.load.at[i, j])

    def _across(self, i, j):
        me, other, *ways = _around(self.units[i][3])
        return pltpu.make_async_remote_copy(self._block(self.units[i], me + other + ([0] + ways)[j]), self.buffers[i][1].at[j], self.send0.at[i, j],
                                            self.recv0.at[i, j], device_id={"dp": me + other}, device_id_type=MESH)

    def _first(self, i, j):
        me, _, first, _, _ = _around(self.units[i][3])
        return pltpu.make_async_remote_copy(self.buffers[i][2].at[j], self.buffers[i][3].at[j], self.send1.at[i, j], self.recv1.at[i, j],
                                            device_id={"dp": me + first}, device_id_type=MESH)

    def _second(self, i):
        me, _, _, second, _ = _around(self.units[i][3])
        return pltpu.make_async_remote_copy(self.buffers[i][4].at[0], self.buffers[i][5].at[0], self.send2.at[i], self.recv2.at[i],
                                            device_id={"dp": me + second}, device_id_type=MESH)

    def begin(self):
        for js in ((1, 3), (2, 0)):
            for i in range(len(self.units)):
                for j in js:
                    self._across(i, j).start()
                    self._own(i, j).start()

    def _ready(self, i, j):
        self._own(i, j).wait()
        self._across(i, j).wait_recv()

    def _add(self, rows, store, *terms):
        def some(t, _):
            at = pl.ds(pl.multiple_of(t * 16, 16), 16)
            store(at, sum(term[at, :].astype(F32) for term in terms))
            return 0

        lax.fori_loop(0, rows // 16, some, 0)

    def part1(self):
        for i, (_, _, rows, _) in enumerate(self.units):
            own, came, out = self.buffers[i][:3]
            for j, k in ((1, 0), (3, 1)):
                self._ready(i, j)

                def store(at, value, k=k, out=out):
                    out[k, at, :] = value.astype(BF16)

                self._add(rows, store, own.at[j], came.at[j])
            if i:
                self._first(i - 1, 0).start()
                self._first(i - 1, 1).start()

    def part2(self):
        for j in range(2):
            self._first(len(self.units) - 1, j).start()

    def part3(self):
        for i, (_, _, rows, _) in enumerate(self.units):
            own, came, _, got, out, _ = self.buffers[i]
            self._ready(i, 2)
            self._first(i, 0).wait_recv()
            self._first(i, 1).wait_recv()

            def store(at, value, out=out):
                out[0, at, :] = value.astype(BF16)

            self._add(rows, store, own.at[2], came.at[2], got.at[1])
            if i:
                self._second(i - 1).start()

    def part4(self):
        self._second(len(self.units) - 1).start()

    def end(self):
        for i, (name, start, rows, _) in enumerate(self.units):
            own, came, _, got, _, last = self.buffers[i]
            self._ready(i, 0)
            self._second(i).wait_recv()

            def store(at, value, name=name, start=start):
                self.outs[name][pl.ds(pl.multiple_of(start + at.start, 16), 16), :] = value.astype(BF16)

            self._add(rows, store, own.at[0], came.at[0], got.at[0], last.at[0])
        for i in range(len(self.units)):
            for j in range(4):
                self._across(i, j).wait_send()
            for j in range(2):
                self._first(i, j).wait_send()
            self._second(i).wait_send()

    def actions(self, steps):
        if steps == 1:
            return {0: ([_meet, self.begin, self.part1, self.part2, self.part3, self.part4, self.end], [])}
        if steps == 4:
            return {0: ([_meet, self.begin], []), 1: ([self.part1], []), 2: ([self.part2], []), 3: ([self.part3], [self.part4, self.end])}
        return {0: ([_meet, self.begin], []), 1: ([self.part1], [self.part2]), steps - 2: ([self.part3], [self.part4]), steps - 1: ([], [self.end])}


def _call(body, steps, ins, in_specs, outs, out_specs, scratch, rider=None, given=(), number=0, flops=0, name=None):
    ni, no, ns = len(in_specs), len(out_specs), len(scratch)
    more_in, more_out, more_specs, more_scratch = ([], [], [], []) if rider is None else (rider.in_specs(), rider.out_shape(), rider.out_specs(), rider.scratch())

    def kernel(*refs):
        cuts = [ni, len(more_in), no, len(more_out), ns, len(more_scratch)]
        parts, at = [], 0
        for n in cuts:
            parts.append(refs[at : at + n])
            at += n
        step = pl.program_id(0)
        acts = {}
        if rider is not None:
            rider.bind(parts[1], parts[3], parts[5])
            acts = rider.actions(steps)

        def run(which):
            for s, lists in acts.items():
                if lists[which]:
                    if steps == 1:
                        for act in lists[which]:
                            act()
                    else:

                        @pl.when(step == s)
                        def _(todo=lists[which]):
                            for act in todo:
                                act()

        run(0)
        body(step, parts[0], parts[2], parts[4])
        run(1)

    params = dict(dimension_semantics=("arbitrary",), vmem_limit_bytes=VMEM)
    if rider is not None:
        params |= dict(collective_id=number, has_side_effects=True)
    got = pl.pallas_call(
        kernel,
        grid=(steps,),
        in_specs=[*in_specs, *more_in],
        out_specs=[*out_specs, *more_specs],
        out_shape=[*outs, *more_out],
        scratch_shapes=[*scratch, *more_scratch],
        compiler_params=pltpu.CompilerParams(**params),
        cost_estimate=pl.CostEstimate(flops=int(flops) + 1, bytes_accessed=10**6, transcendentals=0),
        name=name,
    )(*ins, *given)
    return list(got[:no]), list(got[no:])


def _whole(a):
    return pl.BlockSpec(a.shape, lambda *_: (0,) * len(a.shape))


def _shape(shape, dtype=BF16):
    return jax.ShapeDtypeStruct(shape, dtype)


def alone(rider, given, number):
    return _call(lambda *_: None, 1, [], [], [], [], [], rider, given, number, name="exchange")[1]


def _hidden():
    return lax.broadcasted_iota(jnp.int32, (BLOCK, BLOCK), 0) > lax.broadcasted_iota(jnp.int32, (BLOCK, BLOCK), 1)


def _strip(ref, head, a):
    return ref[a * BLOCK : (a + 1) * BLOCK, head * HEAD : (head + 1) * HEAD]


def attend(q, k, v, rider=None, given=(), number=0):
    tokens, heads = q.shape[0], q.shape[1] // HEAD
    blocks, scale = tokens // BLOCK, HEAD**-0.5
    e = scale * LOG2E

    def body(step, ins, outs, scratch):
        q_ref, k_ref, v_ref = ins
        o_ref, lse_ref = outs
        top_s, mix_s = scratch

        def block(j):
            strips = [(n, a) for a in range(j, blocks) for n in range(heads)]
            keys = k_ref[j * BLOCK : (j + 1) * BLOCK, :]
            values = jnp.concatenate([v_ref[j * BLOCK : (j + 1) * BLOCK, :].T, jnp.ones((8, BLOCK), BF16)], axis=0)
            scores = [_dot(keys, _strip(q_ref, n, a), 1, 1) for n, a in strips]
            weights, keeps = [], []
            for (n, a), s in zip(strips, scores):
                i = a * heads + n
                if a == j:
                    s = jnp.where(_hidden(), HIDDEN, s)
                top = s.max(axis=0, keepdims=True)
                if j:
                    old = top_s[i : i + 1, :]
                    top = jnp.maximum(old, top)
                    keeps.append(jnp.exp2((old - top) * e))
                else:
                    keeps.append(None)
                top_s[i : i + 1, :] = top
                weights.append(jnp.exp2((s - top) * e).astype(BF16))
            for (n, a), p, keep in zip(strips, weights, keeps):
                i = a * heads + n
                mix = _dot(values, p, 1, 0)
                if j:
                    mix = mix_s[i] * keep + mix
                if a > j:
                    mix_s[i] = mix
                else:
                    total = mix[HEAD : HEAD + 1, :]
                    o_ref[a * BLOCK : (a + 1) * BLOCK, n * HEAD : (n + 1) * HEAD] = (mix[:HEAD, :] * (1 / total)).T.astype(BF16)
                    lse_ref[i : i + 1, :] = top_s[i : i + 1, :] * scale + jnp.log(total)

        for j in range(blocks):
            pl.when(step == j)(functools.partial(block, j))

    n = heads * blocks
    ins, outs = [q, k, v], [_shape(q.shape), _shape((n, BLOCK), F32)]
    return _call(body, blocks, ins, [_whole(a) for a in ins], outs, [_whole(a) for a in outs],
                 [pltpu.VMEM((n, BLOCK), F32), pltpu.VMEM((n, HEAD + 8, BLOCK), F32)], rider, given, number, 4 * 0.6 * tokens * tokens * heads * HEAD, "attend")


def attend_bwd(q, k, v, d_out, lse, delta, rider=None, given=(), number=0):
    tokens, heads = q.shape[0], q.shape[1] // HEAD
    blocks, scale = tokens // BLOCK, HEAD**-0.5
    e = scale * LOG2E

    def body(step, ins, outs, scratch):
        q_ref, k_ref, v_ref, do_ref, lse_ref, delta_ref = ins
        dq_ref, dk_ref, dv_ref = outs
        (dq_s,) = scratch

        def block(j):
            here = slice(j * BLOCK, (j + 1) * BLOCK)
            strips = [(n, a) for a in range(j, blocks) for n in range(heads)]
            keys, values = k_ref[here, :], v_ref[here, :]
            turned_keys = keys.T
            dk = dv = None
            scores = [_dot(keys, _strip(q_ref, n, a), 1, 1) for n, a in strips]
            dps = [_dot(values, _strip(do_ref, n, a), 1, 1) for n, a in strips]
            for (n, a), s, dp in zip(strips, scores, dps):
                i = a * heads + n
                p = jnp.exp2(s * e - lse_ref[i : i + 1, :] * LOG2E)
                if a == j:
                    p = jnp.where(_hidden(), 0.0, p)
                ds = (p * (dp - delta_ref[i : i + 1, :])).astype(BF16)
                by_v = _dot(p.astype(BF16), _strip(do_ref, n, a), 1, 0)
                by_k = _dot(ds, _strip(q_ref, n, a), 1, 0)
                dv, dk = (by_v, by_k) if dv is None else (dv + by_v, dk + by_k)
                by_q = _dot(turned_keys, ds, 1, 0)
                if j:
                    by_q = dq_s[i] + by_q
                if a > j:
                    dq_s[i] = by_q
                else:
                    dq_ref[a * BLOCK : (a + 1) * BLOCK, n * HEAD : (n + 1) * HEAD] = (by_q * scale).T.astype(BF16)
            dk_ref[here, :] = (dk * scale).astype(BF16)
            dv_ref[here, :] = dv.astype(BF16)

        for j in range(blocks):
            pl.when(step == j)(functools.partial(block, j))

    ins, outs = [q, k, v, d_out, lse, delta], [_shape(q.shape), _shape(k.shape), _shape(v.shape)]
    return _call(body, blocks, ins, [_whole(a) for a in ins], outs, [_whole(a) for a in outs],
                 [pltpu.VMEM((heads * blocks, HEAD, BLOCK), F32)], rider, given, number, 10 * 0.6 * tokens * tokens * heads * HEAD, "attend_bwd")


def _scale(wide):
    return lax.rsqrt(jnp.mean(wide * wide, -1, keepdims=True) + 1e-6)


def _tokens(n, do):
    def some(t, _):
        do(pl.ds(pl.multiple_of(t * ROWS, ROWS), ROWS))
        return 0

    lax.fori_loop(0, n // ROWS, some, 0)


def _chunks(w_gate, w_down):
    across = pl.BlockSpec((w_gate.shape[0], CHUNK), lambda j: (0, j))
    down = pl.BlockSpec((CHUNK, w_down.shape[1]), lambda j: (j, 0))
    return across, down


def gated(h, w_gate, w_up, w_down, rider=None, given=(), number=0):
    tokens, d = h.shape
    steps = w_gate.shape[1] // CHUNK
    across, down = _chunks(w_gate, w_down)

    def body(step, ins, outs, scratch):
        h_ref, g_ref, u_ref, d_ref = ins
        (o_ref,) = outs
        b_s, sum_s = scratch

        @pl.when(step == 0)
        def _():
            def norm(at):
                wide = h_ref[at, :].astype(F32)
                b_s[at, :] = (wide * _scale(wide)).astype(BF16)
                sum_s[at, :] = jnp.zeros((ROWS, d), F32)

            _tokens(tokens, norm)

        def some(at):
            b = b_s[at, :]
            gate, up = _dot(b, g_ref[...], 1, 0), _dot(b, u_ref[...], 1, 0)
            act = (gate * (1 / (1 + jnp.exp(-gate))) * up).astype(BF16)
            sum_s[at, :] += _dot(act, d_ref[...], 1, 0)

        _tokens(tokens, some)

        @pl.when(step == steps - 1)
        def _():
            def last(at):
                o_ref[at, :] = (h_ref[at, :].astype(F32) + sum_s[at, :].astype(BF16).astype(F32)).astype(BF16)

            _tokens(tokens, last)

    return _call(body, steps, [h, w_gate, w_up, w_down], [_whole(h), across, across, down], [_shape(h.shape)], [_whole(h)],
                 [pltpu.VMEM((tokens, d), BF16), pltpu.VMEM((tokens, d), F32)], rider, given, number, 6 * tokens * d * w_gate.shape[1], "gated")


def gated_bwd(h, by_out, w_gate, w_up, w_down, rider=None, given=(), number=0):
    tokens, d = h.shape
    steps = w_gate.shape[1] // CHUNK
    across, down = _chunks(w_gate, w_down)

    def body(step, ins, outs, scratch):
        h_ref, by_ref, g_ref, u_ref, d_ref = ins
        dh_ref, dg_ref, du_ref, dd_ref = outs
        b_s, bt_s, byt_s, sum_s, act_s, gate_s, up_s = scratch

        @pl.when(step == 0)
        def _():
            def norm(at):
                wide = h_ref[at, :].astype(F32)
                b = (wide * _scale(wide)).astype(BF16)
                b_s[at, :] = b
                bt_s[:, at] = b.T
                byt_s[:, at] = by_ref[at, :].T
                sum_s[at, :] = jnp.zeros((ROWS, d), F32)

            _tokens(tokens, norm)

        def some(at):
            b, by = b_s[at, :], by_ref[at, :]
            gate, up = _dot(b, g_ref[...], 1, 0), _dot(b, u_ref[...], 1, 0)
            by_act = _dot(by, d_ref[...], 1, 1).astype(BF16).astype(F32)
            open_ = 1 / (1 + jnp.exp(-gate))
            silu = gate * open_
            act_s[at, :] = (silu * up).astype(BF16)
            by_up = (by_act * silu).astype(BF16)
            by_gate = (by_act * up * (open_ + silu * (1 - open_))).astype(BF16)
            gate_s[at, :] = by_gate
            up_s[at, :] = by_up
            sum_s[at, :] += _dot(by_gate, g_ref[...], 1, 1) + _dot(by_up, u_ref[...], 1, 1)

        _tokens(tokens, some)
        dg_ref[...] = _dot(bt_s[...], gate_s[...], 1, 0).astype(BF16)
        du_ref[...] = _dot(bt_s[...], up_s[...], 1, 0).astype(BF16)
        dd_ref[...] = _dot(byt_s[...], act_s[...], 1, 0).astype(BF16).T

        @pl.when(step == steps - 1)
        def _():
            def last(at):
                wide = h_ref[at, :].astype(F32)
                scale = _scale(wide)
                by_b = sum_s[at, :].astype(BF16).astype(F32)
                by = by_b * scale - wide * (scale * scale * scale) * jnp.mean(by_b * wide, -1, keepdims=True)
                dh_ref[at, :] = (by.astype(BF16).astype(F32) + by_ref[at, :].astype(F32)).astype(BF16)

            _tokens(tokens, last)

    half, full = pltpu.VMEM((tokens, d), BF16), pltpu.VMEM((tokens, d), F32)
    chunk, turned_ = pltpu.VMEM((tokens, CHUNK), BF16), pltpu.VMEM((d, tokens), BF16)
    return _call(body, steps, [h, by_out, w_gate, w_up, w_down], [_whole(h), _whole(h), across, across, down],
                 [_shape(h.shape), _shape(w_gate.shape), _shape(w_up.shape), _shape(w_down.shape)], [_whole(h), across, across, down],
                 [half, turned_, turned_, full, chunk, chunk, chunk], rider, given, number, 16 * tokens * d * w_gate.shape[1], "gated_bwd")


def matmul(a, w):
    return jnp.dot(a, w, preferred_element_type=F32).astype(BF16)


def normed(h):
    wide = h.astype(F32)
    return (wide * _scale(wide)).astype(BF16)


def turned(t, theta):
    tokens, half = t.shape[0], HEAD // 2
    angle = jnp.arange(tokens, dtype=F32)[:, None] * theta ** (-jnp.arange(half, dtype=F32) / half)
    cos, sin = jnp.cos(angle), jnp.sin(angle)
    parts = []
    for n in range(t.shape[1] // HEAD):
        a, b = t[:, n * HEAD : n * HEAD + half].astype(F32), t[:, n * HEAD + half : (n + 1) * HEAD].astype(F32)
        parts += [a * cos - b * sin, b * cos + a * sin]
    return jnp.concatenate(parts, -1).astype(BF16)


def projected(h, wq, wk, wv):
    a = normed(h)
    return turned(matmul(a, wq), THETA), turned(matmul(a, wk), THETA), matmul(a, wv)


def joined(h, mixed, wo):
    return h + matmul(mixed, wo)


def adamw(w, m, v, g):
    m = 0.9 * m + 0.1 * g
    v = 0.95 * v + 0.05 * g * g
    step = m * lax.rsqrt(v + 1e-8) + 0.1 * w
    return (w - 0.02 * step).astype(BF16), m, v


def clipped(gradients, sum_of_squares, count):
    factor = jnp.minimum(1.0, 0.5 * lax.rsqrt(sum_of_squares / count + 1e-30))
    return [g * factor for g in gradients]


def solution(mesh):
    def step(x, dy, *arrays):
        weights, m, v = (arrays[i : i + 7] for i in (0, 7, 14))
        shards = dict(zip(NAMES, weights, strict=True))
        blocks = {name: w.shape[1:] for name, w in shards.items()}
        given = lambda names: [shards[n] for n in names]
        h, tokens = x[0], x.shape[1]

        w = [{}, {}]
        w[0] |= zip(ATT, alone(Gather(ATT, blocks, 0), given(ATT), 0))
        q0, k0, v0 = qkv0 = projected(h, w[0]["wq"], w[0]["wk"], w[0]["wv"])
        (mix0, lse0), got = attend(*qkv0, Gather(MLP, blocks, 0), given(MLP), 1)
        w[0] |= zip(MLP, got)
        mid0 = joined(h, mix0, w[0]["wo"])
        early = ATT + MLP[:2]
        (h1,), got = gated(mid0, *(w[0][n] for n in MLP), Gather(early, blocks, 1), given(early), 2)
        w[1] |= zip(early, got)
        qkv1 = projected(h1, w[1]["wq"], w[1]["wk"], w[1]["wv"])
        (mix1, lse1), got = attend(*qkv1, Gather(MLP[2:], blocks, 1), given(MLP[2:]), 3)
        w[1] |= zip(MLP[2:], got)
        mid1 = joined(h1, mix1, w[1]["wo"])

        def first_half(h, mid, mixed, lse, qkv, by_mid, w, rider, given, number):
            by_mixed, by_wo = jax.vjp(matmul, mixed, w["wo"])[1](by_mid)
            delta = (by_mixed.astype(F32) * mixed.astype(F32)).reshape(tokens // BLOCK, BLOCK, -1, HEAD).sum(-1).transpose(0, 2, 1).reshape(lse.shape)
            by_qkv, got = attend_bwd(*qkv, by_mixed, lse, delta, rider, given, number)
            back = jax.vjp(projected, h, w["wq"], w["wk"], w["wv"])[1]
            by_h, *by_w = back(tuple(by_qkv))
            return by_mid + by_h, [*by_w, by_wo], got

        (by_mid1, *by_mlp1), _ = gated_bwd(mid1, dy[0], *(w[1][n] for n in MLP))
        by_h1, by_att1, g_mlp1 = first_half(h1, mid1, mix1, lse1, qkv1, by_mid1, w[1], Scatter(MLP, blocks), by_mlp1, 4)
        (by_mid0, *by_mlp0), g_att1 = gated_bwd(mid0, by_h1, *(w[0][n] for n in MLP), Scatter(ATT, blocks), by_att1, 5)
        _, by_att0, g_mlp0 = first_half(h, mid0, mix0, lse0, qkv0, by_mid0, w[0], Scatter(MLP, blocks), by_mlp0, 6)
        g_att0 = alone(Scatter(ATT, blocks), by_att0, 7)

        gradients = [jnp.stack(pair).astype(F32) for pair in zip(g_att0 + g_mlp0, g_att1 + g_mlp1)]
        squares = lax.psum(sum(jnp.sum(g * g) for g in gradients), "dp")
        gradients = clipped(gradients, squares, 8 * sum(g.size for g in gradients))
        new = [adamw(w.astype(F32), m, v, g) for w, m, v, g in zip(weights, m, v, gradients, strict=True)]
        return tuple(one[which] for which in range(3) for one in new)

    states, cut = P(("rep", "dp"), None, None), P(None, "dp", None)
    return jax.shard_map(
        step,
        mesh=mesh,
        in_specs=(states, states) + (cut,) * 21,
        out_specs=(P("rep", "dp", None),) * 21,
        check_vma=False,
    )
```

```python
import functools

import jax
import jax.numpy as jnp
from jax import lax
from jax.experimental import pallas as pl
from jax.experimental.pallas import tpu as pltpu
from jax.sharding import PartitionSpec as P

HEAD = 256
THETA = 10000
NAMES = ("wq", "wk", "wv", "wo", "w_gate", "w_up", "w_down")
ATT, MLP = NAMES[:4], NAMES[4:]
NEG = -1e30
HIDDEN = 2 * NEG
LOG2E = 1.4426950408889634
VMEM = 62 * 2**20
BLOCK = 512
CHUNK = 512
ROWS = 512
ANY = pl.BlockSpec(memory_space=pl.ANY)
MESH = pl.DeviceIdType.MESH
F32, BF16 = jnp.float32, jnp.bfloat16


def _dot(a, b, ca, cb):
    return lax.dot_general(a, b, (((ca,), (cb,)), ((), ())), preferred_element_type=F32)


def _units(names, blocks):
    cut = []
    for name in names:
        rows, columns = blocks[name]
        if name in ("wo", "w_down"):
            cut += [(name, 0, rows // 2, 0), (name, rows // 2, rows // 2, 1)]
        else:
            cut += [(name, 0, rows, 0 if name in ("wq", "w_gate") else 1)]
    return cut


def _around(way):
    me = lax.axis_index("dp")
    core, y, x = lax.rem(me, 2), lax.rem(lax.div(me, 2), 2), lax.div(me, 4)
    over_x, over_y = 4 - 8 * x, 2 - 4 * y
    first, second = (over_x, over_y) if way == 0 else (over_y, over_x)
    return me, 1 - 2 * core, first, second, over_x + over_y


def _meet():
    me, other, first, second, _ = _around(0)
    barrier = pltpu.get_barrier_semaphore()
    for way in (other, first, second):
        pl.semaphore_signal(barrier, inc=1, device_id={"dp": me + way}, device_id_type=MESH)
    pl.semaphore_wait(barrier, 3)


class Gather:
    def __init__(self, names, blocks, layer):
        self.names, self.blocks, self.layer = names, blocks, layer
        self.units = _units(names, blocks)

    def in_specs(self):
        return [ANY] * len(self.names)

    def out_specs(self):
        return [ANY] * len(self.names)

    def out_shape(self):
        return [jax.ShapeDtypeStruct((8 * self.blocks[n][0], self.blocks[n][1]), BF16) for n in self.names]

    def scratch(self):
        n = len(self.units)
        return [pltpu.SemaphoreType.DMA((n,)), pltpu.SemaphoreType.DMA((n, 7)), pltpu.SemaphoreType.DMA((n, 7))]

    def bind(self, ins, outs, scratch):
        self.shards, self.whole = dict(zip(self.names, ins)), dict(zip(self.names, outs))
        self.local, self.send, self.recv = scratch

    def _piece(self, unit, device):
        name, at, rows, _ = unit
        return self.whole[name].at[pl.ds(pl.multiple_of(device * self.blocks[name][0] + at, 16), rows)]

    def _copy(self, i, slot, arrived=False):
        unit = self.units[i]
        name, at, rows, way = unit
        me, other, first, second, across = _around(way)
        own = self.shards[name].at[self.layer, pl.ds(at, rows)]
        source, owner, to, comes = (
            (own, me, first, me + first),
            (own, me, second, me + second),
            (own, me, other, me + other),
            (None, me + first, second, me + across),
            (None, me + first, other, me + first + other),
            (None, me + second, other, me + second + other),
            (None, me + across, other, me + across + other),
        )[slot]
        if arrived:
            source, owner = None, comes
        target = self._piece(unit, owner)
        return pltpu.make_async_remote_copy(target if source is None else source, target, self.send.at[i, slot], self.recv.at[i, slot],
                                            device_id={"dp": me + to}, device_id_type=MESH)

    def _mine(self, i):
        name, at, rows, way = self.units[i]
        return pltpu.make_async_copy(self.shards[name].at[self.layer, pl.ds(at, rows)], self._piece(self.units[i], lax.axis_index("dp")), self.local.at[i])

    def begin(self):
        for i in range(len(self.units)):
            for slot in range(3):
                self._copy(i, slot).start()
            self._mine(i).start()

    def middle(self):
        for i in range(len(self.units)):
            self._copy(i, 0, True).wait_recv()
            self._copy(i, 3).start()
            self._copy(i, 4).start()
            self._copy(i, 1, True).wait_recv()
            self._copy(i, 5).start()

    def end(self):
        for i in range(len(self.units)):
            self._copy(i, 3, True).wait_recv()
            self._copy(i, 6).start()
        for i in range(len(self.units)):
            for slot in (2, 4, 5, 6):
                self._copy(i, slot, True).wait_recv()
            for slot in range(7):
                self._copy(i, slot).wait_send()
            self._mine(i).wait()

    def actions(self, steps):
        if steps == 1:
            return {0: ([_meet, self.begin, self.middle, self.end], [])}
        return {0: ([_meet, self.begin], []), steps - 1: ([self.middle], [self.end])}


class Scatter:
    def __init__(self, names, blocks):
        self.names, self.blocks = names, blocks
        self.units = _units(names, blocks)

    def in_specs(self):
        return [ANY] * len(self.names)

    def out_specs(self):
        return [pl.BlockSpec(self.blocks[n], lambda *_: (0, 0), pipeline_mode=pl.Buffered(1)) for n in self.names]

    def out_shape(self):
        return [jax.ShapeDtypeStruct(self.blocks[n], BF16) for n in self.names]

    def scratch(self):
        n, dma = len(self.units), pltpu.SemaphoreType.DMA
        found = [dma((n, 4)), dma((n, 4)), dma((n, 4)), dma((n, 2)), dma((n, 2)), dma((n,)), dma((n,))]
        for name, _, rows, _ in self.units:
            columns = self.blocks[name][1]
            found += [pltpu.VMEM((k, rows, columns), BF16) for k in (4, 4, 2, 2, 1, 1)]
        return found

    def bind(self, ins, outs, scratch):
        self.terms, self.outs = dict(zip(self.names, ins)), dict(zip(self.names, outs))
        self.load, self.send0, self.recv0, self.send1, self.recv1, self.send2, self.recv2 = scratch[:7]
        rest = scratch[7:]
        self.buffers = [rest[6 * i : 6 * i + 6] for i in range(len(self.units))]

    def _block(self, unit, device):
        name, at, rows, _ = unit
        return self.terms[name].at[pl.ds(pl.multiple_of(device * self.blocks[name][0] + at, 16), rows)]

    def _own(self, i, j):
        me, other, *ways = _around(self.units[i][3])
        return pltpu.make_async_copy(self._block(self.units[i], me + ([0] + ways)[j]), self.buffers[i][0].at[j], self.load.at[i, j])

    def _across(self, i, j):
        me, other, *ways = _around(self.units[i][3])
        return pltpu.make_async_remote_copy(self._block(self.units[i], me + other + ([0] + ways)[j]), self.buffers[i][1].at[j], self.send0.at[i, j],
                                            self.recv0.at[i, j], device_id={"dp": me + other}, device_id_type=MESH)

    def _first(self, i, j):
        me, _, first, _, _ = _around(self.units[i][3])
        return pltpu.make_async_remote_copy(self.buffers[i][2].at[j], self.buffers[i][3].at[j], self.send1.at[i, j], self.recv1.at[i, j],
                                            device_id={"dp": me + first}, device_id_type=MESH)

    def _second(self, i):
        me, _, _, second, _ = _around(self.units[i][3])
        return pltpu.make_async_remote_copy(self.buffers[i][4].at[0], self.buffers[i][5].at[0], self.send2.at[i], self.recv2.at[i],
                                            device_id={"dp": me + second}, device_id_type=MESH)

    def begin(self):
        for js in ((1, 3), (2, 0)):
            for i in range(len(self.units)):
                for j in js:
                    self._across(i, j).start()
                    self._own(i, j).start()

    def _ready(self, i, j):
        self._own(i, j).wait()
        self._across(i, j).wait_recv()

    def _add(self, rows, store, *terms):
        def some(t, _):
            at = pl.ds(pl.multiple_of(t * 16, 16), 16)
            store(at, sum(term[at, :].astype(F32) for term in terms))
            return 0

        lax.fori_loop(0, rows // 16, some, 0)

    def part1(self):
        for i, (_, _, rows, _) in enumerate(self.units):
            own, came, out = self.buffers[i][:3]
            for j, k in ((1, 0), (3, 1)):
                self._ready(i, j)

                def store(at, value, k=k, out=out):
                    out[k, at, :] = value.astype(BF16)

                self._add(rows, store, own.at[j], came.at[j])
            if i:
                self._first(i - 1, 0).start()
                self._first(i - 1, 1).start()

    def part2(self):
        for j in range(2):
            self._first(len(self.units) - 1, j).start()

    def part3(self):
        for i, (_, _, rows, _) in enumerate(self.units):
            own, came, _, got, out, _ = self.buffers[i]
            self._ready(i, 2)
            self._first(i, 0).wait_recv()
            self._first(i, 1).wait_recv()

            def store(at, value, out=out):
                out[0, at, :] = value.astype(BF16)

            self._add(rows, store, own.at[2], came.at[2], got.at[1])
            if i:
                self._second(i - 1).start()

    def part4(self):
        self._second(len(self.units) - 1).start()

    def end(self):
        for i, (name, start, rows, _) in enumerate(self.units):
            own, came, _, got, _, last = self.buffers[i]
            self._ready(i, 0)
            self._second(i).wait_recv()

            def store(at, value, name=name, start=start):
                self.outs[name][pl.ds(pl.multiple_of(start + at.start, 16), 16), :] = value.astype(BF16)

            self._add(rows, store, own.at[0], came.at[0], got.at[0], last.at[0])
        for i in range(len(self.units)):
            for j in range(4):
                self._across(i, j).wait_send()
            for j in range(2):
                self._first(i, j).wait_send()
            self._second(i).wait_send()

    def actions(self, steps):
        if steps == 1:
            return {0: ([_meet, self.begin, self.part1, self.part2, self.part3, self.part4, self.end], [])}
        if steps == 8:
            return {0: ([_meet, self.begin], []), 4: ([self.part1], []), 5: ([self.part2], []), 7: ([self.part3], [self.part4, self.end])}
        return {0: ([_meet, self.begin], []), 1: ([self.part1], [self.part2]), steps - 2: ([self.part3], [self.part4]), steps - 1: ([], [self.end])}


def _call(body, steps, ins, in_specs, outs, out_specs, scratch, rider=None, given=(), number=0, flops=0, name=None):
    ni, no, ns = len(in_specs), len(out_specs), len(scratch)
    more_in, more_out, more_specs, more_scratch = ([], [], [], []) if rider is None else (rider.in_specs(), rider.out_shape(), rider.out_specs(), rider.scratch())

    def kernel(*refs):
        cuts = [ni, len(more_in), no, len(more_out), ns, len(more_scratch)]
        parts, at = [], 0
        for n in cuts:
            parts.append(refs[at : at + n])
            at += n
        step = pl.program_id(0)
        acts = {}
        if rider is not None:
            rider.bind(parts[1], parts[3], parts[5])
            acts = rider.actions(steps)

        def run(which):
            for s, lists in acts.items():
                if lists[which]:
                    if steps == 1:
                        for act in lists[which]:
                            act()
                    else:

                        @pl.when(step == s)
                        def _(todo=lists[which]):
                            for act in todo:
                                act()

        run(0)
        body(step, parts[0], parts[2], parts[4])
        run(1)

    params = dict(dimension_semantics=("arbitrary",), vmem_limit_bytes=VMEM)
    if rider is not None:
        params |= dict(collective_id=number, has_side_effects=True)
    got = pl.pallas_call(
        kernel,
        grid=(steps,),
        in_specs=[*in_specs, *more_in],
        out_specs=[*out_specs, *more_specs],
        out_shape=[*outs, *more_out],
        scratch_shapes=[*scratch, *more_scratch],
        compiler_params=pltpu.CompilerParams(**params),
        cost_estimate=pl.CostEstimate(flops=int(flops) + 1, bytes_accessed=10**6, transcendentals=0),
        name=name,
    )(*ins, *given)
    return list(got[:no]), list(got[no:])


def _whole(a):
    return pl.BlockSpec(a.shape, lambda *_: (0,) * len(a.shape), pipeline_mode=pl.Buffered(1))


def _shape(shape, dtype=BF16):
    return jax.ShapeDtypeStruct(shape, dtype)


def alone(rider, given, number):
    return _call(lambda *_: None, 1, [], [], [], [], [], rider, given, number, name="exchange")[1]


def _hidden():
    return lax.broadcasted_iota(jnp.int32, (BLOCK, BLOCK), 0) > lax.broadcasted_iota(jnp.int32, (BLOCK, BLOCK), 1)


def _strip(ref, head, a):
    return ref[a * BLOCK : (a + 1) * BLOCK, head * HEAD : (head + 1) * HEAD]


def _turn(t, cos, sin):
    half, parts = HEAD // 2, []
    for at in range(0, t.shape[1], HEAD):
        a, b = t[:, at : at + half].astype(F32), t[:, at + half : at + HEAD].astype(F32)
        parts += [a * cos - b * sin, b * cos + a * sin]
    return jnp.concatenate(parts, -1).astype(BF16)


def attend(h, w, tables, rider=None, given=(), number=0):
    wq, wk, wv, wo = (w[n] for n in ATT)
    tokens, heads = h.shape[0], wq.shape[1] // HEAD
    blocks, scale = tokens // BLOCK, HEAD**-0.5
    e = scale * LOG2E

    def body(step, ins, outs, scratch):
        h_ref, wq_ref, wk_ref, wv_ref, wo_ref, cos_ref, sin_ref = ins
        mid_ref, q_ref, k_ref, v_ref, o_ref, lse_ref = outs
        top_s, mix_s = scratch

        @pl.when(step < blocks)
        def _():
            at = pl.ds(pl.multiple_of(step * BLOCK, BLOCK), BLOCK)
            wide = h_ref[at, :].astype(F32)
            a = (wide * _scale(wide)).astype(BF16)
            cos, sin = cos_ref[at, :], sin_ref[at, :]
            q_ref[at, :] = _turn(_dot(a, wq_ref[...], 1, 0).astype(BF16), cos, sin)
            k_ref[at, :] = _turn(_dot(a, wk_ref[...], 1, 0).astype(BF16), cos, sin)
            v_ref[at, :] = _dot(a, wv_ref[...], 1, 0).astype(BF16)

        def block(j):
            strips = [(n, a) for a in range(j, blocks) for n in range(heads)]
            here = slice(j * BLOCK, (j + 1) * BLOCK)
            keys = k_ref[here, :]
            values = jnp.concatenate([v_ref[here, :].T, jnp.ones((8, BLOCK), BF16)], axis=0)
            scores = [_dot(keys, _strip(q_ref, n, a), 1, 1) for n, a in strips]
            weights, keeps = [], []
            for (n, a), s in zip(strips, scores):
                i = a * heads + n
                if a == j:
                    s = jnp.where(_hidden(), HIDDEN, s)
                top = s.max(axis=0, keepdims=True)
                if j:
                    old = top_s[i : i + 1, :]
                    top = jnp.maximum(old, top)
                    keeps.append(jnp.exp2((old - top) * e))
                else:
                    keeps.append(None)
                top_s[i : i + 1, :] = top
                weights.append(jnp.exp2((s - top) * e).astype(BF16))
            done = []
            for (n, a), p, keep in zip(strips, weights, keeps):
                i = a * heads + n
                mix = _dot(values, p, 1, 0)
                if j:
                    mix = mix_s[i] * keep + mix
                if a > j:
                    mix_s[i] = mix
                else:
                    total = mix[HEAD : HEAD + 1, :]
                    done.append((mix[:HEAD, :] * (1 / total)).T.astype(BF16))
                    o_ref[here, n * HEAD : (n + 1) * HEAD] = done[-1]
                    lse_ref[i : i + 1, :] = top_s[i : i + 1, :] * scale + jnp.log(total)
            out = _dot(jnp.concatenate(done, -1), wo_ref[...], 1, 0).astype(BF16).astype(F32)
            mid_ref[here, :] = (h_ref[here, :].astype(F32) + out).astype(BF16)

        for j in range(blocks):
            pl.when(step == blocks + j)(functools.partial(block, j))

    n = heads * blocks
    ins = [h, wq, wk, wv, wo, *tables]
    outs = [_shape(h.shape), _shape((tokens, heads * HEAD)), _shape((tokens, HEAD)), _shape((tokens, HEAD)), _shape((tokens, heads * HEAD)), _shape((n, BLOCK), F32)]
    flops = 2 * tokens * (h.shape[1] * 1536 + 1.2 * tokens * heads * HEAD)
    return _call(body, 2 * blocks, ins, [_whole(a) for a in ins], outs, [_whole(a) for a in outs],
                 [pltpu.VMEM((n, BLOCK), F32), pltpu.VMEM((n, HEAD + 8, BLOCK), F32)], rider, given, number, flops, "attend")


def attend_bwd(h, w, tables, kept, by_mid, wanted, rider=None, given=(), number=0):
    q, k, v, o, lse = kept
    wq, wk, wv, wo = (w[n] for n in ATT)
    (tokens, d), heads = h.shape, wq.shape[1] // HEAD
    blocks, scale = tokens // BLOCK, HEAD**-0.5
    e = scale * LOG2E

    def body(step, ins, outs, scratch):
        h_ref, wq_ref, wk_ref, wv_ref, wo_ref, cos_ref, sin_ref, q_ref, k_ref, v_ref, o_ref, lse_ref, by_ref = ins
        dwq_ref, dwk_ref, dwv_ref, dwo_ref, *dh_ref = outs
        dq_s, do_s, delta_s, dwq_s, dwk_s, dwv_s, dwo_s = scratch

        def before(t):
            here = slice(t * BLOCK, (t + 1) * BLOCK)
            by, o = by_ref[here, :], o_ref[here, :]
            do = _dot(by, wo_ref[...], 1, 1).astype(BF16)
            do_s[here, :] = do
            dots = (do.astype(F32) * o.astype(F32)).T
            for n in range(heads):
                i = t * heads + n
                delta_s[i : i + 1, :] = dots[n * HEAD : (n + 1) * HEAD, :].sum(axis=0, keepdims=True)
            term = _dot(o.T, by, 1, 0)
            if t:
                term = dwo_s[...] + term
            if t < blocks - 1:
                dwo_s[...] = term
            else:
                dwo_ref[...] = term.astype(BF16)

        def block(j):
            here = slice(j * BLOCK, (j + 1) * BLOCK)
            strips = [(n, a) for a in range(j, blocks) for n in range(heads)]
            keys, values = k_ref[here, :], v_ref[here, :]
            turned_keys = keys.T
            dk = dv = None
            dq = []
            scores = [_dot(keys, _strip(q_ref, n, a), 1, 1) for n, a in strips]
            dps = [_dot(values, _strip(do_s, n, a), 1, 1) for n, a in strips]
            for (n, a), s, dp in zip(strips, scores, dps):
                i = a * heads + n
                p = jnp.exp2(s * e - lse_ref[i : i + 1, :] * LOG2E)
                if a == j:
                    p = jnp.where(_hidden(), 0.0, p)
                ds = (p * (dp - delta_s[i : i + 1, :])).astype(BF16)
                by_v = _dot(p.astype(BF16), _strip(do_s, n, a), 1, 0)
                by_k = _dot(ds, _strip(q_ref, n, a), 1, 0)
                dv, dk = (by_v, by_k) if dv is None else (dv + by_v, dk + by_k)
                by_q = _dot(turned_keys, ds, 1, 0)
                if j:
                    by_q = dq_s[i] + by_q
                if a > j:
                    dq_s[i] = by_q
                else:
                    dq.append((by_q * scale).T.astype(BF16))
            cos, sin = cos_ref[here, :], -sin_ref[here, :]
            dq = _turn(jnp.concatenate(dq, -1), cos, sin)
            dk = _turn((dk * scale).astype(BF16), cos, sin)
            dv = dv.astype(BF16)
            wide = h_ref[here, :].astype(F32)
            size = _scale(wide)
            at = (wide * size).astype(BF16).T
            for by, sum_s, out_ref in ((dq, dwq_s, dwq_ref), (dk, dwk_s, dwk_ref), (dv, dwv_s, dwv_ref)):
                term = _dot(at, by, 1, 0)
                if j:
                    term = sum_s[...] + term
                if j < blocks - 1:
                    sum_s[...] = term
                else:
                    out_ref[...] = term.astype(BF16)
            if wanted:
                by_a = (_dot(dv, wv_ref[...], 1, 1).astype(BF16).astype(F32) + _dot(dk, wk_ref[...], 1, 1).astype(BF16).astype(F32)
                        + _dot(dq, wq_ref[...], 1, 1).astype(BF16).astype(F32)).astype(BF16).astype(F32)
                by_h = by_a * size - wide * (size * size * size) * jnp.mean(by_a * wide, -1, keepdims=True)
                dh_ref[0][here, :] = (by_h.astype(BF16).astype(F32) + by_ref[here, :].astype(F32)).astype(BF16)

        for t in range(blocks):
            pl.when(step == t)(functools.partial(before, t))
            pl.when(step == blocks + t)(functools.partial(block, t))

    ins = [h, wq, wk, wv, wo, *tables, q, k, v, o, lse, by_mid]
    outs = [_shape(a.shape) for a in (wq, wk, wv, wo) + ((h,) if wanted else ())]
    n = heads * blocks
    full = lambda a: pltpu.VMEM(a.shape, F32)
    flops = 4 * tokens * (d * 1536 + 1.5 * tokens * heads * HEAD)
    return _call(body, 2 * blocks, ins, [_whole(a) for a in ins], outs, [_whole(a) for a in outs],
                 [pltpu.VMEM((n, HEAD, BLOCK), F32), pltpu.VMEM(o.shape, BF16), pltpu.VMEM((n, BLOCK), F32), full(wq), full(wk), full(wv), full(wo)],
                 rider, given, number, flops, "attend_bwd")


def _scale(wide):
    return lax.rsqrt(jnp.mean(wide * wide, -1, keepdims=True) + 1e-6)


def _tokens(n, do):
    def some(t, _):
        do(pl.ds(pl.multiple_of(t * ROWS, ROWS), ROWS))
        return 0

    lax.fori_loop(0, n // ROWS, some, 0)


def _chunks(w_gate, w_down):
    across = pl.BlockSpec((w_gate.shape[0], CHUNK), lambda j: (0, j))
    down = pl.BlockSpec((CHUNK, w_down.shape[1]), lambda j: (j, 0))
    return across, down


def gated(h, w_gate, w_up, w_down, rider=None, given=(), number=0):
    tokens, d = h.shape
    steps = w_gate.shape[1] // CHUNK
    across, down = _chunks(w_gate, w_down)

    def body(step, ins, outs, scratch):
        h_ref, g_ref, u_ref, d_ref = ins
        (o_ref,) = outs
        b_s, sum_s = scratch

        @pl.when(step == 0)
        def _():
            def norm(at):
                wide = h_ref[at, :].astype(F32)
                b_s[at, :] = (wide * _scale(wide)).astype(BF16)
                sum_s[at, :] = jnp.zeros((ROWS, d), F32)

            _tokens(tokens, norm)

        def some(at):
            b = b_s[at, :]
            gate, up = _dot(b, g_ref[...], 1, 0), _dot(b, u_ref[...], 1, 0)
            act = (gate * (1 / (1 + jnp.exp(-gate))) * up).astype(BF16)
            sum_s[at, :] += _dot(act, d_ref[...], 1, 0)

        _tokens(tokens, some)

        @pl.when(step == steps - 1)
        def _():
            def last(at):
                o_ref[at, :] = (h_ref[at, :].astype(F32) + sum_s[at, :].astype(BF16).astype(F32)).astype(BF16)

            _tokens(tokens, last)

    return _call(body, steps, [h, w_gate, w_up, w_down], [_whole(h), across, across, down], [_shape(h.shape)], [_whole(h)],
                 [pltpu.VMEM((tokens, d), BF16), pltpu.VMEM((tokens, d), F32)], rider, given, number, 6 * tokens * d * w_gate.shape[1], "gated")


def gated_bwd(h, by_out, w_gate, w_up, w_down, rider=None, given=(), number=0):
    tokens, d = h.shape
    steps = w_gate.shape[1] // CHUNK
    across, down = _chunks(w_gate, w_down)

    def body(step, ins, outs, scratch):
        h_ref, by_ref, g_ref, u_ref, d_ref = ins
        dh_ref, dg_ref, du_ref, dd_ref = outs
        b_s, bt_s, byt_s, sum_s, act_s, gate_s, up_s = scratch

        @pl.when(step == 0)
        def _():
            def norm(at):
                wide = h_ref[at, :].astype(F32)
                b = (wide * _scale(wide)).astype(BF16)
                b_s[at, :] = b
                bt_s[:, at] = b.T
                byt_s[:, at] = by_ref[at, :].T
                sum_s[at, :] = jnp.zeros((ROWS, d), F32)

            _tokens(tokens, norm)

        def some(at):
            b, by = b_s[at, :], by_ref[at, :]
            gate, up = _dot(b, g_ref[...], 1, 0), _dot(b, u_ref[...], 1, 0)
            by_act = _dot(by, d_ref[...], 1, 1).astype(BF16).astype(F32)
            open_ = 1 / (1 + jnp.exp(-gate))
            silu = gate * open_
            act_s[at, :] = (silu * up).astype(BF16)
            by_up = (by_act * silu).astype(BF16)
            by_gate = (by_act * up * (open_ + silu * (1 - open_))).astype(BF16)
            gate_s[at, :] = by_gate
            up_s[at, :] = by_up
            sum_s[at, :] += _dot(by_gate, g_ref[...], 1, 1) + _dot(by_up, u_ref[...], 1, 1)

        _tokens(tokens, some)
        dg_ref[...] = _dot(bt_s[...], gate_s[...], 1, 0).astype(BF16)
        du_ref[...] = _dot(bt_s[...], up_s[...], 1, 0).astype(BF16)
        dd_ref[...] = _dot(byt_s[...], act_s[...], 1, 0).astype(BF16).T

        @pl.when(step == steps - 1)
        def _():
            def last(at):
                wide = h_ref[at, :].astype(F32)
                scale = _scale(wide)
                by_b = sum_s[at, :].astype(BF16).astype(F32)
                by = by_b * scale - wide * (scale * scale * scale) * jnp.mean(by_b * wide, -1, keepdims=True)
                dh_ref[at, :] = (by.astype(BF16).astype(F32) + by_ref[at, :].astype(F32)).astype(BF16)

            _tokens(tokens, last)

    half, full = pltpu.VMEM((tokens, d), BF16), pltpu.VMEM((tokens, d), F32)
    chunk, turned_ = pltpu.VMEM((tokens, CHUNK), BF16), pltpu.VMEM((d, tokens), BF16)
    return _call(body, steps, [h, by_out, w_gate, w_up, w_down], [_whole(h), _whole(h), across, across, down],
                 [_shape(h.shape), _shape(w_gate.shape), _shape(w_up.shape), _shape(w_down.shape)], [_whole(h), across, across, down],
                 [half, turned_, turned_, full, chunk, chunk, chunk], rider, given, number, 16 * tokens * d * w_gate.shape[1], "gated_bwd")


def finish(rider, given, others, number):
    n, ng = len(others), len(given)

    def squares(ref):
        rows, columns = ref.shape

        def some(t, total):
            g = ref[pl.ds(pl.multiple_of(t * 16, 16), 16), :].astype(F32)
            g = g * g
            g = g[:8, :] + g[8:, :]
            return total + sum(g[:, c : c + 128] for c in range(0, columns, 128))

        return lax.fori_loop(0, rows // 16, some, jnp.zeros((8, 128), F32))

    def kernel(*refs):
        other_refs, given_refs, refs = refs[:n], refs[n : n + ng], refs[n + ng :]
        out_refs, total_ref, refs = refs[:ng], refs[ng], refs[ng + 1 :]
        mine_s, all_s, send, recv = refs[:4]
        rider.bind(given_refs, out_refs, refs[4:])
        me = lax.axis_index("dp")
        barrier = pltpu.get_barrier_semaphore()
        for k in range(1, 8):
            pl.semaphore_signal(barrier, inc=1, device_id={"dp": lax.rem(me + k, 8)}, device_id_type=MESH)
        pl.semaphore_wait(barrier, 7)
        rider.begin()
        total = sum(squares(ref) for ref in other_refs)
        for act in (rider.part1, rider.part2, rider.part3, rider.part4, rider.end):
            act()
        mine_s[...] = total + sum(squares(ref) for ref in out_refs)

        def copy(k):
            return pltpu.make_async_remote_copy(mine_s, all_s.at[me], send.at[k], recv.at[k], device_id={"dp": lax.rem(me + k, 8)}, device_id_type=MESH)

        def arrived(k):
            place = all_s.at[lax.rem(me + 8 - k, 8)]
            return pltpu.make_async_remote_copy(place, place, send.at[k], recv.at[k], device_id={"dp": me}, device_id_type=MESH)

        for k in range(1, 8):
            copy(k).start()
        all_s[me] = mine_s[...]
        for k in range(1, 8):
            arrived(k).wait_recv()
        for k in range(1, 8):
            copy(k).wait_send()
        total_ref[...] = sum(all_s[k] for k in range(8))

    outs = [*rider.out_shape(), _shape((8, 128), F32)]
    got = pl.pallas_call(
        kernel,
        grid=(1,),
        in_specs=[*(_whole(a) for a in others), *rider.in_specs()],
        out_specs=[*rider.out_specs(), _whole(outs[-1])],
        out_shape=outs,
        scratch_shapes=[pltpu.VMEM((8, 128), F32), pltpu.VMEM((8, 8, 128), F32), pltpu.SemaphoreType.DMA((8,)), pltpu.SemaphoreType.DMA((8,)), *rider.scratch()],
        compiler_params=pltpu.CompilerParams(dimension_semantics=("arbitrary",), vmem_limit_bytes=VMEM, collective_id=number, has_side_effects=True),
        name="finish",
    )(*others, *given)
    return list(got[:-1]), got[-1]


def angles(tokens):
    half = HEAD // 2
    angle = jnp.arange(tokens, dtype=F32)[:, None] * THETA ** (-jnp.arange(half, dtype=F32) / half)
    return jnp.cos(angle), jnp.sin(angle)


def adamw(w, m, v, g):
    m = 0.9 * m + 0.1 * g
    v = 0.95 * v + 0.05 * g * g
    step = m * lax.rsqrt(v + 1e-8) + 0.1 * w
    return (w - 0.02 * step).astype(BF16), m, v


def clipped(gradients, sum_of_squares, count):
    factor = jnp.minimum(1.0, 0.5 * lax.rsqrt(sum_of_squares / count + 1e-30))
    return [g * factor for g in gradients]


def solution(mesh):
    def step(x, dy, *arrays):
        weights, m, v = (arrays[i : i + 7] for i in (0, 7, 14))
        shards = dict(zip(NAMES, weights, strict=True))
        blocks = {name: w.shape[1:] for name, w in shards.items()}
        given = lambda names: [shards[n] for n in names]
        h0, tokens = x[0], x.shape[1]
        tables = angles(tokens)

        w = [{}, {}]
        w[0] |= zip(ATT, alone(Gather(ATT, blocks, 0), given(ATT), 0))
        (mid0, *kept0), got = attend(h0, w[0], tables, Gather(MLP, blocks, 0), given(MLP), 1)
        w[0] |= zip(MLP, got)
        early = ATT + MLP[:2]
        (h1,), got = gated(mid0, *(w[0][n] for n in MLP), Gather(early, blocks, 1), given(early), 2)
        w[1] |= zip(early, got)
        (mid1, *kept1), got = attend(h1, w[1], tables, Gather(MLP[2:], blocks, 1), given(MLP[2:]), 3)
        w[1] |= zip(MLP[2:], got)

        by, g = [{}, {}], [{}, {}]
        (by_mid1, *got), _ = gated_bwd(mid1, dy[0], *(w[1][n] for n in MLP))
        by[1] |= zip(MLP, got)
        names = MLP[:2]
        (*got, by_h1), sums = attend_bwd(h1, w[1], tables, kept1, by_mid1, True, Scatter(names, blocks), [by[1][n] for n in names], 4)
        by[1] |= zip(ATT, got)
        g[1] |= zip(names, sums)
        names = MLP[2:] + ATT
        (by_mid0, *got), sums = gated_bwd(mid0, by_h1, *(w[0][n] for n in MLP), Scatter(names, blocks), [by[1][n] for n in names], 5)
        by[0] |= zip(MLP, got)
        g[1] |= zip(names, sums)
        got, sums = attend_bwd(h0, w[0], tables, kept0, by_mid0, False, Scatter(MLP, blocks), [by[0][n] for n in MLP], 6)
        by[0] |= zip(ATT, got)
        g[0] |= zip(MLP, sums)
        others = [g[1][n] for n in NAMES] + [g[0][n] for n in MLP]
        sums, squares = finish(Scatter(ATT, blocks), [by[0][n] for n in ATT], others, 7)
        g[0] |= zip(ATT, sums)

        gradients = [jnp.stack([g[0][n], g[1][n]]).astype(F32) for n in NAMES]
        gradients = clipped(gradients, jnp.sum(squares), 8 * sum(g.size for g in gradients))
        new = [adamw(w.astype(F32), m, v, g) for w, m, v, g in zip(weights, m, v, gradients, strict=True)]
        return tuple(one[which] for which in range(3) for one in new)

    states, cut = P(("rep", "dp"), None, None), P(None, "dp", None)
    return jax.shard_map(
        step,
        mesh=mesh,
        in_specs=(states, states) + (cut,) * 21,
        out_specs=(P("rep", "dp", None),) * 21,
        check_vma=False,
    )
```

```python
import functools

import jax
import jax.numpy as jnp
from jax import lax
from jax.experimental import pallas as pl
from jax.experimental.pallas import tpu as pltpu
from jax.sharding import PartitionSpec as P

HEAD = 256
THETA = 10000
NAMES = ("wq", "wk", "wv", "wo", "w_gate", "w_up", "w_down")
ATT, MLP = NAMES[:4], NAMES[4:]
NEG = -1e30
HIDDEN = 2 * NEG
LOG2E = 1.4426950408889634
VMEM = 62 * 2**20
BLOCK = 512
CHUNK = 512
ROWS = 512
ANY = pl.BlockSpec(memory_space=pl.ANY)
MESH = pl.DeviceIdType.MESH
F32, BF16 = jnp.float32, jnp.bfloat16


def _dot(a, b, ca, cb):
    return lax.dot_general(a, b, (((ca,), (cb,)), ((), ())), preferred_element_type=F32)


def _units(names, blocks):
    cut = []
    for name in names:
        rows, columns = blocks[name]
        if name in ("wo", "w_down"):
            cut += [(name, 0, rows // 2, 0), (name, rows // 2, rows // 2, 1)]
        else:
            cut += [(name, 0, rows, 0 if name in ("wq", "w_gate", "last_gate") else 1)]
    return cut


def _around(way):
    me = lax.axis_index("dp")
    core, y, x = lax.rem(me, 2), lax.rem(lax.div(me, 2), 2), lax.div(me, 4)
    over_x, over_y = 4 - 8 * x, 2 - 4 * y
    first, second = (over_x, over_y) if way == 0 else (over_y, over_x)
    return me, 1 - 2 * core, first, second, over_x + over_y


def _meet():
    me, other, first, second, _ = _around(0)
    barrier = pltpu.get_barrier_semaphore()
    for way in (other, first, second):
        pl.semaphore_signal(barrier, inc=1, device_id={"dp": me + way}, device_id_type=MESH)
    pl.semaphore_wait(barrier, 3)


class Gather:
    def __init__(self, names, blocks, layer):
        self.names, self.blocks, self.layer = names, blocks, layer
        self.units = _units(names, blocks)

    def in_specs(self):
        return [ANY] * len(self.names)

    def out_specs(self):
        return [ANY] * len(self.names)

    def out_shape(self):
        return [jax.ShapeDtypeStruct((8 * self.blocks[n][0], self.blocks[n][1]), BF16) for n in self.names]

    def scratch(self):
        n = len(self.units)
        return [pltpu.SemaphoreType.DMA((n,)), pltpu.SemaphoreType.DMA((n, 7)), pltpu.SemaphoreType.DMA((n, 7))]

    def bind(self, ins, outs, scratch):
        self.shards, self.whole = dict(zip(self.names, ins)), dict(zip(self.names, outs))
        self.local, self.send, self.recv = scratch

    def _piece(self, unit, device):
        name, at, rows, _ = unit
        return self.whole[name].at[pl.ds(pl.multiple_of(device * self.blocks[name][0] + at, 16), rows)]

    def _copy(self, i, slot, arrived=False):
        unit = self.units[i]
        name, at, rows, way = unit
        me, other, first, second, across = _around(way)
        own = self.shards[name].at[self.layer, pl.ds(at, rows)]
        source, owner, to, comes = (
            (own, me, first, me + first),
            (own, me, second, me + second),
            (own, me, other, me + other),
            (None, me + first, second, me + across),
            (None, me + first, other, me + first + other),
            (None, me + second, other, me + second + other),
            (None, me + across, other, me + across + other),
        )[slot]
        if arrived:
            source, owner = None, comes
        target = self._piece(unit, owner)
        return pltpu.make_async_remote_copy(target if source is None else source, target, self.send.at[i, slot], self.recv.at[i, slot],
                                            device_id={"dp": me + to}, device_id_type=MESH)

    def _mine(self, i):
        name, at, rows, way = self.units[i]
        return pltpu.make_async_copy(self.shards[name].at[self.layer, pl.ds(at, rows)], self._piece(self.units[i], lax.axis_index("dp")), self.local.at[i])

    def begin(self):
        for i in range(len(self.units)):
            for slot in range(3):
                self._copy(i, slot).start()
            self._mine(i).start()

    def middle(self):
        for i in range(len(self.units)):
            self._copy(i, 0, True).wait_recv()
            self._copy(i, 3).start()
            self._copy(i, 4).start()
            self._copy(i, 1, True).wait_recv()
            self._copy(i, 5).start()

    def end(self):
        for i in range(len(self.units)):
            self._copy(i, 3, True).wait_recv()
            self._copy(i, 6).start()
        for i in range(len(self.units)):
            for slot in (2, 4, 5, 6):
                self._copy(i, slot, True).wait_recv()
            for slot in range(7):
                self._copy(i, slot).wait_send()
            self._mine(i).wait()

    def actions(self, steps):
        if steps == 1:
            return {0: ([_meet, self.begin, self.middle, self.end], [])}
        return {0: ([_meet, self.begin], []), steps - 1: ([self.middle], [self.end])}


class Scatter:
    def __init__(self, names, blocks):
        self.names, self.blocks = names, blocks
        self.units = _units(names, blocks)

    def in_specs(self):
        return [ANY] * len(self.names)

    def out_specs(self):
        return [pl.BlockSpec(self.blocks[n], lambda *_: (0, 0), pipeline_mode=pl.Buffered(1)) for n in self.names]

    def out_shape(self):
        return [jax.ShapeDtypeStruct(self.blocks[n], BF16) for n in self.names]

    def scratch(self):
        n, dma = len(self.units), pltpu.SemaphoreType.DMA
        found = [dma((n, 4)), dma((n, 4)), dma((n, 4)), dma((n, 2)), dma((n, 2)), dma((n,)), dma((n,))]
        for name, _, rows, _ in self.units:
            columns = self.blocks[name][1]
            found += [pltpu.VMEM((k, rows, columns), BF16) for k in (4, 4, 2, 2, 1, 1)]
        return found

    def bind(self, ins, outs, scratch):
        self.terms, self.outs = dict(zip(self.names, ins)), dict(zip(self.names, outs))
        self.load, self.send0, self.recv0, self.send1, self.recv1, self.send2, self.recv2 = scratch[:7]
        rest = scratch[7:]
        self.buffers = [rest[6 * i : 6 * i + 6] for i in range(len(self.units))]

    def _block(self, unit, device):
        name, at, rows, _ = unit
        return self.terms[name].at[pl.ds(pl.multiple_of(device * self.blocks[name][0] + at, 16), rows)]

    def _own(self, i, j):
        me, other, *ways = _around(self.units[i][3])
        return pltpu.make_async_copy(self._block(self.units[i], me + ([0] + ways)[j]), self.buffers[i][0].at[j], self.load.at[i, j])

    def _across(self, i, j):
        me, other, *ways = _around(self.units[i][3])
        return pltpu.make_async_remote_copy(self._block(self.units[i], me + other + ([0] + ways)[j]), self.buffers[i][1].at[j], self.send0.at[i, j],
                                            self.recv0.at[i, j], device_id={"dp": me + other}, device_id_type=MESH)

    def _first(self, i, j):
        me, _, first, _, _ = _around(self.units[i][3])
        return pltpu.make_async_remote_copy(self.buffers[i][2].at[j], self.buffers[i][3].at[j], self.send1.at[i, j], self.recv1.at[i, j],
                                            device_id={"dp": me + first}, device_id_type=MESH)

    def _second(self, i):
        me, _, _, second, _ = _around(self.units[i][3])
        return pltpu.make_async_remote_copy(self.buffers[i][4].at[0], self.buffers[i][5].at[0], self.send2.at[i], self.recv2.at[i],
                                            device_id={"dp": me + second}, device_id_type=MESH)

    def begin(self):
        for js in ((1, 3), (2, 0)):
            for i in range(len(self.units)):
                for j in js:
                    self._across(i, j).start()
                    self._own(i, j).start()

    def _ready(self, i, j):
        self._own(i, j).wait()
        self._across(i, j).wait_recv()

    def _add(self, rows, store, *terms):
        def some(t, _):
            at = pl.ds(pl.multiple_of(t * 16, 16), 16)
            store(at, sum(term[at, :].astype(F32) for term in terms))
            return 0

        lax.fori_loop(0, rows // 16, some, 0)

    def part1(self):
        for i, (_, _, rows, _) in enumerate(self.units):
            own, came, out = self.buffers[i][:3]
            for j, k in ((1, 0), (3, 1)):
                self._ready(i, j)

                def store(at, value, k=k, out=out):
                    out[k, at, :] = value.astype(BF16)

                self._add(rows, store, own.at[j], came.at[j])
            for i in ([i - 1] if i else []) + ([i] if i == len(self.units) - 1 else []):
                self._first(i, 0).start()
                self._first(i, 1).start()

    def part2(self):
        for i, (_, _, rows, _) in enumerate(self.units):
            own, came, _, got, out, _ = self.buffers[i]
            self._ready(i, 2)
            self._first(i, 0).wait_recv()
            self._first(i, 1).wait_recv()

            def store(at, value, out=out):
                out[0, at, :] = value.astype(BF16)

            self._add(rows, store, own.at[2], came.at[2], got.at[1])
            for i in ([i - 1] if i else []) + ([i] if i == len(self.units) - 1 else []):
                self._second(i).start()

    def end(self):
        for i, (name, start, rows, _) in enumerate(self.units):
            own, came, _, got, _, last = self.buffers[i]
            self._ready(i, 0)
            self._second(i).wait_recv()

            def store(at, value, name=name, start=start):
                self.outs[name][pl.ds(pl.multiple_of(start + at.start, 16), 16), :] = value.astype(BF16)

            self._add(rows, store, own.at[0], came.at[0], got.at[0], last.at[0])
        for i in range(len(self.units)):
            for j in range(4):
                self._across(i, j).wait_send()
            for j in range(2):
                self._first(i, j).wait_send()
            self._second(i).wait_send()

    def actions(self, steps):
        if steps == 8:
            return {0: ([_meet, self.begin], []), 4: ([self.part1], []), 7: ([self.part2], [self.end])}
        return {0: ([_meet, self.begin], []), 1: ([self.part1], []), steps - 2: ([self.part2], []), steps - 1: ([], [self.end])}


class Chunks:
    def __init__(self, rows, chunks):
        self.rows, self.n = rows, chunks - 1

    def scratch(self):
        n, rows, dma = self.n, self.rows, pltpu.SemaphoreType.DMA
        sems = [dma((n, 2, 4)), dma((n, 2, 4)), dma((n, 2, 2)), dma((n, 2, 2)), dma((n, 2)), dma((n, 2))]
        block = lambda *lead: pltpu.VMEM((*lead, rows, CHUNK), BF16)
        return [*sems, pltpu.VMEM((2, 2, 8 * rows, CHUNK), BF16), block(n, 2, 4), block(n, 2, 2), block(n, 2, 2), block(n, 2), block(n, 2)]

    def bind(self, outs, scratch):
        self.outs = outs
        self.send0, self.recv0, self.send1, self.recv1, self.send2, self.recv2, self.terms, self.came, self.sum1, self.got1, self.sum2, self.got2 = scratch

    def _block(self, j, u, device):
        return self.terms.at[lax.rem(j, 2), u, pl.ds(pl.multiple_of(device * self.rows, 16), self.rows)]

    def _own(self, j, u, k):
        me, _, *ways = _around(u)
        return self._block(j, u, me + ([0] + ways)[k])[...].astype(F32) + self.came[j, u, k].astype(F32)

    def _across(self, j, u, k):
        me, other, *ways = _around(u)
        return pltpu.make_async_remote_copy(self._block(j, u, me + other + ([0] + ways)[k]), self.came.at[j, u, k], self.send0.at[j, u, k],
                                            self.recv0.at[j, u, k], device_id={"dp": me + other}, device_id_type=MESH)

    def _first(self, j, u, k):
        me, _, first, _, _ = _around(u)
        return pltpu.make_async_remote_copy(self.sum1.at[j, u, k], self.got1.at[j, u, k], self.send1.at[j, u, k], self.recv1.at[j, u, k],
                                            device_id={"dp": me + first}, device_id_type=MESH)

    def _second(self, j, u):
        me, _, _, second, _ = _around(u)
        return pltpu.make_async_remote_copy(self.sum2.at[j, u], self.got2.at[j, u], self.send2.at[j, u], self.recv2.at[j, u],
                                            device_id={"dp": me + second}, device_id_type=MESH)

    def part0(self, j):
        for u in range(2):
            for k in (1, 3, 2, 0):
                self._across(j, u, k).start()

    def part1(self, j):
        for u in range(2):
            for k, at in ((1, 0), (3, 1)):
                self._across(j, u, k).wait_recv()
                self.sum1[j, u, at] = self._own(j, u, k).astype(BF16)

    def part2(self, j):
        for u in range(2):
            for k in range(2):
                self._first(j, u, k).start()

    def part3(self, j):
        for u in range(2):
            self._across(j, u, 2).wait_recv()
            for k in range(2):
                self._first(j, u, k).wait_recv()
            self.sum2[j, u] = (self._own(j, u, 2) + self.got1[j, u, 1].astype(F32)).astype(BF16)

    def part4(self, j):
        for u in range(2):
            self._second(j, u).start()

    def end(self, j):
        for u in range(2):
            self._across(j, u, 0).wait_recv()
            self._second(j, u).wait_recv()
            total = self._own(j, u, 0) + self.got1[j, u, 0].astype(F32) + self.got2[j, u].astype(F32)
            self.outs[u][:, pl.ds(pl.multiple_of(j * CHUNK, CHUNK), CHUNK)] = total.astype(BF16)
        for u in range(2):
            for k in range(4):
                self._across(j, u, k).wait_send()
            for k in range(2):
                self._first(j, u, k).wait_send()
            self._second(j, u).wait_send()


def _call(body, steps, ins, in_specs, outs, out_specs, scratch, rider=None, given=(), number=0, flops=0, name=None, meet=False):
    ni, no, ns = len(in_specs), len(out_specs), len(scratch)
    more_in, more_out, more_specs, more_scratch = ([], [], [], []) if rider is None else (rider.in_specs(), rider.out_shape(), rider.out_specs(), rider.scratch())

    def kernel(*refs):
        cuts = [ni, len(more_in), no, len(more_out), ns, len(more_scratch)]
        parts, at = [], 0
        for n in cuts:
            parts.append(refs[at : at + n])
            at += n
        step = pl.program_id(0)
        acts = {}
        if rider is not None:
            rider.bind(parts[1], parts[3], parts[5])
            acts = rider.actions(steps)
        elif meet:
            acts = {0: ([_meet], [])}

        def run(which):
            for s, lists in acts.items():
                if lists[which]:
                    if steps == 1:
                        for act in lists[which]:
                            act()
                    else:

                        @pl.when(step == s)
                        def _(todo=lists[which]):
                            for act in todo:
                                act()

        run(0)
        body(step, parts[0], parts[2], parts[4])
        run(1)

    params = dict(dimension_semantics=("arbitrary",), vmem_limit_bytes=VMEM)
    if rider is not None or meet:
        params |= dict(collective_id=number, has_side_effects=True)
    got = pl.pallas_call(
        kernel,
        grid=(steps,),
        in_specs=[*in_specs, *more_in],
        out_specs=[*out_specs, *more_specs],
        out_shape=[*outs, *more_out],
        scratch_shapes=[*scratch, *more_scratch],
        compiler_params=pltpu.CompilerParams(**params),
        cost_estimate=pl.CostEstimate(flops=int(flops) + 1, bytes_accessed=10**6, transcendentals=0),
        name=name,
    )(*ins, *given)
    return list(got[:no]), list(got[no:])


def _whole(a):
    return pl.BlockSpec(a.shape, lambda *_: (0,) * len(a.shape), pipeline_mode=pl.Buffered(1))


def _shape(shape, dtype=BF16):
    return jax.ShapeDtypeStruct(shape, dtype)


def alone(rider, given, number):
    return _call(lambda *_: None, 1, [], [], [], [], [], rider, given, number, name="exchange")[1]


def _hidden():
    return lax.broadcasted_iota(jnp.int32, (BLOCK, BLOCK), 0) > lax.broadcasted_iota(jnp.int32, (BLOCK, BLOCK), 1)


def _strip(ref, head, a):
    return ref[a * BLOCK : (a + 1) * BLOCK, head * HEAD : (head + 1) * HEAD]


def _turn(t, cos, sin):
    half, parts = HEAD // 2, []
    for at in range(0, t.shape[1], HEAD):
        a, b = t[:, at : at + half].astype(F32), t[:, at + half : at + HEAD].astype(F32)
        parts += [a * cos - b * sin, b * cos + a * sin]
    return jnp.concatenate(parts, -1).astype(BF16)


def attend(h, w, tables, rider=None, given=(), number=0):
    wq, wk, wv, wo = (w[n] for n in ATT)
    tokens, heads = h.shape[0], wq.shape[1] // HEAD
    blocks, scale = tokens // BLOCK, HEAD**-0.5
    e = scale * LOG2E

    def body(step, ins, outs, scratch):
        h_ref, wq_ref, wk_ref, wv_ref, wo_ref, cos_ref, sin_ref = ins
        mid_ref, q_ref, k_ref, v_ref, o_ref, lse_ref = outs
        top_s, mix_s = scratch

        @pl.when(step < blocks)
        def _():
            at = pl.ds(pl.multiple_of(step * BLOCK, BLOCK), BLOCK)
            wide = h_ref[at, :].astype(F32)
            a = (wide * _scale(wide)).astype(BF16)
            cos, sin = cos_ref[at, :], sin_ref[at, :]
            q_ref[at, :] = _turn(_dot(a, wq_ref[...], 1, 0).astype(BF16), cos, sin)
            k_ref[at, :] = _turn(_dot(a, wk_ref[...], 1, 0).astype(BF16), cos, sin)
            v_ref[at, :] = _dot(a, wv_ref[...], 1, 0).astype(BF16)

        def block(j):
            strips = [(n, a) for a in range(j, blocks) for n in range(heads)]
            here = slice(j * BLOCK, (j + 1) * BLOCK)
            keys = k_ref[here, :]
            values = jnp.concatenate([v_ref[here, :].T, jnp.ones((8, BLOCK), BF16)], axis=0)
            scores = [_dot(keys, _strip(q_ref, n, a), 1, 1) for n, a in strips]
            weights, keeps = [], []
            for (n, a), s in zip(strips, scores):
                i = a * heads + n
                if a == j:
                    s = jnp.where(_hidden(), HIDDEN, s)
                top = s.max(axis=0, keepdims=True)
                if j:
                    old = top_s[i : i + 1, :]
                    top = jnp.maximum(old, top)
                    keeps.append(jnp.exp2((old - top) * e))
                else:
                    keeps.append(None)
                top_s[i : i + 1, :] = top
                weights.append(jnp.exp2((s - top) * e).astype(BF16))
            done = []
            for (n, a), p, keep in zip(strips, weights, keeps):
                i = a * heads + n
                mix = _dot(values, p, 1, 0)
                if j:
                    mix = mix_s[i] * keep + mix
                if a > j:
                    mix_s[i] = mix
                else:
                    total = mix[HEAD : HEAD + 1, :]
                    done.append((mix[:HEAD, :] * (1 / total)).T.astype(BF16))
                    o_ref[here, n * HEAD : (n + 1) * HEAD] = done[-1]
                    lse_ref[i : i + 1, :] = top_s[i : i + 1, :] * scale + jnp.log(total)
            out = _dot(jnp.concatenate(done, -1), wo_ref[...], 1, 0).astype(BF16).astype(F32)
            mid_ref[here, :] = (h_ref[here, :].astype(F32) + out).astype(BF16)

        for j in range(blocks):
            pl.when(step == blocks + j)(functools.partial(block, j))

    n = heads * blocks
    ins = [h, wq, wk, wv, wo, *tables]
    outs = [_shape(h.shape), _shape((tokens, heads * HEAD)), _shape((tokens, HEAD)), _shape((tokens, HEAD)), _shape((tokens, heads * HEAD)), _shape((n, BLOCK), F32)]
    flops = 2 * tokens * (h.shape[1] * 1536 + 1.2 * tokens * heads * HEAD)
    return _call(body, 2 * blocks, ins, [_whole(a) for a in ins], outs, [_whole(a) for a in outs],
                 [pltpu.VMEM((n, BLOCK), F32), pltpu.VMEM((n, HEAD + 8, BLOCK), F32)], rider, given, number, flops, "attend")


def attend_bwd(h, w, tables, kept, by_mid, wanted, rider=None, given=(), number=0):
    q, k, v, o, lse = kept
    wq, wk, wv, wo = (w[n] for n in ATT)
    (tokens, d), heads = h.shape, wq.shape[1] // HEAD
    blocks, scale = tokens // BLOCK, HEAD**-0.5
    e = scale * LOG2E

    def body(step, ins, outs, scratch):
        h_ref, wq_ref, wk_ref, wv_ref, wo_ref, cos_ref, sin_ref, q_ref, k_ref, v_ref, o_ref, lse_ref, by_ref = ins
        dwq_ref, dwk_ref, dwv_ref, dwo_ref, *dh_ref = outs
        dq_s, do_s, delta_s, dwq_s, dwk_s, dwv_s, dwo_s = scratch

        def before(t):
            here = slice(t * BLOCK, (t + 1) * BLOCK)
            by, o = by_ref[here, :], o_ref[here, :]
            do = _dot(by, wo_ref[...], 1, 1).astype(BF16)
            do_s[here, :] = do
            dots = (do.astype(F32) * o.astype(F32)).T
            for n in range(heads):
                i = t * heads + n
                delta_s[i : i + 1, :] = dots[n * HEAD : (n + 1) * HEAD, :].sum(axis=0, keepdims=True)
            term = _dot(o.T, by, 1, 0)
            if t:
                term = dwo_s[...] + term
            if t < blocks - 1:
                dwo_s[...] = term
            else:
                dwo_ref[...] = term.astype(BF16)

        def block(j):
            here = slice(j * BLOCK, (j + 1) * BLOCK)
            strips = [(n, a) for a in range(j, blocks) for n in range(heads)]
            keys, values = k_ref[here, :], v_ref[here, :]
            turned_keys = keys.T
            dk = dv = None
            dq = []
            scores = [_dot(keys, _strip(q_ref, n, a), 1, 1) for n, a in strips]
            dps = [_dot(values, _strip(do_s, n, a), 1, 1) for n, a in strips]
            for (n, a), s, dp in zip(strips, scores, dps):
                i = a * heads + n
                p = jnp.exp2(s * e - lse_ref[i : i + 1, :] * LOG2E)
                if a == j:
                    p = jnp.where(_hidden(), 0.0, p)
                ds = (p * (dp - delta_s[i : i + 1, :])).astype(BF16)
                by_v = _dot(p.astype(BF16), _strip(do_s, n, a), 1, 0)
                by_k = _dot(ds, _strip(q_ref, n, a), 1, 0)
                dv, dk = (by_v, by_k) if dv is None else (dv + by_v, dk + by_k)
                by_q = _dot(turned_keys, ds, 1, 0)
                if j:
                    by_q = dq_s[i] + by_q
                if a > j:
                    dq_s[i] = by_q
                else:
                    dq.append((by_q * scale).T.astype(BF16))
            cos, sin = cos_ref[here, :], -sin_ref[here, :]
            dq = _turn(jnp.concatenate(dq, -1), cos, sin)
            dk = _turn((dk * scale).astype(BF16), cos, sin)
            dv = dv.astype(BF16)
            wide = h_ref[here, :].astype(F32)
            size = _scale(wide)
            at = (wide * size).astype(BF16).T
            for by, sum_s, out_ref in ((dq, dwq_s, dwq_ref), (dk, dwk_s, dwk_ref), (dv, dwv_s, dwv_ref)):
                term = _dot(at, by, 1, 0)
                if j:
                    term = sum_s[...] + term
                if j < blocks - 1:
                    sum_s[...] = term
                else:
                    out_ref[...] = term.astype(BF16)
            if wanted:
                by_a = (_dot(dv, wv_ref[...], 1, 1).astype(BF16).astype(F32) + _dot(dk, wk_ref[...], 1, 1).astype(BF16).astype(F32)
                        + _dot(dq, wq_ref[...], 1, 1).astype(BF16).astype(F32)).astype(BF16).astype(F32)
                by_h = by_a * size - wide * (size * size * size) * jnp.mean(by_a * wide, -1, keepdims=True)
                dh_ref[0][here, :] = (by_h.astype(BF16).astype(F32) + by_ref[here, :].astype(F32)).astype(BF16)

        for t in range(blocks):
            pl.when(step == t)(functools.partial(before, t))
            pl.when(step == blocks + t)(functools.partial(block, t))

    ins = [h, wq, wk, wv, wo, *tables, q, k, v, o, lse, by_mid]
    outs = [_shape(a.shape) for a in (wq, wk, wv, wo) + ((h,) if wanted else ())]
    n = heads * blocks
    full = lambda a: pltpu.VMEM(a.shape, F32)
    flops = 4 * tokens * (d * 1536 + 1.5 * tokens * heads * HEAD)
    return _call(body, 2 * blocks, ins, [_whole(a) for a in ins], outs, [_whole(a) for a in outs],
                 [pltpu.VMEM((n, HEAD, BLOCK), F32), pltpu.VMEM(o.shape, BF16), pltpu.VMEM((n, BLOCK), F32), full(wq), full(wk), full(wv), full(wo)],
                 rider, given, number, flops, "attend_bwd")


def _scale(wide):
    return lax.rsqrt(jnp.mean(wide * wide, -1, keepdims=True) + 1e-6)


def _tokens(n, do):
    def some(t, _):
        do(pl.ds(pl.multiple_of(t * ROWS, ROWS), ROWS))
        return 0

    lax.fori_loop(0, n // ROWS, some, 0)


def _chunks(w_gate, w_down):
    across = pl.BlockSpec((w_gate.shape[0], CHUNK), lambda j: (0, j))
    down = pl.BlockSpec((CHUNK, w_down.shape[1]), lambda j: (j, 0))
    return across, down


def gated(h, w_gate, w_up, w_down, rider=None, given=(), number=0):
    tokens, d = h.shape
    steps = w_gate.shape[1] // CHUNK
    across, down = _chunks(w_gate, w_down)

    def body(step, ins, outs, scratch):
        h_ref, g_ref, u_ref, d_ref = ins
        (o_ref,) = outs
        b_s, sum_s = scratch

        @pl.when(step == 0)
        def _():
            def norm(at):
                wide = h_ref[at, :].astype(F32)
                b_s[at, :] = (wide * _scale(wide)).astype(BF16)
                sum_s[at, :] = jnp.zeros((ROWS, d), F32)

            _tokens(tokens, norm)

        def some(at):
            b = b_s[at, :]
            gate, up = _dot(b, g_ref[...], 1, 0), _dot(b, u_ref[...], 1, 0)
            act = (gate * (1 / (1 + jnp.exp(-gate))) * up).astype(BF16)
            sum_s[at, :] += _dot(act, d_ref[...], 1, 0)

        _tokens(tokens, some)

        @pl.when(step == steps - 1)
        def _():
            def last(at):
                o_ref[at, :] = (h_ref[at, :].astype(F32) + sum_s[at, :].astype(BF16).astype(F32)).astype(BF16)

            _tokens(tokens, last)

    return _call(body, steps, [h, w_gate, w_up, w_down], [_whole(h), across, across, down], [_shape(h.shape)], [_whole(h)],
                 [pltpu.VMEM((tokens, d), BF16), pltpu.VMEM((tokens, d), F32)], rider, given, number, 6 * tokens * d * w_gate.shape[1], "gated")


def gated_bwd(h, by_out, w_gate, w_up, w_down, rider=None, given=(), number=0):
    tokens, d = h.shape
    steps = w_gate.shape[1] // CHUNK
    across, down = _chunks(w_gate, w_down)
    sums = Chunks(d // 8, steps)

    def body(step, ins, outs, scratch):
        h_ref, by_ref, g_ref, u_ref, d_ref = ins
        dh_ref, dd_ref, lg_ref, lu_ref, *sum_refs = outs
        b_s, bt_s, byt_s, sum_s, act_s, gate_s, up_s = scratch[:7]
        sums.bind(sum_refs, scratch[7:])

        @pl.when(step > 0)
        def _():
            sums.part0(step - 1)

        @pl.when(step == 0)
        def _():
            def norm(at):
                wide = h_ref[at, :].astype(F32)
                b = (wide * _scale(wide)).astype(BF16)
                b_s[at, :] = b
                bt_s[:, at] = b.T
                byt_s[:, at] = by_ref[at, :].T
                sum_s[at, :] = jnp.zeros((ROWS, d), F32)

            _tokens(tokens, norm)

        def some(t, _):
            for when, part in ((1, sums.part1), (2, sums.part2)):
                pl.when((t == when) & (step > 0))(lambda part=part: part(step - 1))
            at = pl.ds(pl.multiple_of(t * ROWS, ROWS), ROWS)
            b, by = b_s[at, :], by_ref[at, :]
            gate, up = _dot(b, g_ref[...], 1, 0), _dot(b, u_ref[...], 1, 0)
            by_act = _dot(by, d_ref[...], 1, 1).astype(BF16).astype(F32)
            open_ = 1 / (1 + jnp.exp(-gate))
            silu = gate * open_
            act_s[at, :] = (silu * up).astype(BF16)
            by_up = (by_act * silu).astype(BF16)
            by_gate = (by_act * up * (open_ + silu * (1 - open_))).astype(BF16)
            gate_s[at, :] = by_gate
            up_s[at, :] = by_up
            sum_s[at, :] += _dot(by_gate, g_ref[...], 1, 1) + _dot(by_up, u_ref[...], 1, 1)
            return 0

        lax.fori_loop(0, tokens // ROWS, some, 0)
        pl.when(step > 0)(lambda: sums.part3(step - 1))
        slot = lax.rem(step, 2)
        sums.terms[slot, 0] = _dot(bt_s[...], gate_s[...], 1, 0).astype(BF16)
        pl.when(step > 0)(lambda: sums.part4(step - 1))
        sums.terms[slot, 1] = _dot(bt_s[...], up_s[...], 1, 0).astype(BF16)
        dd_ref[...] = _dot(byt_s[...], act_s[...], 1, 0).astype(BF16).T
        pl.when(step > 0)(lambda: sums.end(step - 1))

        @pl.when(step == steps - 1)
        def _():
            lg_ref[...], lu_ref[...] = sums.terms[slot, 0], sums.terms[slot, 1]

            def last(at):
                wide = h_ref[at, :].astype(F32)
                scale = _scale(wide)
                by_b = sum_s[at, :].astype(BF16).astype(F32)
                by = by_b * scale - wide * (scale * scale * scale) * jnp.mean(by_b * wide, -1, keepdims=True)
                dh_ref[at, :] = (by.astype(BF16).astype(F32) + by_ref[at, :].astype(F32)).astype(BF16)

            _tokens(tokens, last)

    half, full = pltpu.VMEM((tokens, d), BF16), pltpu.VMEM((tokens, d), F32)
    chunk, turned_ = pltpu.VMEM((tokens, CHUNK), BF16), pltpu.VMEM((d, tokens), BF16)
    outs = [_shape(h.shape), _shape(w_down.shape), *[_shape((d, CHUNK))] * 2, *[_shape((d // 8, (steps - 1) * CHUNK))] * 2]
    return _call(body, steps, [h, by_out, w_gate, w_up, w_down], [_whole(h), _whole(h), across, across, down],
                 outs, [_whole(h), down, *(_whole(a) for a in outs[2:])],
                 [half, turned_, turned_, full, chunk, chunk, chunk, *sums.scratch()], rider, given, number, 16 * tokens * d * w_gate.shape[1], "gated_bwd", True)


def finish(rider, given, others, number):
    n, ng = len(others), len(given)

    def squares(ref):
        rows, columns = ref.shape

        def some(t, total):
            g = ref[pl.ds(pl.multiple_of(t * 16, 16), 16), :].astype(F32)
            g = g * g
            g = g[:8, :] + g[8:, :]
            return total + sum(g[:, c : c + 128] for c in range(0, columns, 128))

        return lax.fori_loop(0, rows // 16, some, jnp.zeros((8, 128), F32))

    def kernel(*refs):
        other_refs, given_refs, refs = refs[:n], refs[n : n + ng], refs[n + ng :]
        out_refs, total_ref, refs = refs[:ng], refs[ng], refs[ng + 1 :]
        mine_s, all_s, send, recv = refs[:4]
        rider.bind(given_refs, out_refs, refs[4:])
        me = lax.axis_index("dp")
        barrier = pltpu.get_barrier_semaphore()
        for k in range(1, 8):
            pl.semaphore_signal(barrier, inc=1, device_id={"dp": lax.rem(me + k, 8)}, device_id_type=MESH)
        pl.semaphore_wait(barrier, 7)
        rider.begin()
        total = sum(squares(ref) for ref in other_refs)
        for act in (rider.part1, rider.part2, rider.end):
            act()
        mine_s[...] = total + sum(squares(ref) for ref in out_refs)

        def copy(k):
            return pltpu.make_async_remote_copy(mine_s, all_s.at[me], send.at[k], recv.at[k], device_id={"dp": lax.rem(me + k, 8)}, device_id_type=MESH)

        def arrived(k):
            place = all_s.at[lax.rem(me + 8 - k, 8)]
            return pltpu.make_async_remote_copy(place, place, send.at[k], recv.at[k], device_id={"dp": me}, device_id_type=MESH)

        for k in range(1, 8):
            copy(k).start()
        all_s[me] = mine_s[...]
        for k in range(1, 8):
            arrived(k).wait_recv()
        for k in range(1, 8):
            copy(k).wait_send()
        total_ref[...] = sum(all_s[k] for k in range(8))

    outs = [*rider.out_shape(), _shape((8, 128), F32)]
    got = pl.pallas_call(
        kernel,
        grid=(1,),
        in_specs=[*(_whole(a) for a in others), *rider.in_specs()],
        out_specs=[*rider.out_specs(), _whole(outs[-1])],
        out_shape=outs,
        scratch_shapes=[pltpu.VMEM((8, 128), F32), pltpu.VMEM((8, 8, 128), F32), pltpu.SemaphoreType.DMA((8,)), pltpu.SemaphoreType.DMA((8,)), *rider.scratch()],
        compiler_params=pltpu.CompilerParams(dimension_semantics=("arbitrary",), vmem_limit_bytes=VMEM, collective_id=number, has_side_effects=True),
        name="finish",
    )(*others, *given)
    return list(got[:-1]), got[-1]


def angles(tokens):
    half = HEAD // 2
    angle = jnp.arange(tokens, dtype=F32)[:, None] * THETA ** (-jnp.arange(half, dtype=F32) / half)
    return jnp.cos(angle), jnp.sin(angle)


def adamw(w, m, v, g):
    m = 0.9 * m + 0.1 * g
    v = 0.95 * v + 0.05 * g * g
    step = m * lax.rsqrt(v + 1e-8) + 0.1 * w
    return (w - 0.02 * step).astype(BF16), m, v


def clipped(gradients, sum_of_squares, count):
    factor = jnp.minimum(1.0, 0.5 * lax.rsqrt(sum_of_squares / count + 1e-30))
    return [g * factor for g in gradients]


def solution(mesh):
    def step(x, dy, *arrays):
        weights, m, v = (arrays[i : i + 7] for i in (0, 7, 14))
        shards = dict(zip(NAMES, weights, strict=True))
        blocks = {name: w.shape[1:] for name, w in shards.items()}
        given = lambda names: [shards[n] for n in names]
        h0, tokens = x[0], x.shape[1]
        tables = angles(tokens)

        w = [{}, {}]
        w[0] |= zip(ATT, alone(Gather(ATT, blocks, 0), given(ATT), 0))
        (mid0, *kept0), got = attend(h0, w[0], tables, Gather(MLP, blocks, 0), given(MLP), 1)
        w[0] |= zip(MLP, got)
        early = ATT + MLP[:2]
        (h1,), got = gated(mid0, *(w[0][n] for n in MLP), Gather(early, blocks, 1), given(early), 2)
        w[1] |= zip(early, got)
        (mid1, *kept1), got = attend(h1, w[1], tables, Gather(MLP[2:], blocks, 1), given(MLP[2:]), 3)
        w[1] |= zip(MLP[2:], got)

        by, g = [{}, {}], [{}, {}]
        first, last = ("first_gate", "first_up"), ("last_gate", "last_up")
        rest = ("w_down", *last)
        blocks |= {n: (blocks["w_up"][0], CHUNK) for n in last}
        (by_mid1, *got), _ = gated_bwd(mid1, dy[0], *(w[1][n] for n in MLP), number=4)
        by[1] |= zip(rest, got[:3])
        g[1] |= zip(first, got[3:])
        (*got, by_h1), sums = attend_bwd(h1, w[1], tables, kept1, by_mid1, True, Scatter(rest, blocks), [by[1][n] for n in rest], 5)
        by[1] |= zip(ATT, got)
        g[1] |= zip(rest, sums)
        (by_mid0, *got), sums = gated_bwd(mid0, by_h1, *(w[0][n] for n in MLP), Scatter(ATT, blocks), [by[1][n] for n in ATT], 6)
        by[0] |= zip(rest, got[:3])
        g[0] |= zip(first, got[3:])
        g[1] |= zip(ATT, sums)
        got, sums = attend_bwd(h0, w[0], tables, kept0, by_mid0, False, Scatter(rest, blocks), [by[0][n] for n in rest], 7)
        by[0] |= zip(ATT, got)
        g[0] |= zip(rest, sums)
        sums, squares = finish(Scatter(ATT, blocks), [by[0][n] for n in ATT], [*g[1].values(), *g[0].values()], 8)
        g[0] |= zip(ATT, sums)
        for of in g:
            of |= {n: jnp.concatenate([of[a], of[b]], 1) for n, a, b in zip(MLP, first, last)}

        gradients = [jnp.stack([g[0][n], g[1][n]]).astype(F32) for n in NAMES]
        gradients = clipped(gradients, jnp.sum(squares), 8 * sum(g.size for g in gradients))
        new = [adamw(w.astype(F32), m, v, g) for w, m, v, g in zip(weights, m, v, gradients, strict=True)]
        return tuple(one[which] for which in range(3) for one in new)

    states, cut = P(("rep", "dp"), None, None), P(None, "dp", None)
    return jax.shard_map(
        step,
        mesh=mesh,
        in_specs=(states, states) + (cut,) * 21,
        out_specs=(P("rep", "dp", None),) * 21,
        check_vma=False,
    )
```

```python
import functools

import jax
import jax.numpy as jnp
import numpy as np
from jax import lax
from jax.experimental import pallas as pl
from jax.experimental.pallas import tpu as pltpu
from jax.sharding import PartitionSpec as P

HEAD = 256
THETA = 10000
NAMES = ("wq", "wk", "wv", "wo", "w_gate", "w_up", "w_down")
ATT, MLP = NAMES[:4], NAMES[4:]
NEG = -1e30
HIDDEN = 2 * NEG
LOG2E = 1.4426950408889634
VMEM = 62 * 2**20
BLOCK = 512
CHUNK = 512
ROWS = 512
ANY = pl.BlockSpec(memory_space=pl.ANY)
MESH = pl.DeviceIdType.MESH
F32, BF16 = jnp.float32, jnp.bfloat16


def _dot(a, b, ca, cb):
    return lax.dot_general(a, b, (((ca,), (cb,)), ((), ())), preferred_element_type=F32)


def _units(names, blocks):
    cut = []
    for name in names:
        rows, columns = blocks[name]
        if name in ("wo", "w_down"):
            cut += [(name, 0, rows // 2, 0), (name, rows // 2, rows // 2, 1)]
        else:
            cut += [(name, 0, rows, 0 if name in ("wq", "w_gate", "last_gate") else 1)]
    return cut


def _around(way):
    me = lax.axis_index("dp")
    core, y, x = lax.rem(me, 2), lax.rem(lax.div(me, 2), 2), lax.div(me, 4)
    over_x, over_y = 4 - 8 * x, 2 - 4 * y
    first, second = (over_x, over_y) if way == 0 else (over_y, over_x)
    return me, 1 - 2 * core, first, second, over_x + over_y


def _meet():
    me, other, first, second, _ = _around(0)
    barrier = pltpu.get_barrier_semaphore()
    for way in (other, first, second):
        pl.semaphore_signal(barrier, inc=1, device_id={"dp": me + way}, device_id_type=MESH)
    pl.semaphore_wait(barrier, 3)


class Gather:
    def __init__(self, names, blocks, layer):
        self.names, self.blocks, self.layer = names, blocks, layer
        self.units = _units(names, blocks)

    def in_specs(self):
        return [ANY] * len(self.names)

    def out_specs(self):
        return [ANY] * len(self.names)

    def out_shape(self):
        return [jax.ShapeDtypeStruct((8 * self.blocks[n][0], self.blocks[n][1]), BF16) for n in self.names]

    def scratch(self):
        n = len(self.units)
        return [pltpu.SemaphoreType.DMA((n,)), pltpu.SemaphoreType.DMA((n, 7)), pltpu.SemaphoreType.DMA((n, 7))]

    def bind(self, ins, outs, scratch):
        self.shards, self.whole = dict(zip(self.names, ins)), dict(zip(self.names, outs))
        self.local, self.send, self.recv = scratch

    def _piece(self, unit, device):
        name, at, rows, _ = unit
        return self.whole[name].at[pl.ds(pl.multiple_of(device * self.blocks[name][0] + at, 16), rows)]

    def _copy(self, i, slot, arrived=False):
        unit = self.units[i]
        name, at, rows, way = unit
        me, other, first, second, across = _around(way)
        own = self.shards[name].at[self.layer, pl.ds(at, rows)]
        source, owner, to, comes = (
            (own, me, first, me + first),
            (own, me, second, me + second),
            (own, me, other, me + other),
            (None, me + first, second, me + across),
            (None, me + first, other, me + first + other),
            (None, me + second, other, me + second + other),
            (None, me + across, other, me + across + other),
        )[slot]
        if arrived:
            source, owner = None, comes
        target = self._piece(unit, owner)
        return pltpu.make_async_remote_copy(target if source is None else source, target, self.send.at[i, slot], self.recv.at[i, slot],
                                            device_id={"dp": me + to}, device_id_type=MESH)

    def _mine(self, i):
        name, at, rows, way = self.units[i]
        return pltpu.make_async_copy(self.shards[name].at[self.layer, pl.ds(at, rows)], self._piece(self.units[i], lax.axis_index("dp")), self.local.at[i])

    def begin(self):
        for i in range(len(self.units)):
            for slot in range(3):
                self._copy(i, slot).start()
            self._mine(i).start()

    def middle(self):
        for i in range(len(self.units)):
            self._copy(i, 0, True).wait_recv()
            self._copy(i, 3).start()
            self._copy(i, 4).start()
            self._copy(i, 1, True).wait_recv()
            self._copy(i, 5).start()

    def end(self):
        for i in range(len(self.units)):
            self._copy(i, 3, True).wait_recv()
            self._copy(i, 6).start()
        for i in range(len(self.units)):
            for slot in (2, 4, 5, 6):
                self._copy(i, slot, True).wait_recv()
            for slot in range(7):
                self._copy(i, slot).wait_send()
            self._mine(i).wait()

    def actions(self, steps):
        if steps == 1:
            return {0: ([_meet, self.begin], [self.middle, self.end])}
        return {0: ([_meet, self.begin], []), steps - 1: ([self.middle], [self.end])}


class Scatter:
    def __init__(self, names, blocks):
        self.names, self.blocks = names, blocks
        self.units = _units(names, blocks)

    def in_specs(self):
        return [ANY] * len(self.names)

    def out_specs(self):
        return [pl.BlockSpec(self.blocks[n], lambda *_: (0, 0), pipeline_mode=pl.Buffered(1)) for n in self.names]

    def out_shape(self):
        return [jax.ShapeDtypeStruct(self.blocks[n], BF16) for n in self.names]

    def scratch(self):
        n, dma = len(self.units), pltpu.SemaphoreType.DMA
        found = [dma((n, 4)), dma((n, 4)), dma((n, 4)), dma((n, 2)), dma((n, 2)), dma((n,)), dma((n,))]
        for name, _, rows, _ in self.units:
            columns = self.blocks[name][1]
            found += [pltpu.VMEM((k, rows, columns), BF16) for k in (4, 4, 2, 2, 1, 1)]
        return found

    def bind(self, ins, outs, scratch):
        self.terms, self.outs = dict(zip(self.names, ins)), dict(zip(self.names, outs))
        self.load, self.send0, self.recv0, self.send1, self.recv1, self.send2, self.recv2 = scratch[:7]
        rest = scratch[7:]
        self.buffers = [rest[6 * i : 6 * i + 6] for i in range(len(self.units))]

    def _block(self, unit, device):
        name, at, rows, _ = unit
        return self.terms[name].at[pl.ds(pl.multiple_of(device * self.blocks[name][0] + at, 16), rows)]

    def _own(self, i, j):
        me, other, *ways = _around(self.units[i][3])
        return pltpu.make_async_copy(self._block(self.units[i], me + ([0] + ways)[j]), self.buffers[i][0].at[j], self.load.at[i, j])

    def _across(self, i, j):
        me, other, *ways = _around(self.units[i][3])
        return pltpu.make_async_remote_copy(self._block(self.units[i], me + other + ([0] + ways)[j]), self.buffers[i][1].at[j], self.send0.at[i, j],
                                            self.recv0.at[i, j], device_id={"dp": me + other}, device_id_type=MESH)

    def _first(self, i, j):
        me, _, first, _, _ = _around(self.units[i][3])
        return pltpu.make_async_remote_copy(self.buffers[i][2].at[j], self.buffers[i][3].at[j], self.send1.at[i, j], self.recv1.at[i, j],
                                            device_id={"dp": me + first}, device_id_type=MESH)

    def _second(self, i):
        me, _, _, second, _ = _around(self.units[i][3])
        return pltpu.make_async_remote_copy(self.buffers[i][4].at[0], self.buffers[i][5].at[0], self.send2.at[i], self.recv2.at[i],
                                            device_id={"dp": me + second}, device_id_type=MESH)

    def begin(self):
        for js in ((1, 3), (2, 0)):
            for i in range(len(self.units)):
                for j in js:
                    self._across(i, j).start()
                    self._own(i, j).start()

    def _ready(self, i, j):
        self._own(i, j).wait()
        self._across(i, j).wait_recv()

    def _add(self, rows, store, *terms):
        def some(t, _):
            at = pl.ds(pl.multiple_of(t * 16, 16), 16)
            store(at, sum(term[at, :].astype(F32) for term in terms))
            return 0

        lax.fori_loop(0, rows // 16, some, 0)

    def part1(self):
        for i, (_, _, rows, _) in enumerate(self.units):
            own, came, out = self.buffers[i][:3]
            for j, k in ((1, 0), (3, 1)):
                self._ready(i, j)

                def store(at, value, k=k, out=out):
                    out[k, at, :] = value.astype(BF16)

                self._add(rows, store, own.at[j], came.at[j])
            for i in ([i - 1] if i else []) + ([i] if i == len(self.units) - 1 else []):
                self._first(i, 0).start()
                self._first(i, 1).start()

    def part2(self):
        for i, (_, _, rows, _) in enumerate(self.units):
            own, came, _, got, out, _ = self.buffers[i]
            self._ready(i, 2)
            self._first(i, 0).wait_recv()
            self._first(i, 1).wait_recv()

            def store(at, value, out=out):
                out[0, at, :] = value.astype(BF16)

            self._add(rows, store, own.at[2], came.at[2], got.at[1])
            for i in ([i - 1] if i else []) + ([i] if i == len(self.units) - 1 else []):
                self._second(i).start()

    def end(self):
        for i, (name, start, rows, _) in enumerate(self.units):
            own, came, _, got, _, last = self.buffers[i]
            self._ready(i, 0)
            self._second(i).wait_recv()

            def store(at, value, name=name, start=start):
                self.outs[name][pl.ds(pl.multiple_of(start + at.start, 16), 16), :] = value.astype(BF16)

            self._add(rows, store, own.at[0], came.at[0], got.at[0], last.at[0])
        for i in range(len(self.units)):
            for j in range(4):
                self._across(i, j).wait_send()
            for j in range(2):
                self._first(i, j).wait_send()
            self._second(i).wait_send()

    def actions(self, steps):
        if steps == 8:
            return {0: ([_meet, self.begin], []), 4: ([self.part1], []), 7: ([self.part2], [self.end])}
        return {0: ([_meet, self.begin], []), 1: ([self.part1], []), steps - 2: ([self.part2], []), steps - 1: ([], [self.end])}


class Chunks:
    def __init__(self, rows, chunks):
        self.rows, self.n = rows, chunks - 1

    def scratch(self):
        n, rows, dma = self.n, self.rows, pltpu.SemaphoreType.DMA
        sems = [dma((n, 2, 4)), dma((n, 2, 4)), dma((n, 2, 2)), dma((n, 2, 2)), dma((n, 2)), dma((n, 2))]
        block = lambda *lead: pltpu.VMEM((*lead, rows, CHUNK), BF16)
        return [*sems, pltpu.VMEM((2, 2, 8 * rows, CHUNK), BF16), block(n, 2, 4), block(n, 2, 2), block(n, 2, 2), block(n, 2), block(n, 2)]

    def bind(self, outs, scratch):
        self.outs = outs
        self.send0, self.recv0, self.send1, self.recv1, self.send2, self.recv2, self.terms, self.came, self.sum1, self.got1, self.sum2, self.got2 = scratch

    def _block(self, j, u, device):
        return self.terms.at[lax.rem(j, 2), u, pl.ds(pl.multiple_of(device * self.rows, 16), self.rows)]

    def _own(self, j, u, k):
        me, _, *ways = _around(u)
        return self._block(j, u, me + ([0] + ways)[k])[...].astype(F32) + self.came[j, u, k].astype(F32)

    def _across(self, j, u, k):
        me, other, *ways = _around(u)
        return pltpu.make_async_remote_copy(self._block(j, u, me + other + ([0] + ways)[k]), self.came.at[j, u, k], self.send0.at[j, u, k],
                                            self.recv0.at[j, u, k], device_id={"dp": me + other}, device_id_type=MESH)

    def _first(self, j, u, k):
        me, _, first, _, _ = _around(u)
        return pltpu.make_async_remote_copy(self.sum1.at[j, u, k], self.got1.at[j, u, k], self.send1.at[j, u, k], self.recv1.at[j, u, k],
                                            device_id={"dp": me + first}, device_id_type=MESH)

    def _second(self, j, u):
        me, _, _, second, _ = _around(u)
        return pltpu.make_async_remote_copy(self.sum2.at[j, u], self.got2.at[j, u], self.send2.at[j, u], self.recv2.at[j, u],
                                            device_id={"dp": me + second}, device_id_type=MESH)

    def part0(self, j):
        for u in range(2):
            for k in (1, 3, 2, 0):
                self._across(j, u, k).start()

    def part1(self, j):
        for u in range(2):
            for k, at in ((1, 0), (3, 1)):
                self._across(j, u, k).wait_recv()
                self.sum1[j, u, at] = self._own(j, u, k).astype(BF16)

    def part2(self, j):
        for u in range(2):
            for k in range(2):
                self._first(j, u, k).start()

    def part3(self, j):
        for u in range(2):
            self._across(j, u, 2).wait_recv()
            for k in range(2):
                self._first(j, u, k).wait_recv()
            self.sum2[j, u] = (self._own(j, u, 2) + self.got1[j, u, 1].astype(F32)).astype(BF16)

    def part4(self, j):
        for u in range(2):
            self._second(j, u).start()

    def end(self, j):
        for u in range(2):
            self._across(j, u, 0).wait_recv()
            self._second(j, u).wait_recv()
            total = self._own(j, u, 0) + self.got1[j, u, 0].astype(F32) + self.got2[j, u].astype(F32)
            self.outs[u][:, pl.ds(pl.multiple_of(j * CHUNK, CHUNK), CHUNK)] = total.astype(BF16)
        for u in range(2):
            for k in range(4):
                self._across(j, u, k).wait_send()
            for k in range(2):
                self._first(j, u, k).wait_send()
            self._second(j, u).wait_send()


def _call(body, steps, ins, in_specs, outs, out_specs, scratch, rider=None, given=(), number=0, flops=0, name=None, meet=False):
    ni, no, ns = len(in_specs), len(out_specs), len(scratch)
    more_in, more_out, more_specs, more_scratch = ([], [], [], []) if rider is None else (rider.in_specs(), rider.out_shape(), rider.out_specs(), rider.scratch())

    def kernel(*refs):
        cuts = [ni, len(more_in), no, len(more_out), ns, len(more_scratch)]
        parts, at = [], 0
        for n in cuts:
            parts.append(refs[at : at + n])
            at += n
        step = pl.program_id(0)
        acts = {}
        if rider is not None:
            rider.bind(parts[1], parts[3], parts[5])
            acts = rider.actions(steps)
        elif meet:
            acts = {0: ([_meet], [])}

        def run(which):
            for s, lists in acts.items():
                if lists[which]:
                    if steps == 1:
                        for act in lists[which]:
                            act()
                    else:

                        @pl.when(step == s)
                        def _(todo=lists[which]):
                            for act in todo:
                                act()

        run(0)
        body(step, parts[0], parts[2], parts[4])
        run(1)

    params = dict(dimension_semantics=("arbitrary",), vmem_limit_bytes=VMEM)
    if rider is not None or meet:
        params |= dict(collective_id=number, has_side_effects=True)
    got = pl.pallas_call(
        kernel,
        grid=(steps,),
        in_specs=[*in_specs, *more_in],
        out_specs=[*out_specs, *more_specs],
        out_shape=[*outs, *more_out],
        scratch_shapes=[*scratch, *more_scratch],
        compiler_params=pltpu.CompilerParams(**params),
        cost_estimate=pl.CostEstimate(flops=int(flops) + 1, bytes_accessed=10**6, transcendentals=0),
        name=name,
    )(*ins, *given)
    return list(got[:no]), list(got[no:])


def _whole(a):
    return pl.BlockSpec(a.shape, lambda *_: (0,) * len(a.shape), pipeline_mode=pl.Buffered(1))


def _shape(shape, dtype=BF16):
    return jax.ShapeDtypeStruct(shape, dtype)


def first(tokens, rider, given, number):
    half = HEAD // 2
    speed = jnp.asarray(THETA ** (-np.arange(half) / half), F32)[None]

    def body(step, ins, outs, scratch):
        def some(t, _):
            at = pl.ds(pl.multiple_of(t * 256, 256), 256)
            angle = (lax.broadcasted_iota(jnp.int32, (256, half), 0) + t * 256).astype(F32) * ins[0][...]
            outs[0][at, :], outs[1][at, :] = jnp.cos(angle), jnp.sin(angle)
            return 0

        lax.fori_loop(0, tokens // 256, some, 0)

    outs = [_shape((tokens, half), F32)] * 2
    return _call(body, 1, [speed], [_whole(speed)], outs, [_whole(a) for a in outs], [], rider, given, number, name="first")


def _hidden():
    return lax.broadcasted_iota(jnp.int32, (BLOCK, BLOCK), 0) > lax.broadcasted_iota(jnp.int32, (BLOCK, BLOCK), 1)


def _strip(ref, head, a):
    return ref[a * BLOCK : (a + 1) * BLOCK, head * HEAD : (head + 1) * HEAD]


def _turn(t, cos, sin):
    half, parts = HEAD // 2, []
    for at in range(0, t.shape[1], HEAD):
        a, b = t[:, at : at + half].astype(F32), t[:, at + half : at + HEAD].astype(F32)
        parts += [a * cos - b * sin, b * cos + a * sin]
    return jnp.concatenate(parts, -1).astype(BF16)


def attend(h, w, tables, rider=None, given=(), number=0):
    wq, wk, wv, wo = (w[n] for n in ATT)
    tokens, heads = h.shape[0], wq.shape[1] // HEAD
    blocks, scale = tokens // BLOCK, HEAD**-0.5
    e = scale * LOG2E

    def body(step, ins, outs, scratch):
        h_ref, wq_ref, wk_ref, wv_ref, wo_ref, cos_ref, sin_ref = ins
        mid_ref, q_ref, k_ref, v_ref, o_ref, lse_ref = outs
        top_s, mix_s = scratch

        @pl.when(step < blocks)
        def _():
            at = pl.ds(pl.multiple_of(step * BLOCK, BLOCK), BLOCK)
            wide = h_ref[at, :].astype(F32)
            a = (wide * _scale(wide)).astype(BF16)
            cos, sin = cos_ref[at, :], sin_ref[at, :]
            q_ref[at, :] = _turn(_dot(a, wq_ref[...], 1, 0).astype(BF16), cos, sin)
            k_ref[at, :] = _turn(_dot(a, wk_ref[...], 1, 0).astype(BF16), cos, sin)
            v_ref[at, :] = _dot(a, wv_ref[...], 1, 0).astype(BF16)

        def block(j):
            strips = [(n, a) for a in range(j, blocks) for n in range(heads)]
            here = slice(j * BLOCK, (j + 1) * BLOCK)
            keys = k_ref[here, :]
            values = jnp.concatenate([v_ref[here, :].T, jnp.ones((8, BLOCK), BF16)], axis=0)
            scores = [_dot(keys, _strip(q_ref, n, a), 1, 1) for n, a in strips]
            weights, keeps = [], []
            for (n, a), s in zip(strips, scores):
                i = a * heads + n
                if a == j:
                    s = jnp.where(_hidden(), HIDDEN, s)
                top = s.max(axis=0, keepdims=True)
                if j:
                    old = top_s[i : i + 1, :]
                    top = jnp.maximum(old, top)
                    keeps.append(jnp.exp2((old - top) * e))
                else:
                    keeps.append(None)
                top_s[i : i + 1, :] = top
                weights.append(jnp.exp2((s - top) * e).astype(BF16))
            done = []
            for (n, a), p, keep in zip(strips, weights, keeps):
                i = a * heads + n
                mix = _dot(values, p, 1, 0)
                if j:
                    mix = mix_s[i] * keep + mix
                if a > j:
                    mix_s[i] = mix
                else:
                    total = mix[HEAD : HEAD + 1, :]
                    done.append((mix[:HEAD, :] * (1 / total)).T.astype(BF16))
                    o_ref[here, n * HEAD : (n + 1) * HEAD] = done[-1]
                    lse_ref[i : i + 1, :] = top_s[i : i + 1, :] * scale + jnp.log(total)
            out = _dot(jnp.concatenate(done, -1), wo_ref[...], 1, 0).astype(BF16).astype(F32)
            mid_ref[here, :] = (h_ref[here, :].astype(F32) + out).astype(BF16)

        for j in range(blocks):
            pl.when(step == blocks + j)(functools.partial(block, j))

    n = heads * blocks
    ins = [h, wq, wk, wv, wo, *tables]
    outs = [_shape(h.shape), _shape((tokens, heads * HEAD)), _shape((tokens, HEAD)), _shape((tokens, HEAD)), _shape((tokens, heads * HEAD)), _shape((n, BLOCK), F32)]
    flops = 2 * tokens * (h.shape[1] * 1536 + 1.2 * tokens * heads * HEAD)
    return _call(body, 2 * blocks, ins, [_whole(a) for a in ins], outs, [_whole(a) for a in outs],
                 [pltpu.VMEM((n, BLOCK), F32), pltpu.VMEM((n, HEAD + 8, BLOCK), F32)], rider, given, number, flops, "attend")


def attend_bwd(h, w, tables, kept, by_mid, wanted, rider=None, given=(), number=0):
    q, k, v, o, lse = kept
    wq, wk, wv, wo = (w[n] for n in ATT)
    (tokens, d), heads = h.shape, wq.shape[1] // HEAD
    blocks, scale = tokens // BLOCK, HEAD**-0.5
    e = scale * LOG2E

    def body(step, ins, outs, scratch):
        h_ref, wq_ref, wk_ref, wv_ref, wo_ref, cos_ref, sin_ref, q_ref, k_ref, v_ref, o_ref, lse_ref, by_ref = ins
        dwq_ref, dwk_ref, dwv_ref, dwo_ref, *dh_ref = outs
        dq_s, do_s, delta_s, dwq_s, dwk_s, dwv_s, dwo_s = scratch

        def before(t):
            here = slice(t * BLOCK, (t + 1) * BLOCK)
            by, o = by_ref[here, :], o_ref[here, :]
            do = _dot(by, wo_ref[...], 1, 1).astype(BF16)
            do_s[here, :] = do
            dots = (do.astype(F32) * o.astype(F32)).T
            for n in range(heads):
                i = t * heads + n
                delta_s[i : i + 1, :] = dots[n * HEAD : (n + 1) * HEAD, :].sum(axis=0, keepdims=True)
            term = _dot(o.T, by, 1, 0)
            if t:
                term = dwo_s[...] + term
            if t < blocks - 1:
                dwo_s[...] = term
            else:
                dwo_ref[...] = term.astype(BF16)

        def block(j):
            here = slice(j * BLOCK, (j + 1) * BLOCK)
            strips = [(n, a) for a in range(j, blocks) for n in range(heads)]
            keys, values = k_ref[here, :], v_ref[here, :]
            turned_keys = keys.T
            dk = dv = None
            dq = []
            scores = [_dot(keys, _strip(q_ref, n, a), 1, 1) for n, a in strips]
            dps = [_dot(values, _strip(do_s, n, a), 1, 1) for n, a in strips]
            for (n, a), s, dp in zip(strips, scores, dps):
                i = a * heads + n
                p = jnp.exp2(s * e - lse_ref[i : i + 1, :] * LOG2E)
                if a == j:
                    p = jnp.where(_hidden(), 0.0, p)
                ds = (p * (dp - delta_s[i : i + 1, :])).astype(BF16)
                by_v = _dot(p.astype(BF16), _strip(do_s, n, a), 1, 0)
                by_k = _dot(ds, _strip(q_ref, n, a), 1, 0)
                dv, dk = (by_v, by_k) if dv is None else (dv + by_v, dk + by_k)
                by_q = _dot(turned_keys, ds, 1, 0)
                if j:
                    by_q = dq_s[i] + by_q
                if a > j:
                    dq_s[i] = by_q
                else:
                    dq.append((by_q * scale).T.astype(BF16))
            cos, sin = cos_ref[here, :], -sin_ref[here, :]
            dq = _turn(jnp.concatenate(dq, -1), cos, sin)
            dk = _turn((dk * scale).astype(BF16), cos, sin)
            dv = dv.astype(BF16)
            wide = h_ref[here, :].astype(F32)
            size = _scale(wide)
            at = (wide * size).astype(BF16).T
            for by, sum_s, out_ref in ((dq, dwq_s, dwq_ref), (dk, dwk_s, dwk_ref), (dv, dwv_s, dwv_ref)):
                term = _dot(at, by, 1, 0)
                if j:
                    term = sum_s[...] + term
                if j < blocks - 1:
                    sum_s[...] = term
                else:
                    out_ref[...] = term.astype(BF16)
            if wanted:
                by_a = (_dot(dv, wv_ref[...], 1, 1).astype(BF16).astype(F32) + _dot(dk, wk_ref[...], 1, 1).astype(BF16).astype(F32)
                        + _dot(dq, wq_ref[...], 1, 1).astype(BF16).astype(F32)).astype(BF16).astype(F32)
                by_h = by_a * size - wide * (size * size * size) * jnp.mean(by_a * wide, -1, keepdims=True)
                dh_ref[0][here, :] = (by_h.astype(BF16).astype(F32) + by_ref[here, :].astype(F32)).astype(BF16)

        for t in range(blocks):
            pl.when(step == t)(functools.partial(before, t))
            pl.when(step == blocks + t)(functools.partial(block, t))

    ins = [h, wq, wk, wv, wo, *tables, q, k, v, o, lse, by_mid]
    outs = [_shape(a.shape) for a in (wq, wk, wv, wo) + ((h,) if wanted else ())]
    n = heads * blocks
    full = lambda a: pltpu.VMEM(a.shape, F32)
    flops = 4 * tokens * (d * 1536 + 1.5 * tokens * heads * HEAD)
    return _call(body, 2 * blocks, ins, [_whole(a) for a in ins], outs, [_whole(a) for a in outs],
                 [pltpu.VMEM((n, HEAD, BLOCK), F32), pltpu.VMEM(o.shape, BF16), pltpu.VMEM((n, BLOCK), F32), full(wq), full(wk), full(wv), full(wo)],
                 rider, given, number, flops, "attend_bwd")


def _scale(wide):
    return lax.rsqrt(jnp.mean(wide * wide, -1, keepdims=True) + 1e-6)


def _tokens(n, do):
    def some(t, _):
        do(pl.ds(pl.multiple_of(t * ROWS, ROWS), ROWS))
        return 0

    lax.fori_loop(0, n // ROWS, some, 0)


def _chunks(w_gate, w_down):
    across = pl.BlockSpec((w_gate.shape[0], CHUNK), lambda j: (0, j))
    down = pl.BlockSpec((CHUNK, w_down.shape[1]), lambda j: (j, 0))
    return across, down


def gated(h, w_gate, w_up, w_down, rider=None, given=(), number=0):
    tokens, d = h.shape
    steps = w_gate.shape[1] // CHUNK
    across, down = _chunks(w_gate, w_down)

    def body(step, ins, outs, scratch):
        h_ref, g_ref, u_ref, d_ref = ins
        o_ref, gate_ref, up_ref = outs
        b_s, sum_s = scratch

        @pl.when(step == 0)
        def _():
            def norm(at):
                wide = h_ref[at, :].astype(F32)
                b_s[at, :] = (wide * _scale(wide)).astype(BF16)
                sum_s[at, :] = jnp.zeros((ROWS, d), F32)

            _tokens(tokens, norm)

        def some(at):
            b = b_s[at, :]
            gate, up = _dot(b, g_ref[...], 1, 0), _dot(b, u_ref[...], 1, 0)
            gate_ref[0, at, :], up_ref[0, at, :] = gate, up
            act = (gate * (1 / (1 + jnp.exp(-gate))) * up).astype(BF16)
            sum_s[at, :] += _dot(act, d_ref[...], 1, 0)

        _tokens(tokens, some)

        @pl.when(step == steps - 1)
        def _():
            def last(at):
                o_ref[at, :] = (h_ref[at, :].astype(F32) + sum_s[at, :].astype(BF16).astype(F32)).astype(BF16)

            _tokens(tokens, last)

    keep = pl.BlockSpec((1, tokens, CHUNK), lambda j: (j, 0, 0))
    kept = _shape((steps, tokens, CHUNK), F32)
    return _call(body, steps, [h, w_gate, w_up, w_down], [_whole(h), across, across, down], [_shape(h.shape), kept, kept], [_whole(h), keep, keep],
                 [pltpu.VMEM((tokens, d), BF16), pltpu.VMEM((tokens, d), F32)], rider, given, number, 6 * tokens * d * w_gate.shape[1], "gated")


def gated_bwd(h, by_out, w_gate, w_up, w_down, kept=(), rider=None, given=(), number=0):
    tokens, d = h.shape
    steps = w_gate.shape[1] // CHUNK
    across, down = _chunks(w_gate, w_down)
    sums, inner = Chunks(d // 8, steps), tokens // ROWS

    def body(step, ins, outs, scratch):
        h_ref, by_ref, g_ref, u_ref, d_ref, *kept_refs = ins
        dh_ref, dd_ref, lg_ref, lu_ref, *sum_refs = outs
        bt_s, byt_s, sum_s, act_s, gate_s, up_s = scratch[:6]
        sums.bind(sum_refs, scratch[8:])
        if kept:
            tile_s, sem = scratch[6:8]
        else:
            b_s = scratch[6]

        def tiles(i):
            at = pl.ds(pl.multiple_of(lax.rem(i, inner) * ROWS, ROWS), ROWS)
            slot = lax.rem(i, 2)
            return [pltpu.make_async_copy(ref.at[lax.div(i, inner), at], tile_s.at[slot, k], sem.at[slot, k]) for k, ref in enumerate(kept_refs)]

        if kept:

            @pl.when(step == 0)
            def _():
                for copy in tiles(0):
                    copy.start()

        @pl.when(step > 0)
        def _():
            sums.part0(step - 1)

        @pl.when(step == 0)
        def _():
            def norm(at):
                wide = h_ref[at, :].astype(F32)
                b = (wide * _scale(wide)).astype(BF16)
                if not kept:
                    b_s[at, :] = b
                bt_s[:, at] = b.T
                byt_s[:, at] = by_ref[at, :].T
                sum_s[at, :] = jnp.zeros((ROWS, d), F32)

            _tokens(tokens, norm)

        def some(t, _):
            for when, part in ((1, sums.part1), (2, sums.part2)):
                pl.when((t == when) & (step > 0))(lambda part=part: part(step - 1))
            at = pl.ds(pl.multiple_of(t * ROWS, ROWS), ROWS)
            by = by_ref[at, :]
            if kept:
                i = step * inner + t

                @pl.when(i + 1 < steps * inner)
                def _():
                    for copy in tiles(i + 1):
                        copy.start()

                for copy in tiles(i):
                    copy.wait()
                gate, up = tile_s[lax.rem(i, 2), 0], tile_s[lax.rem(i, 2), 1]
            else:
                b = b_s[at, :]
                gate, up = _dot(b, g_ref[...], 1, 0), _dot(b, u_ref[...], 1, 0)
            by_act = _dot(by, d_ref[...], 1, 1).astype(BF16).astype(F32)
            open_ = 1 / (1 + jnp.exp(-gate))
            silu = gate * open_
            act_s[at, :] = (silu * up).astype(BF16)
            by_up = (by_act * silu).astype(BF16)
            by_gate = (by_act * up * (open_ + silu * (1 - open_))).astype(BF16)
            gate_s[at, :] = by_gate
            up_s[at, :] = by_up
            sum_s[at, :] += _dot(by_gate, g_ref[...], 1, 1) + _dot(by_up, u_ref[...], 1, 1)
            return 0

        lax.fori_loop(0, inner, some, 0)
        pl.when(step > 0)(lambda: sums.part3(step - 1))
        slot = lax.rem(step, 2)
        sums.terms[slot, 0] = _dot(bt_s[...], gate_s[...], 1, 0).astype(BF16)
        pl.when(step > 0)(lambda: sums.part4(step - 1))
        sums.terms[slot, 1] = _dot(bt_s[...], up_s[...], 1, 0).astype(BF16)
        dd_ref[...] = _dot(byt_s[...], act_s[...], 1, 0).astype(BF16).T
        pl.when(step > 0)(lambda: sums.end(step - 1))

        @pl.when(step == steps - 1)
        def _():
            lg_ref[...], lu_ref[...] = sums.terms[slot, 0], sums.terms[slot, 1]

            def last(at):
                wide = h_ref[at, :].astype(F32)
                scale = _scale(wide)
                by_b = sum_s[at, :].astype(BF16).astype(F32)
                by = by_b * scale - wide * (scale * scale * scale) * jnp.mean(by_b * wide, -1, keepdims=True)
                dh_ref[at, :] = (by.astype(BF16).astype(F32) + by_ref[at, :].astype(F32)).astype(BF16)

            _tokens(tokens, last)

    half, full = pltpu.VMEM((tokens, d), BF16), pltpu.VMEM((tokens, d), F32)
    chunk, turned_ = pltpu.VMEM((tokens, CHUNK), BF16), pltpu.VMEM((d, tokens), BF16)
    outs = [_shape(h.shape), _shape(w_down.shape), *[_shape((d, CHUNK))] * 2, *[_shape((d // 8, (steps - 1) * CHUNK))] * 2]
    more = [pltpu.VMEM((2, 2, ROWS, CHUNK), F32), pltpu.SemaphoreType.DMA((2, 2))] if kept else [half, pltpu.SemaphoreType.DMA((1,))]
    return _call(body, steps, [h, by_out, w_gate, w_up, w_down, *kept], [_whole(h), _whole(h), across, across, down, *[ANY] * len(kept)],
                 outs, [_whole(h), down, *(_whole(a) for a in outs[2:])], [turned_, turned_, full, chunk, chunk, chunk, *more, *sums.scratch()],
                 rider, given, number, (12 if kept else 16) * tokens * d * w_gate.shape[1], "gated_bwd", True)


def finish(rider, given, others, number):
    n, ng = len(others), len(given)

    def squares(ref):
        rows, columns = ref.shape

        def some(t, total):
            g = ref[pl.ds(pl.multiple_of(t * 16, 16), 16), :].astype(F32)
            g = g * g
            g = g[:8, :] + g[8:, :]
            return total + sum(g[:, c : c + 128] for c in range(0, columns, 128))

        return lax.fori_loop(0, rows // 16, some, jnp.zeros((8, 128), F32))

    def kernel(*refs):
        other_refs, given_refs, refs = refs[:n], refs[n : n + ng], refs[n + ng :]
        out_refs, total_ref, refs = refs[:ng], refs[ng], refs[ng + 1 :]
        mine_s, all_s, send, recv = refs[:4]
        rider.bind(given_refs, out_refs, refs[4:])
        me = lax.axis_index("dp")
        barrier = pltpu.get_barrier_semaphore()
        for k in range(1, 8):
            pl.semaphore_signal(barrier, inc=1, device_id={"dp": lax.rem(me + k, 8)}, device_id_type=MESH)
        pl.semaphore_wait(barrier, 7)
        rider.begin()
        total = sum(squares(ref) for ref in other_refs)
        for act in (rider.part1, rider.part2, rider.end):
            act()
        mine_s[...] = total + sum(squares(ref) for ref in out_refs)

        def copy(k):
            return pltpu.make_async_remote_copy(mine_s, all_s.at[me], send.at[k], recv.at[k], device_id={"dp": lax.rem(me + k, 8)}, device_id_type=MESH)

        def arrived(k):
            place = all_s.at[lax.rem(me + 8 - k, 8)]
            return pltpu.make_async_remote_copy(place, place, send.at[k], recv.at[k], device_id={"dp": me}, device_id_type=MESH)

        for k in range(1, 8):
            copy(k).start()
        all_s[me] = mine_s[...]
        for k in range(1, 8):
            arrived(k).wait_recv()
        for k in range(1, 8):
            copy(k).wait_send()
        total_ref[...] = sum(all_s[k] for k in range(8))

    outs = [*rider.out_shape(), _shape((8, 128), F32)]
    got = pl.pallas_call(
        kernel,
        grid=(1,),
        in_specs=[*(_whole(a) for a in others), *rider.in_specs()],
        out_specs=[*rider.out_specs(), _whole(outs[-1])],
        out_shape=outs,
        scratch_shapes=[pltpu.VMEM((8, 128), F32), pltpu.VMEM((8, 8, 128), F32), pltpu.SemaphoreType.DMA((8,)), pltpu.SemaphoreType.DMA((8,)), *rider.scratch()],
        compiler_params=pltpu.CompilerParams(dimension_semantics=("arbitrary",), vmem_limit_bytes=VMEM, collective_id=number, has_side_effects=True),
        name="finish",
    )(*others, *given)
    return list(got[:-1]), got[-1]


def adamw(w, m, v, g):
    m = 0.9 * m + 0.1 * g
    v = 0.95 * v + 0.05 * g * g
    step = m * lax.rsqrt(v + 1e-8) + 0.1 * w
    return (w - 0.02 * step).astype(BF16), m, v


def update(weights, m, v, g, squares):
    parts = {"w_gate": ("first_gate", "last_gate"), "w_up": ("first_up", "last_up")}
    pieces = [p for n in NAMES for p in parts.get(n, (n,))]
    layers, count = weights[0].shape[0], 8 * sum(w.size for w in weights)

    def kernel(*refs):
        refs = list(refs)
        take = lambda n: [refs.pop(0) for _ in range(n)]
        square_ref, w_refs, m_refs, v_refs = take(1)[0], take(7), take(7), take(7)
        g_refs = [dict(zip(pieces, take(len(pieces)))) for _ in range(layers)]
        outs = take(7), take(7), take(7)
        total = square_ref[...].sum(axis=0, keepdims=True).sum(axis=1, keepdims=True)
        factor = jnp.minimum(1.0, 0.5 * lax.rsqrt(total / count + 1e-30))

        def one(layer):
            for i, name in enumerate(NAMES):
                left = 0
                for piece in parts.get(name, (name,)):
                    g_ref = g_refs[layer][piece]
                    rows, columns = g_ref.shape

                    def some(t, _):
                        at = pl.ds(pl.multiple_of(t * 16, 16), 16)
                        for c in range(0, columns, 256):
                            wide = min(256, columns - c)
                            there = slice(left + c, left + c + wide)
                            got = adamw(w_refs[i][0, at, there].astype(F32), m_refs[i][0, at, there], v_refs[i][0, at, there],
                                        g_ref[at, c : c + wide].astype(F32) * factor)
                            for out, value in zip(outs, got):
                                out[i][0, at, there] = value
                        return 0

                    lax.fori_loop(0, rows // 16, some, 0)
                    left += columns

        for layer in range(layers):
            pl.when(pl.program_id(0) == layer)(functools.partial(one, layer))

    ins = [squares, *weights, *m, *v, *(of[p] for of in g for p in pieces)]
    layer = lambda a: pl.BlockSpec((1, *a.shape[1:]), lambda n: (n, 0, 0))
    outs = [*(_shape(a.shape) for a in weights), *(_shape(a.shape, F32) for a in (*m, *v))]
    return pl.pallas_call(
        kernel,
        grid=(layers,),
        in_specs=[layer(a) if a.ndim == 3 else _whole(a) for a in ins],
        out_specs=[layer(a) for a in outs],
        out_shape=outs,
        compiler_params=pltpu.CompilerParams(dimension_semantics=("arbitrary",), vmem_limit_bytes=VMEM),
        cost_estimate=pl.CostEstimate(flops=10**7, bytes_accessed=32 * 10**6, transcendentals=0),
        name="update",
    )(*ins)


def solution(mesh):
    def step(x, dy, *arrays):
        weights, m, v = (arrays[i : i + 7] for i in (0, 7, 14))
        shards = dict(zip(NAMES, weights, strict=True))
        blocks = {name: w.shape[1:] for name, w in shards.items()}
        given = lambda names: [shards[n] for n in names]
        h0, tokens = x[0], x.shape[1]

        w = [{}, {}]
        tables, got = first(tokens, Gather(ATT, blocks, 0), given(ATT), 0)
        w[0] |= zip(ATT, got)
        (mid0, *kept0), got = attend(h0, w[0], tables, Gather(MLP, blocks, 0), given(MLP), 1)
        w[0] |= zip(MLP, got)
        early = ATT + MLP[:2]
        (h1, *kept_gated), got = gated(mid0, *(w[0][n] for n in MLP), Gather(early, blocks, 1), given(early), 2)
        w[1] |= zip(early, got)
        (mid1, *kept1), got = attend(h1, w[1], tables, Gather(MLP[2:], blocks, 1), given(MLP[2:]), 3)
        w[1] |= zip(MLP[2:], got)

        by, g = [{}, {}], [{}, {}]
        early, last = ("first_gate", "first_up"), ("last_gate", "last_up")
        rest = ("w_down", *last)
        blocks |= {n: (blocks["w_up"][0], CHUNK) for n in last}
        (by_mid1, *got), _ = gated_bwd(mid1, dy[0], *(w[1][n] for n in MLP), number=4)
        by[1] |= zip(rest, got[:3])
        g[1] |= zip(early, got[3:])
        (*got, by_h1), sums = attend_bwd(h1, w[1], tables, kept1, by_mid1, True, Scatter(last, blocks), [by[1][n] for n in last], 5)
        by[1] |= zip(ATT, got)
        g[1] |= zip(last, sums)
        names = ("w_down", *ATT)
        (by_mid0, *got), sums = gated_bwd(mid0, by_h1, *(w[0][n] for n in MLP), kept_gated, Scatter(names, blocks), [by[1][n] for n in names], 6)
        by[0] |= zip(rest, got[:3])
        g[0] |= zip(early, got[3:])
        g[1] |= zip(names, sums)
        got, sums = attend_bwd(h0, w[0], tables, kept0, by_mid0, False, Scatter(rest, blocks), [by[0][n] for n in rest], 7)
        by[0] |= zip(ATT, got)
        g[0] |= zip(rest, sums)
        sums, squares = finish(Scatter(ATT, blocks), [by[0][n] for n in ATT], [*g[1].values(), *g[0].values()], 8)
        g[0] |= zip(ATT, sums)

        return tuple(update(weights, m, v, g, squares))

    states, cut = P(("rep", "dp"), None, None), P(None, "dp", None)
    return jax.shard_map(
        step,
        mesh=mesh,
        in_specs=(states, states) + (cut,) * 21,
        out_specs=(P("rep", "dp", None),) * 21,
        check_vma=False,
    )
```

```python
import functools

import jax
import jax.numpy as jnp
import numpy as np
from jax import lax
from jax.experimental import pallas as pl
from jax.experimental.pallas import tpu as pltpu
from jax.sharding import PartitionSpec as P

HEAD = 256
THETA = 10000
NAMES = ("wq", "wk", "wv", "wo", "w_gate", "w_up", "w_down")
ATT, MLP = NAMES[:4], NAMES[4:]
NEG = -1e30
HIDDEN = 2 * NEG
LOG2E = 1.4426950408889634
VMEM = 62 * 2**20
BLOCK = 512
CHUNK = 512
ROWS = 512
ANY = pl.BlockSpec(memory_space=pl.ANY)
MESH = pl.DeviceIdType.MESH
F32, BF16 = jnp.float32, jnp.bfloat16


def _nn(a, b):
    return lax.dot_general(a, b, (((1,), (0,)), ((), ())), preferred_element_type=F32)


def _nt(a, b):
    return lax.dot_general(a, b, (((1,), (1,)), ((), ())), preferred_element_type=F32)


def _loop(n, do):
    def some(t, state):
        do(t)
        return state

    lax.fori_loop(0, n, some, 0)


def _slab(start, rows):
    return pl.ds(pl.multiple_of(start, 16), rows)


def _some_rows(t):
    return _slab(t * 16, 16)


def _units(names, blocks):
    cut = []
    for name in names:
        rows, columns = blocks[name]
        if name in ("wo", "w_down"):
            cut += [(name, 0, rows // 2, 0), (name, rows // 2, rows // 2, 1)]
        else:
            cut += [(name, 0, rows, 0 if name in ("wq", "w_gate", "last_gate") else 1)]
    return cut


def _around(way):
    me = lax.axis_index("dp")
    core, y, x = lax.rem(me, 2), lax.rem(lax.div(me, 2), 2), lax.div(me, 4)
    over_x, over_y = 4 - 8 * x, 2 - 4 * y
    first, second = (over_x, over_y) if way == 0 else (over_y, over_x)
    return me, 1 - 2 * core, first, second, over_x + over_y


def _meet():
    me, other, first, second, _ = _around(0)
    barrier = pltpu.get_barrier_semaphore()
    for way in (other, first, second):
        pl.semaphore_signal(barrier, inc=1, device_id={"dp": me + way}, device_id_type=MESH)
    pl.semaphore_wait(barrier, 3)


class Gather:
    def __init__(self, names, blocks, layer):
        self.names, self.blocks, self.layer = names, blocks, layer
        self.units = _units(names, blocks)

    def in_specs(self):
        return [ANY] * len(self.names)

    def out_specs(self):
        return [ANY] * len(self.names)

    def out_shape(self):
        return [jax.ShapeDtypeStruct((8 * self.blocks[n][0], self.blocks[n][1]), BF16) for n in self.names]

    def scratch(self):
        n = len(self.units)
        return [pltpu.SemaphoreType.DMA((n,)), pltpu.SemaphoreType.DMA((n, 7)), pltpu.SemaphoreType.DMA((n, 7))]

    def bind(self, ins, outs, scratch):
        self.shards, self.whole = dict(zip(self.names, ins)), dict(zip(self.names, outs))
        self.local, self.send, self.recv = scratch

    def _piece(self, unit, device):
        name, at, rows, _ = unit
        return self.whole[name].at[_slab(device * self.blocks[name][0] + at, rows)]

    def _copy(self, i, slot, arrived=False):
        unit = self.units[i]
        name, at, rows, way = unit
        me, other, first, second, across = _around(way)
        own = self.shards[name].at[self.layer, pl.ds(at, rows)]
        source, owner, to, comes = (
            (own, me, first, me + first),
            (own, me, second, me + second),
            (own, me, other, me + other),
            (None, me + first, second, me + across),
            (None, me + first, other, me + first + other),
            (None, me + second, other, me + second + other),
            (None, me + across, other, me + across + other),
        )[slot]
        if arrived:
            source, owner = None, comes
        target = self._piece(unit, owner)
        return pltpu.make_async_remote_copy(target if source is None else source, target, self.send.at[i, slot], self.recv.at[i, slot],
                                            device_id={"dp": me + to}, device_id_type=MESH)

    def _mine(self, i):
        name, at, rows, way = self.units[i]
        return pltpu.make_async_copy(self.shards[name].at[self.layer, pl.ds(at, rows)], self._piece(self.units[i], lax.axis_index("dp")), self.local.at[i])

    def begin(self):
        for i in range(len(self.units)):
            for slot in range(3):
                self._copy(i, slot).start()
            self._mine(i).start()

    def middle(self):
        for i in range(len(self.units)):
            self._copy(i, 0, True).wait_recv()
            self._copy(i, 3).start()
            self._copy(i, 4).start()
            self._copy(i, 1, True).wait_recv()
            self._copy(i, 5).start()

    def end(self):
        for i in range(len(self.units)):
            self._copy(i, 3, True).wait_recv()
            self._copy(i, 6).start()
        for i in range(len(self.units)):
            for slot in (2, 4, 5, 6):
                self._copy(i, slot, True).wait_recv()
            for slot in range(7):
                self._copy(i, slot).wait_send()
            self._mine(i).wait()

    def actions(self, steps):
        if steps == 1:
            return {0: ([_meet, self.begin], [self.middle, self.end])}
        return {0: ([_meet, self.begin], []), steps - 1: ([self.middle], [self.end])}


class Scatter:
    def __init__(self, names, blocks):
        self.names, self.blocks = names, blocks
        self.units = _units(names, blocks)

    def in_specs(self):
        return [ANY] * len(self.names)

    def out_specs(self):
        return [pl.BlockSpec(self.blocks[n], lambda *_: (0, 0), pipeline_mode=pl.Buffered(1)) for n in self.names]

    def out_shape(self):
        return [jax.ShapeDtypeStruct(self.blocks[n], BF16) for n in self.names]

    def scratch(self):
        n, dma = len(self.units), pltpu.SemaphoreType.DMA
        found = [dma((n, 4)), dma((n, 4)), dma((n, 4)), dma((n, 2)), dma((n, 2)), dma((n,)), dma((n,))]
        for name, _, rows, _ in self.units:
            columns = self.blocks[name][1]
            found += [pltpu.VMEM((k, rows, columns), BF16) for k in (4, 4, 2, 2, 1, 1)]
        return found

    def bind(self, ins, outs, scratch):
        self.terms, self.outs = dict(zip(self.names, ins)), dict(zip(self.names, outs))
        self.load, self.send0, self.recv0, self.send1, self.recv1, self.send2, self.recv2 = scratch[:7]
        rest = scratch[7:]
        self.buffers = [rest[6 * i : 6 * i + 6] for i in range(len(self.units))]

    def _block(self, unit, device):
        name, at, rows, _ = unit
        return self.terms[name].at[_slab(device * self.blocks[name][0] + at, rows)]

    def _own(self, i, j):
        me, other, *ways = _around(self.units[i][3])
        return pltpu.make_async_copy(self._block(self.units[i], me + ([0] + ways)[j]), self.buffers[i][0].at[j], self.load.at[i, j])

    def _across(self, i, j):
        me, other, *ways = _around(self.units[i][3])
        return pltpu.make_async_remote_copy(self._block(self.units[i], me + other + ([0] + ways)[j]), self.buffers[i][1].at[j], self.send0.at[i, j],
                                            self.recv0.at[i, j], device_id={"dp": me + other}, device_id_type=MESH)

    def _first(self, i, j):
        me, _, first, _, _ = _around(self.units[i][3])
        return pltpu.make_async_remote_copy(self.buffers[i][2].at[j], self.buffers[i][3].at[j], self.send1.at[i, j], self.recv1.at[i, j],
                                            device_id={"dp": me + first}, device_id_type=MESH)

    def _second(self, i):
        me, _, _, second, _ = _around(self.units[i][3])
        return pltpu.make_async_remote_copy(self.buffers[i][4].at[0], self.buffers[i][5].at[0], self.send2.at[i], self.recv2.at[i],
                                            device_id={"dp": me + second}, device_id_type=MESH)

    def begin(self):
        for js in ((1, 3), (2, 0)):
            for i in range(len(self.units)):
                for j in js:
                    self._across(i, j).start()
                    self._own(i, j).start()

    def _ready(self, i, j):
        self._own(i, j).wait()
        self._across(i, j).wait_recv()

    def _add(self, rows, store, *terms):
        def some(t):
            at = _some_rows(t)
            store(at, sum(term[at, :].astype(F32) for term in terms))

        _loop(rows // 16, some)

    def part1(self):
        for i, (_, _, rows, _) in enumerate(self.units):
            own, came, out = self.buffers[i][:3]
            for j, k in ((1, 0), (3, 1)):
                self._ready(i, j)

                def store(at, value, k=k, out=out):
                    out[k, at, :] = value.astype(BF16)

                self._add(rows, store, own.at[j], came.at[j])
            for i in ([i - 1] if i else []) + ([i] if i == len(self.units) - 1 else []):
                self._first(i, 0).start()
                self._first(i, 1).start()

    def part2(self):
        for i, (_, _, rows, _) in enumerate(self.units):
            own, came, _, got, out, _ = self.buffers[i]
            self._ready(i, 2)
            self._first(i, 0).wait_recv()
            self._first(i, 1).wait_recv()

            def store(at, value, out=out):
                out[0, at, :] = value.astype(BF16)

            self._add(rows, store, own.at[2], came.at[2], got.at[1])
            for i in ([i - 1] if i else []) + ([i] if i == len(self.units) - 1 else []):
                self._second(i).start()

    def end(self):
        for i, (name, start, rows, _) in enumerate(self.units):
            own, came, _, got, _, last = self.buffers[i]
            self._ready(i, 0)
            self._second(i).wait_recv()

            def store(at, value, name=name, start=start):
                self.outs[name][_slab(start + at.start, at.size), :] = value.astype(BF16)

            self._add(rows, store, own.at[0], came.at[0], got.at[0], last.at[0])
        for i in range(len(self.units)):
            for j in range(4):
                self._across(i, j).wait_send()
            for j in range(2):
                self._first(i, j).wait_send()
            self._second(i).wait_send()

    def actions(self, steps):
        if steps == 8:
            return {0: ([_meet, self.begin], []), 4: ([self.part1], []), 7: ([self.part2], [self.end])}
        return {0: ([_meet, self.begin], []), 1: ([self.part1], []), steps - 2: ([self.part2], []), steps - 1: ([], [self.end])}


class Chunks:
    def __init__(self, rows, chunks):
        self.rows, self.n = rows, chunks - 2

    def scratch(self):
        n, rows, dma = self.n, self.rows, pltpu.SemaphoreType.DMA
        sems = [dma((n, 2, 4)), dma((n, 2, 4)), dma((n, 2, 2)), dma((n, 2, 2)), dma((n, 2)), dma((n, 2))]
        block = lambda *lead: pltpu.VMEM((*lead, rows, CHUNK), BF16)
        return [*sems, pltpu.VMEM((n, 2, 8 * rows, CHUNK), BF16), block(n, 2, 4), block(n, 2, 2), block(n, 2, 2), block(n, 2), block(n, 2)]

    def bind(self, outs, scratch):
        self.outs = outs
        self.send0, self.recv0, self.send1, self.recv1, self.send2, self.recv2, self.terms, self.came, self.sum1, self.got1, self.sum2, self.got2 = scratch

    def _block(self, j, u, device):
        return self.terms.at[j, u, _slab(device * self.rows, self.rows)]

    def _own(self, j, u, k):
        me, _, *ways = _around(u)
        return self._block(j, u, me + ([0] + ways)[k])[...].astype(F32) + self.came[j, u, k].astype(F32)

    def _across(self, j, u, k):
        me, other, *ways = _around(u)
        return pltpu.make_async_remote_copy(self._block(j, u, me + other + ([0] + ways)[k]), self.came.at[j, u, k], self.send0.at[j, u, k],
                                            self.recv0.at[j, u, k], device_id={"dp": me + other}, device_id_type=MESH)

    def _first(self, j, u, k):
        me, _, first, _, _ = _around(u)
        return pltpu.make_async_remote_copy(self.sum1.at[j, u, k], self.got1.at[j, u, k], self.send1.at[j, u, k], self.recv1.at[j, u, k],
                                            device_id={"dp": me + first}, device_id_type=MESH)

    def _second(self, j, u):
        me, _, _, second, _ = _around(u)
        return pltpu.make_async_remote_copy(self.sum2.at[j, u], self.got2.at[j, u], self.send2.at[j, u], self.recv2.at[j, u],
                                            device_id={"dp": me + second}, device_id_type=MESH)

    def part0(self, j):
        for u in range(2):
            for k in (1, 3, 2, 0):
                self._across(j, u, k).start()

    def part1(self, j):
        for u in range(2):
            for k, at in ((1, 0), (3, 1)):
                self._across(j, u, k).wait_recv()
                self.sum1[j, u, at] = self._own(j, u, k).astype(BF16)

    def part2(self, j):
        for u in range(2):
            for k in range(2):
                self._first(j, u, k).start()

    def part3(self, j):
        for u in range(2):
            self._across(j, u, 2).wait_recv()
            for k in range(2):
                self._first(j, u, k).wait_recv()
            self.sum2[j, u] = (self._own(j, u, 2) + self.got1[j, u, 1].astype(F32)).astype(BF16)

    def part4(self, j):
        for u in range(2):
            self._second(j, u).start()

    def end(self, j):
        for u in range(2):
            self._across(j, u, 0).wait_recv()
            self._second(j, u).wait_recv()
            total = self._own(j, u, 0) + self.got1[j, u, 0].astype(F32) + self.got2[j, u].astype(F32)
            self.outs[u][:, pl.ds(pl.multiple_of(j * CHUNK, CHUNK), CHUNK)] = total.astype(BF16)
        for u in range(2):
            for k in range(4):
                self._across(j, u, k).wait_send()
            for k in range(2):
                self._first(j, u, k).wait_send()
            self._second(j, u).wait_send()


def _call(body, steps, ins, in_specs, outs, out_specs, scratch, rider=None, given=(), number=0, flops=0, name=None, meet=False):
    ni, no, ns = len(in_specs), len(out_specs), len(scratch)
    more_in, more_out, more_specs, more_scratch = ([], [], [], []) if rider is None else (rider.in_specs(), rider.out_shape(), rider.out_specs(), rider.scratch())

    def kernel(*refs):
        cuts = [ni, len(more_in), no, len(more_out), ns, len(more_scratch)]
        parts, at = [], 0
        for n in cuts:
            parts.append(refs[at : at + n])
            at += n
        my_in, its_in, my_out, its_out, mine, its = parts
        step = pl.program_id(0)
        acts = {}
        if rider is not None:
            rider.bind(its_in, its_out, its)
            acts = rider.actions(steps)
        elif meet:
            acts = {0: ([_meet], [])}

        def run(which):
            for s, lists in acts.items():
                if lists[which]:
                    if steps == 1:
                        for act in lists[which]:
                            act()
                    else:

                        @pl.when(step == s)
                        def _(todo=lists[which]):
                            for act in todo:
                                act()

        run(0)
        body(step, my_in, my_out, mine)
        run(1)

    params = dict(dimension_semantics=("arbitrary",), vmem_limit_bytes=VMEM)
    if rider is not None or meet:
        params |= dict(collective_id=number, has_side_effects=True)
    got = pl.pallas_call(
        kernel,
        grid=(steps,),
        in_specs=[*in_specs, *more_in],
        out_specs=[*out_specs, *more_specs],
        out_shape=[*outs, *more_out],
        scratch_shapes=[*scratch, *more_scratch],
        compiler_params=pltpu.CompilerParams(**params),
        cost_estimate=pl.CostEstimate(flops=int(flops) + 1, bytes_accessed=10**6, transcendentals=0),
        name=name,
    )(*ins, *given)
    return list(got[:no]), list(got[no:])


def _whole(a):
    return pl.BlockSpec(a.shape, lambda *_: (0,) * len(a.shape), pipeline_mode=pl.Buffered(1))


def _shape(shape, dtype=BF16):
    return jax.ShapeDtypeStruct(shape, dtype)


def first(tokens, rider, given, number):
    half = HEAD // 2
    speed = jnp.asarray(THETA ** (-np.arange(half) / half), F32)[None]

    def body(step, ins, outs, scratch):
        (speed_ref,) = ins

        def some(t):
            at = pl.ds(pl.multiple_of(t * 256, 256), 256)
            angle = (lax.broadcasted_iota(jnp.int32, (256, half), 0) + t * 256).astype(F32) * speed_ref[...]
            cos_ref, sin_ref = outs
            cos_ref[at, :], sin_ref[at, :] = jnp.cos(angle), jnp.sin(angle)

        _loop(tokens // 256, some)

    outs = [_shape((tokens, half), F32)] * 2
    return _call(body, 1, [speed], [_whole(speed)], outs, [_whole(a) for a in outs], [], rider, given, number, name="first")


def _hidden():
    return lax.broadcasted_iota(jnp.int32, (BLOCK, BLOCK), 0) > lax.broadcasted_iota(jnp.int32, (BLOCK, BLOCK), 1)


def _strip(ref, head, a):
    return ref[a * BLOCK : (a + 1) * BLOCK, head * HEAD : (head + 1) * HEAD]


def _turn(t, cos, sin):
    half, parts = HEAD // 2, []
    for at in range(0, t.shape[1], HEAD):
        a, b = t[:, at : at + half].astype(F32), t[:, at + half : at + HEAD].astype(F32)
        parts += [a * cos - b * sin, b * cos + a * sin]
    return jnp.concatenate(parts, -1).astype(BF16)


def attend(h, w, tables, rider, given, number):
    wq, wk, wv, wo = (w[n] for n in ATT)
    tokens, heads = h.shape[0], wq.shape[1] // HEAD
    blocks, scale = tokens // BLOCK, HEAD**-0.5
    e = scale * LOG2E

    def body(step, ins, outs, scratch):
        h_ref, wq_ref, wk_ref, wv_ref, wo_ref, cos_ref, sin_ref = ins
        mid_ref, q_ref, k_ref, v_ref, o_ref, lse_ref = outs
        top_s, mix_s = scratch

        @pl.when(step < blocks)
        def _():
            at = pl.ds(pl.multiple_of(step * BLOCK, BLOCK), BLOCK)
            wide = h_ref[at, :].astype(F32)
            a = (wide * _scale(wide)).astype(BF16)
            cos, sin = cos_ref[at, :], sin_ref[at, :]
            q_ref[at, :] = _turn(_nn(a, wq_ref[...]).astype(BF16), cos, sin)
            k_ref[at, :] = _turn(_nn(a, wk_ref[...]).astype(BF16), cos, sin)
            v_ref[at, :] = _nn(a, wv_ref[...]).astype(BF16)

        def block(j):
            strips = [(n, a) for a in range(j, blocks) for n in range(heads)]
            here = slice(j * BLOCK, (j + 1) * BLOCK)
            keys = k_ref[here, :]
            values = jnp.concatenate([v_ref[here, :].T, jnp.ones((8, BLOCK), BF16)], axis=0)
            scores = [_nt(keys, _strip(q_ref, n, a)) for n, a in strips]
            weights, keeps = [], []
            for (n, a), s in zip(strips, scores):
                i = a * heads + n
                if a == j:
                    s = jnp.where(_hidden(), HIDDEN, s)
                top = s.max(axis=0, keepdims=True)
                if j:
                    old = top_s[i : i + 1, :]
                    top = jnp.maximum(old, top)
                    keeps.append(jnp.exp2((old - top) * e))
                else:
                    keeps.append(None)
                top_s[i : i + 1, :] = top
                weights.append(jnp.exp2((s - top) * e).astype(BF16))
            done = []
            for (n, a), p, keep in zip(strips, weights, keeps):
                i = a * heads + n
                mix = _nn(values, p)
                if j:
                    mix = mix_s[i] * keep + mix
                if a > j:
                    mix_s[i] = mix
                else:
                    total = mix[HEAD : HEAD + 1, :]
                    done.append((mix[:HEAD, :] * (1 / total)).T.astype(BF16))
                    o_ref[here, n * HEAD : (n + 1) * HEAD] = done[-1]
                    lse_ref[i : i + 1, :] = top_s[i : i + 1, :] * scale + jnp.log(total)
            out = _nn(jnp.concatenate(done, -1), wo_ref[...]).astype(BF16).astype(F32)
            mid_ref[here, :] = (h_ref[here, :].astype(F32) + out).astype(BF16)

        for j in range(blocks):
            pl.when(step == blocks + j)(functools.partial(block, j))

    n = heads * blocks
    ins = [h, wq, wk, wv, wo, *tables]
    outs = [_shape(h.shape), _shape((tokens, heads * HEAD)), _shape((tokens, HEAD)), _shape((tokens, HEAD)), _shape((tokens, heads * HEAD)), _shape((n, BLOCK), F32)]
    flops = 2 * tokens * (h.shape[1] * 1536 + 1.2 * tokens * heads * HEAD)
    return _call(body, 2 * blocks, ins, [_whole(a) for a in ins], outs, [_whole(a) for a in outs],
                 [pltpu.VMEM((n, BLOCK), F32), pltpu.VMEM((n, HEAD + 8, BLOCK), F32)], rider, given, number, flops, "attend")


def attend_bwd(h, w, tables, kept, by_mid, wanted, rider, given, number):
    q, k, v, o, lse = kept
    wq, wk, wv, wo = (w[n] for n in ATT)
    (tokens, d), heads = h.shape, wq.shape[1] // HEAD
    blocks, scale = tokens // BLOCK, HEAD**-0.5
    e = scale * LOG2E

    def body(step, ins, outs, scratch):
        h_ref, wq_ref, wk_ref, wv_ref, wo_ref, cos_ref, sin_ref, q_ref, k_ref, v_ref, o_ref, lse_ref, by_ref = ins
        dwq_ref, dwk_ref, dwv_ref, dwo_ref, *dh_ref = outs
        dq_s, do_s, delta_s, dwq_s, dwk_s, dwv_s, dwo_s = scratch

        def before(t):
            here = slice(t * BLOCK, (t + 1) * BLOCK)
            by, o = by_ref[here, :], o_ref[here, :]
            do = _nt(by, wo_ref[...]).astype(BF16)
            do_s[here, :] = do
            dots = (do.astype(F32) * o.astype(F32)).T
            for n in range(heads):
                i = t * heads + n
                delta_s[i : i + 1, :] = dots[n * HEAD : (n + 1) * HEAD, :].sum(axis=0, keepdims=True)
            term = _nn(o.T, by)
            if t:
                term = dwo_s[...] + term
            if t < blocks - 1:
                dwo_s[...] = term
            else:
                dwo_ref[...] = term.astype(BF16)

        def block(j):
            here = slice(j * BLOCK, (j + 1) * BLOCK)
            strips = [(n, a) for a in range(j, blocks) for n in range(heads)]
            keys, values = k_ref[here, :], v_ref[here, :]
            turned_keys = keys.T
            dk = dv = None
            dq = []
            scores = [_nt(keys, _strip(q_ref, n, a)) for n, a in strips]
            dps = [_nt(values, _strip(do_s, n, a)) for n, a in strips]
            for (n, a), s, dp in zip(strips, scores, dps):
                i = a * heads + n
                p = jnp.exp2(s * e - lse_ref[i : i + 1, :] * LOG2E)
                if a == j:
                    p = jnp.where(_hidden(), 0.0, p)
                ds = (p * (dp - delta_s[i : i + 1, :])).astype(BF16)
                by_v = _nn(p.astype(BF16), _strip(do_s, n, a))
                by_k = _nn(ds, _strip(q_ref, n, a))
                dv, dk = (by_v, by_k) if dv is None else (dv + by_v, dk + by_k)
                by_q = _nn(turned_keys, ds)
                if j:
                    by_q = dq_s[i] + by_q
                if a > j:
                    dq_s[i] = by_q
                else:
                    dq.append((by_q * scale).T.astype(BF16))
            cos, sin = cos_ref[here, :], -sin_ref[here, :]
            dq = _turn(jnp.concatenate(dq, -1), cos, sin)
            dk = _turn((dk * scale).astype(BF16), cos, sin)
            dv = dv.astype(BF16)
            wide = h_ref[here, :].astype(F32)
            size = _scale(wide)
            at = (wide * size).astype(BF16).T
            for by, sum_s, out_ref in ((dq, dwq_s, dwq_ref), (dk, dwk_s, dwk_ref), (dv, dwv_s, dwv_ref)):
                term = _nn(at, by)
                if j:
                    term = sum_s[...] + term
                if j < blocks - 1:
                    sum_s[...] = term
                else:
                    out_ref[...] = term.astype(BF16)
            if wanted:
                by_a = (_nt(dv, wv_ref[...]).astype(BF16).astype(F32) + _nt(dk, wk_ref[...]).astype(BF16).astype(F32)
                        + _nt(dq, wq_ref[...]).astype(BF16).astype(F32)).astype(BF16).astype(F32)
                by_h = by_a * size - wide * (size * size * size) * jnp.mean(by_a * wide, -1, keepdims=True)
                dh_ref[0][here, :] = (by_h.astype(BF16).astype(F32) + by_ref[here, :].astype(F32)).astype(BF16)

        for t in range(blocks):
            pl.when(step == t)(functools.partial(before, t))
            pl.when(step == blocks + t)(functools.partial(block, t))

    ins = [h, wq, wk, wv, wo, *tables, q, k, v, o, lse, by_mid]
    outs = [_shape(a.shape) for a in (wq, wk, wv, wo) + ((h,) if wanted else ())]
    n = heads * blocks
    full = lambda a: pltpu.VMEM(a.shape, F32)
    flops = 4 * tokens * (d * 1536 + 1.5 * tokens * heads * HEAD)
    return _call(body, 2 * blocks, ins, [_whole(a) for a in ins], outs, [_whole(a) for a in outs],
                 [pltpu.VMEM((n, HEAD, BLOCK), F32), pltpu.VMEM(o.shape, BF16), pltpu.VMEM((n, BLOCK), F32), full(wq), full(wk), full(wv), full(wo)],
                 rider, given, number, flops, "attend_bwd")


def _scale(wide):
    return lax.rsqrt(jnp.mean(wide * wide, -1, keepdims=True) + 1e-6)


def _tokens(n, do):
    _loop(n // ROWS, lambda t: do(pl.ds(pl.multiple_of(t * ROWS, ROWS), ROWS)))


def _chunks(w_gate, w_down):
    across = pl.BlockSpec((w_gate.shape[0], CHUNK), lambda j: (0, j))
    down = pl.BlockSpec((CHUNK, w_down.shape[1]), lambda j: (j, 0))
    return across, down


def gated(h, w_gate, w_up, w_down, rider, given, number):
    tokens, d = h.shape
    steps = w_gate.shape[1] // CHUNK
    across, down = _chunks(w_gate, w_down)

    def body(step, ins, outs, scratch):
        h_ref, g_ref, u_ref, d_ref = ins
        o_ref, gate_ref, up_ref = outs
        b_s, sum_s = scratch

        @pl.when(step == 0)
        def _():
            def norm(at):
                wide = h_ref[at, :].astype(F32)
                b_s[at, :] = (wide * _scale(wide)).astype(BF16)
                sum_s[at, :] = jnp.zeros((ROWS, d), F32)

            _tokens(tokens, norm)

        def some(at):
            b = b_s[at, :]
            gate, up = _nn(b, g_ref[...]), _nn(b, u_ref[...])
            gate_ref[0, at, :], up_ref[0, at, :] = gate, up
            act = (gate * (1 / (1 + jnp.exp(-gate))) * up).astype(BF16)
            sum_s[at, :] += _nn(act, d_ref[...])

        _tokens(tokens, some)

        @pl.when(step == steps - 1)
        def _():
            def last(at):
                o_ref[at, :] = (h_ref[at, :].astype(F32) + sum_s[at, :].astype(BF16).astype(F32)).astype(BF16)

            _tokens(tokens, last)

    keep = pl.BlockSpec((1, tokens, CHUNK), lambda j: (j, 0, 0))
    kept = _shape((steps, tokens, CHUNK), F32)
    return _call(body, steps, [h, w_gate, w_up, w_down], [_whole(h), across, across, down], [_shape(h.shape), kept, kept], [_whole(h), keep, keep],
                 [pltpu.VMEM((tokens, d), BF16), pltpu.VMEM((tokens, d), F32)], rider, given, number, 6 * tokens * d * w_gate.shape[1], "gated")


def gated_bwd(h, by_out, w_gate, w_up, w_down, kept=(), rider=None, given=(), number=0):
    tokens, d = h.shape
    steps = w_gate.shape[1] // CHUNK
    across, down = _chunks(w_gate, w_down)
    sums, inner = Chunks(d // 8, steps), tokens // ROWS

    def body(step, ins, outs, scratch):
        h_ref, by_ref, g_ref, u_ref, d_ref, *kept_refs = ins
        dh_ref, dd_ref, lg_ref, lu_ref, *sum_refs = outs
        bt_s, byt_s, sum_s, act_s, gate_s, up_s = scratch[:6]
        sums.bind(sum_refs, scratch[8:])
        if kept:
            tile_s, sem = scratch[6:8]
        else:
            b_s = scratch[6]

        def tiles(i):
            at = pl.ds(pl.multiple_of(lax.rem(i, inner) * ROWS, ROWS), ROWS)
            slot = lax.rem(i, 2)
            return [pltpu.make_async_copy(ref.at[lax.div(i, inner), at], tile_s.at[slot, k], sem.at[slot, k]) for k, ref in enumerate(kept_refs)]

        if kept:

            @pl.when(step == 0)
            def _():
                for copy in tiles(0):
                    copy.start()

        new, old = (step >= 1) & (step <= sums.n), step >= 2
        pl.when(new)(lambda: sums.part0(step - 1))

        @pl.when(step == 0)
        def _():
            def norm(at):
                wide = h_ref[at, :].astype(F32)
                b = (wide * _scale(wide)).astype(BF16)
                if not kept:
                    b_s[at, :] = b
                bt_s[:, at] = b.T
                byt_s[:, at] = by_ref[at, :].T
                sum_s[at, :] = jnp.zeros((ROWS, d), F32)

            _tokens(tokens, norm)

        def some(t):
            @pl.when(t == inner - 2)
            def _():
                pl.when(old)(lambda: sums.part3(step - 2))
                pl.when(new)(lambda: sums.part1(step - 1))

            @pl.when(t == inner - 1)
            def _():
                pl.when(old)(lambda: sums.part4(step - 2))
                pl.when(new)(lambda: sums.part2(step - 1))

            at = pl.ds(pl.multiple_of(t * ROWS, ROWS), ROWS)
            by = by_ref[at, :]
            if kept:
                i = step * inner + t

                @pl.when(i + 1 < steps * inner)
                def _():
                    for copy in tiles(i + 1):
                        copy.start()

                for copy in tiles(i):
                    copy.wait()
                gate, up = tile_s[lax.rem(i, 2), 0], tile_s[lax.rem(i, 2), 1]
            else:
                b = b_s[at, :]
                gate, up = _nn(b, g_ref[...]), _nn(b, u_ref[...])
            by_act = _nt(by, d_ref[...]).astype(BF16).astype(F32)
            open_ = 1 / (1 + jnp.exp(-gate))
            silu = gate * open_
            act_s[at, :] = (silu * up).astype(BF16)
            by_up = (by_act * silu).astype(BF16)
            by_gate = (by_act * up * (open_ + silu * (1 - open_))).astype(BF16)
            gate_s[at, :] = by_gate
            up_s[at, :] = by_up
            sum_s[at, :] += _nt(by_gate, g_ref[...]) + _nt(by_up, u_ref[...])

        _loop(inner, some)
        for u, by_s, last_ref in ((0, gate_s, lg_ref), (1, up_s, lu_ref)):
            term = _nn(bt_s[...], by_s[...]).astype(BF16)

            @pl.when(step < sums.n)
            def _(u=u, term=term):
                sums.terms[step, u] = term

            @pl.when(step >= sums.n)
            def _(last_ref=last_ref, term=term):
                last_ref[:, pl.ds(pl.multiple_of((step - sums.n) * CHUNK, CHUNK), CHUNK)] = term

        dd_ref[...] = _nn(byt_s[...], act_s[...]).astype(BF16).T
        pl.when(old)(lambda: sums.end(step - 2))

        @pl.when(step == steps - 1)
        def _():
            def last(at):
                wide = h_ref[at, :].astype(F32)
                scale = _scale(wide)
                by_b = sum_s[at, :].astype(BF16).astype(F32)
                by = by_b * scale - wide * (scale * scale * scale) * jnp.mean(by_b * wide, -1, keepdims=True)
                dh_ref[at, :] = (by.astype(BF16).astype(F32) + by_ref[at, :].astype(F32)).astype(BF16)

            _tokens(tokens, last)

    half, full = pltpu.VMEM((tokens, d), BF16), pltpu.VMEM((tokens, d), F32)
    chunk, turned_ = pltpu.VMEM((tokens, CHUNK), BF16), pltpu.VMEM((d, tokens), BF16)
    outs = [_shape(h.shape), _shape(w_down.shape), *[_shape((d, (steps - sums.n) * CHUNK))] * 2, *[_shape((d // 8, sums.n * CHUNK))] * 2]
    more = [pltpu.VMEM((2, 2, ROWS, CHUNK), F32), pltpu.SemaphoreType.DMA((2, 2))] if kept else [half, pltpu.SemaphoreType.DMA((1,))]
    return _call(body, steps, [h, by_out, w_gate, w_up, w_down, *kept], [_whole(h), _whole(h), across, across, down, *[ANY] * len(kept)],
                 outs, [_whole(h), down, *(_whole(a) for a in outs[2:])], [turned_, turned_, full, chunk, chunk, chunk, *more, *sums.scratch()],
                 rider, given, number, (12 if kept else 16) * tokens * d * w_gate.shape[1], "gated_bwd", True)


def finish(rider, given, others, number):
    n, ng, distances = len(others), len(given), range(1, 8)

    def squares(ref):
        rows, columns = ref.shape

        def some(t, total):
            g = ref[_some_rows(t), :].astype(F32)
            g = g * g
            g = g[:8, :] + g[8:, :]
            return total + sum(g[:, c : c + 128] for c in range(0, columns, 128))

        return lax.fori_loop(0, rows // 16, some, jnp.zeros((8, 128), F32))

    def kernel(*refs):
        other_refs, given_refs, refs = refs[:n], refs[n : n + ng], refs[n + ng :]
        out_refs, total_ref, refs = refs[:ng], refs[ng], refs[ng + 1 :]
        mine_s, all_s, send, recv = refs[:4]
        rider.bind(given_refs, out_refs, refs[4:])
        me = lax.axis_index("dp")
        barrier = pltpu.get_barrier_semaphore()
        for k in distances:
            pl.semaphore_signal(barrier, inc=1, device_id={"dp": lax.rem(me + k, 8)}, device_id_type=MESH)
        pl.semaphore_wait(barrier, 7)
        rider.begin()
        total = sum(squares(ref) for ref in other_refs)
        for act in (rider.part1, rider.part2, rider.end):
            act()
        mine_s[...] = total + sum(squares(ref) for ref in out_refs)

        def copy(k):
            return pltpu.make_async_remote_copy(mine_s, all_s.at[me], send.at[k], recv.at[k], device_id={"dp": lax.rem(me + k, 8)}, device_id_type=MESH)

        def arrived(k):
            place = all_s.at[lax.rem(me + 8 - k, 8)]
            return pltpu.make_async_remote_copy(place, place, send.at[k], recv.at[k], device_id={"dp": me}, device_id_type=MESH)

        for k in distances:
            copy(k).start()
        all_s[me] = mine_s[...]
        for k in distances:
            arrived(k).wait_recv()
        for k in distances:
            copy(k).wait_send()
        total_ref[...] = sum(all_s[k] for k in range(8))

    outs = [*rider.out_shape(), _shape((8, 128), F32)]
    got = pl.pallas_call(
        kernel,
        grid=(1,),
        in_specs=[*(_whole(a) for a in others), *rider.in_specs()],
        out_specs=[*rider.out_specs(), _whole(outs[-1])],
        out_shape=outs,
        scratch_shapes=[pltpu.VMEM((8, 128), F32), pltpu.VMEM((8, 8, 128), F32), pltpu.SemaphoreType.DMA((8,)), pltpu.SemaphoreType.DMA((8,)), *rider.scratch()],
        compiler_params=pltpu.CompilerParams(dimension_semantics=("arbitrary",), vmem_limit_bytes=VMEM, collective_id=number, has_side_effects=True),
        name="finish",
    )(*others, *given)
    return list(got[:-1]), got[-1]


def adamw(w, m, v, g):
    m = 0.9 * m + 0.1 * g
    v = 0.95 * v + 0.05 * g * g
    step = m * lax.rsqrt(v + 1e-8) + 0.1 * w
    return (w - 0.02 * step).astype(BF16), m, v


def update(weights, m, v, g, squares):
    parts = {"w_gate": ("first_gate", "last_gate"), "w_up": ("first_up", "last_up")}
    pieces = [p for n in NAMES for p in parts.get(n, (n,))]
    seven, layers, count = len(NAMES), weights[0].shape[0], 8 * sum(w.size for w in weights)

    def kernel(*refs):
        refs = list(refs)
        take = lambda n: [refs.pop(0) for _ in range(n)]
        square_ref, w_refs, m_refs, v_refs = refs.pop(0), take(seven), take(seven), take(seven)
        g_refs = [dict(zip(pieces, take(len(pieces)))) for _ in range(layers)]
        outs = take(seven), take(seven), take(seven)
        total = square_ref[...].sum(axis=0, keepdims=True).sum(axis=1, keepdims=True)
        factor = jnp.minimum(1.0, 0.5 * lax.rsqrt(total / count + 1e-30))

        def one(layer):
            for i, name in enumerate(NAMES):
                left = 0
                for piece in parts.get(name, (name,)):
                    g_ref = g_refs[layer][piece]
                    rows, columns = g_ref.shape

                    def some(t):
                        at = _some_rows(t)
                        for c in range(0, columns, 256):
                            wide = min(256, columns - c)
                            there = slice(left + c, left + c + wide)
                            got = adamw(w_refs[i][0, at, there].astype(F32), m_refs[i][0, at, there], v_refs[i][0, at, there],
                                        g_ref[at, c : c + wide].astype(F32) * factor)
                            for out, value in zip(outs, got):
                                out[i][0, at, there] = value

                    _loop(rows // 16, some)
                    left += columns

        for layer in range(layers):
            pl.when(pl.program_id(0) == layer)(functools.partial(one, layer))

    ins = [squares, *weights, *m, *v, *(of[p] for of in g for p in pieces)]
    layer = lambda a: pl.BlockSpec((1, *a.shape[1:]), lambda n: (n, 0, 0))
    outs = [*(_shape(a.shape) for a in weights), *(_shape(a.shape, F32) for a in (*m, *v))]
    return pl.pallas_call(
        kernel,
        grid=(layers,),
        in_specs=[layer(a) if a.ndim == 3 else _whole(a) for a in ins],
        out_specs=[layer(a) for a in outs],
        out_shape=outs,
        compiler_params=pltpu.CompilerParams(dimension_semantics=("arbitrary",), vmem_limit_bytes=VMEM),
        cost_estimate=pl.CostEstimate(flops=10**7, bytes_accessed=32 * 10**6, transcendentals=0),
        name="update",
    )(*ins)


def solution(mesh):
    def step(x, dy, *arrays):
        weights, m, v = (arrays[i : i + 7] for i in (0, 7, 14))
        shards = dict(zip(NAMES, weights, strict=True))
        blocks = {name: w.shape[1:] for name, w in shards.items()}
        given = lambda names: [shards[n] for n in names]
        h0, tokens = x[0], x.shape[1]

        w0, w1 = {}, {}
        tables, got = first(tokens, Gather(ATT, blocks, 0), given(ATT), 0)
        w0 |= zip(ATT, got)
        (mid0, *kept0), got = attend(h0, w0, tables, Gather(MLP, blocks, 0), given(MLP), 1)
        w0 |= zip(MLP, got)
        early = ATT + MLP[:2]
        (h1, *kept_gated), got = gated(mid0, *(w0[n] for n in MLP), Gather(early, blocks, 1), given(early), 2)
        w1 |= zip(early, got)
        (mid1, *kept1), got = attend(h1, w1, tables, Gather(MLP[2:], blocks, 1), given(MLP[2:]), 3)
        w1 |= zip(MLP[2:], got)

        by0, by1, g0, g1 = {}, {}, {}, {}
        early, last = ("first_gate", "first_up"), ("last_gate", "last_up")
        rest = ("w_down", *last)
        blocks |= {n: (blocks["w_up"][0], 2 * CHUNK) for n in last}
        (by_mid1, *got), _ = gated_bwd(mid1, dy[0], *(w1[n] for n in MLP), number=4)
        by1 |= zip(rest, got)
        g1 |= zip(early, got[len(rest) :])
        (*got, by_h1), sums = attend_bwd(h1, w1, tables, kept1, by_mid1, True, Scatter(last, blocks), [by1[n] for n in last], 5)
        by1 |= zip(ATT, got)
        g1 |= zip(last, sums)
        names = ("w_down", *ATT)
        (by_mid0, *got), sums = gated_bwd(mid0, by_h1, *(w0[n] for n in MLP), kept_gated, Scatter(names, blocks), [by1[n] for n in names], 6)
        by0 |= zip(rest, got)
        g0 |= zip(early, got[len(rest) :])
        g1 |= zip(names, sums)
        got, sums = attend_bwd(h0, w0, tables, kept0, by_mid0, False, Scatter(rest, blocks), [by0[n] for n in rest], 7)
        by0 |= zip(ATT, got)
        g0 |= zip(rest, sums)
        sums, squares = finish(Scatter(ATT, blocks), [by0[n] for n in ATT], [*g1.values(), *g0.values()], 8)
        g0 |= zip(ATT, sums)

        return tuple(update(weights, m, v, (g0, g1), squares))

    states, cut = P(("rep", "dp"), None, None), P(None, "dp", None)
    return jax.shard_map(
        step,
        mesh=mesh,
        in_specs=(states, states) + (cut,) * 21,
        out_specs=(P("rep", "dp", None),) * 21,
        check_vma=False,
    )
```

```python
import functools

import jax
import jax.numpy as jnp
import numpy as np
from jax import lax
from jax.experimental import pallas as pl
from jax.experimental.pallas import tpu as pltpu
from jax.sharding import PartitionSpec as P

HEAD = 256
THETA = 10000
NAMES = ("wq", "wk", "wv", "wo", "w_gate", "w_up", "w_down")
ATT, MLP = NAMES[:4], NAMES[4:]
NEG = -1e30
HIDDEN = 2 * NEG
LOG2E = 1.4426950408889634
VMEM = 62 * 2**20
BLOCK = 512
CHUNK = 512
ROWS = 512
ANY = pl.BlockSpec(memory_space=pl.ANY)
MESH = pl.DeviceIdType.MESH
F32, BF16 = jnp.float32, jnp.bfloat16


def _nn(a, b):
    return lax.dot_general(a, b, (((1,), (0,)), ((), ())), preferred_element_type=F32)


def _nt(a, b):
    return lax.dot_general(a, b, (((1,), (1,)), ((), ())), preferred_element_type=F32)


def _loop(n, do):
    def some(t, state):
        do(t)
        return state

    lax.fori_loop(0, n, some, 0)


def _slab(start, rows):
    return pl.ds(pl.multiple_of(start, 16), rows)


def _some_rows(t):
    return _slab(t * 16, 16)


def _units(names, blocks):
    cut = []
    for name in names:
        rows, columns = blocks[name]
        if name in ("wo", "w_down"):
            cut += [(name, 0, rows // 2, 0), (name, rows // 2, rows // 2, 1)]
        else:
            cut += [(name, 0, rows, 0 if name in ("wq", "w_gate", "last_gate") else 1)]
    return cut


def _around(way):
    me = lax.axis_index("dp")
    core, y, x = lax.rem(me, 2), lax.rem(lax.div(me, 2), 2), lax.div(me, 4)
    over_x, over_y = 4 - 8 * x, 2 - 4 * y
    first, second = (over_x, over_y) if way == 0 else (over_y, over_x)
    return me, 1 - 2 * core, first, second, over_x + over_y


def _meet():
    me, other, first, second, _ = _around(0)
    barrier = pltpu.get_barrier_semaphore()
    for way in (other, first, second):
        pl.semaphore_signal(barrier, inc=1, device_id={"dp": me + way}, device_id_type=MESH)
    pl.semaphore_wait(barrier, 3)


class Gather:
    def __init__(self, names, blocks, layer):
        self.names, self.blocks, self.layer = names, blocks, layer
        self.units = _units(names, blocks)

    def in_specs(self):
        return [ANY] * len(self.names)

    def out_specs(self):
        return [ANY] * len(self.names)

    def out_shape(self):
        return [jax.ShapeDtypeStruct((8 * self.blocks[n][0], self.blocks[n][1]), BF16) for n in self.names]

    def scratch(self):
        n = len(self.units)
        return [pltpu.SemaphoreType.DMA((n,)), pltpu.SemaphoreType.DMA((n, 7)), pltpu.SemaphoreType.DMA((n, 7))]

    def bind(self, ins, outs, scratch):
        self.shards, self.whole = dict(zip(self.names, ins)), dict(zip(self.names, outs))
        self.local, self.send, self.recv = scratch

    def _piece(self, unit, device):
        name, at, rows, _ = unit
        return self.whole[name].at[_slab(device * self.blocks[name][0] + at, rows)]

    def _copy(self, i, slot, arrived=False):
        unit = self.units[i]
        name, at, rows, way = unit
        me, other, first, second, across = _around(way)
        own = self.shards[name].at[self.layer, pl.ds(at, rows)]
        source, owner, to, comes = (
            (own, me, first, me + first),
            (own, me, second, me + second),
            (own, me, other, me + other),
            (None, me + first, second, me + across),
            (None, me + first, other, me + first + other),
            (None, me + second, other, me + second + other),
            (None, me + across, other, me + across + other),
        )[slot]
        if arrived:
            source, owner = None, comes
        target = self._piece(unit, owner)
        return pltpu.make_async_remote_copy(target if source is None else source, target, self.send.at[i, slot], self.recv.at[i, slot],
                                            device_id={"dp": me + to}, device_id_type=MESH)

    def _mine(self, i):
        name, at, rows, way = self.units[i]
        return pltpu.make_async_copy(self.shards[name].at[self.layer, pl.ds(at, rows)], self._piece(self.units[i], lax.axis_index("dp")), self.local.at[i])

    def begin(self):
        for i in range(len(self.units)):
            for slot in range(3):
                self._copy(i, slot).start()
            self._mine(i).start()

    def middle(self):
        for i in range(len(self.units)):
            self._copy(i, 0, True).wait_recv()
            self._copy(i, 3).start()
            self._copy(i, 4).start()
            self._copy(i, 1, True).wait_recv()
            self._copy(i, 5).start()

    def end(self):
        for i in range(len(self.units)):
            self._copy(i, 3, True).wait_recv()
            self._copy(i, 6).start()
        for i in range(len(self.units)):
            for slot in (2, 4, 5, 6):
                self._copy(i, slot, True).wait_recv()
            for slot in range(7):
                self._copy(i, slot).wait_send()
            self._mine(i).wait()

    def actions(self, steps):
        if steps == 1:
            return {0: ([_meet, self.begin], [self.middle, self.end])}
        return {0: ([_meet, self.begin], []), steps - 1: ([self.middle], [self.end])}


class Scatter:
    def __init__(self, names, blocks):
        self.names, self.blocks = names, blocks
        self.units = _units(names, blocks)

    def in_specs(self):
        return [ANY] * len(self.names)

    def out_specs(self):
        return [pl.BlockSpec(self.blocks[n], lambda *_: (0, 0), pipeline_mode=pl.Buffered(1)) for n in self.names]

    def out_shape(self):
        return [jax.ShapeDtypeStruct(self.blocks[n], BF16) for n in self.names]

    def scratch(self):
        n, dma = len(self.units), pltpu.SemaphoreType.DMA
        found = [dma((n, 4)), dma((n, 4)), dma((n, 4)), dma((n, 2)), dma((n, 2)), dma((n,)), dma((n,))]
        for name, _, rows, _ in self.units:
            columns = self.blocks[name][1]
            found += [pltpu.VMEM((k, rows, columns), BF16) for k in (4, 4, 2, 2, 1, 1)]
        return found

    def bind(self, ins, outs, scratch):
        self.terms, self.outs = dict(zip(self.names, ins)), dict(zip(self.names, outs))
        self.load, self.send0, self.recv0, self.send1, self.recv1, self.send2, self.recv2 = scratch[:7]
        rest = scratch[7:]
        self.buffers = [rest[6 * i : 6 * i + 6] for i in range(len(self.units))]

    def _block(self, unit, device):
        name, at, rows, _ = unit
        return self.terms[name].at[_slab(device * self.blocks[name][0] + at, rows)]

    def _own(self, i, j):
        me, other, *ways = _around(self.units[i][3])
        return pltpu.make_async_copy(self._block(self.units[i], me + ([0] + ways)[j]), self.buffers[i][0].at[j], self.load.at[i, j])

    def _across(self, i, j):
        me, other, *ways = _around(self.units[i][3])
        return pltpu.make_async_remote_copy(self._block(self.units[i], me + other + ([0] + ways)[j]), self.buffers[i][1].at[j], self.send0.at[i, j],
                                            self.recv0.at[i, j], device_id={"dp": me + other}, device_id_type=MESH)

    def _first(self, i, j):
        me, _, first, _, _ = _around(self.units[i][3])
        return pltpu.make_async_remote_copy(self.buffers[i][2].at[j], self.buffers[i][3].at[j], self.send1.at[i, j], self.recv1.at[i, j],
                                            device_id={"dp": me + first}, device_id_type=MESH)

    def _second(self, i):
        me, _, _, second, _ = _around(self.units[i][3])
        return pltpu.make_async_remote_copy(self.buffers[i][4].at[0], self.buffers[i][5].at[0], self.send2.at[i], self.recv2.at[i],
                                            device_id={"dp": me + second}, device_id_type=MESH)

    def begin(self):
        for js in ((1, 3), (2, 0)):
            for i in range(len(self.units)):
                for j in js:
                    self._across(i, j).start()
                    self._own(i, j).start()

    def _ready(self, i, j):
        self._own(i, j).wait()
        self._across(i, j).wait_recv()

    def _add(self, rows, store, *terms):
        def some(t):
            at = _some_rows(t)
            store(at, sum(term[at, :].astype(F32) for term in terms))

        _loop(rows // 16, some)

    def part1(self):
        for i, (_, _, rows, _) in enumerate(self.units):
            own, came, out = self.buffers[i][:3]
            for j, k in ((1, 0), (3, 1)):
                self._ready(i, j)

                def store(at, value, k=k, out=out):
                    out[k, at, :] = value.astype(BF16)

                self._add(rows, store, own.at[j], came.at[j])
            for i in ([i - 1] if i else []) + ([i] if i == len(self.units) - 1 else []):
                self._first(i, 0).start()
                self._first(i, 1).start()

    def part2(self):
        for i, (_, _, rows, _) in enumerate(self.units):
            own, came, _, got, out, _ = self.buffers[i]
            self._ready(i, 2)
            self._first(i, 0).wait_recv()
            self._first(i, 1).wait_recv()

            def store(at, value, out=out):
                out[0, at, :] = value.astype(BF16)

            self._add(rows, store, own.at[2], came.at[2], got.at[1])
            for i in ([i - 1] if i else []) + ([i] if i == len(self.units) - 1 else []):
                self._second(i).start()

    def end(self):
        for i, (name, start, rows, _) in enumerate(self.units):
            own, came, _, got, _, last = self.buffers[i]
            self._ready(i, 0)
            self._second(i).wait_recv()

            def store(at, value, name=name, start=start):
                self.outs[name][_slab(start + at.start, at.size), :] = value.astype(BF16)

            self._add(rows, store, own.at[0], came.at[0], got.at[0], last.at[0])
        for i in range(len(self.units)):
            for j in range(4):
                self._across(i, j).wait_send()
            for j in range(2):
                self._first(i, j).wait_send()
            self._second(i).wait_send()

    def actions(self, steps):
        if steps == 8:
            return {0: ([_meet, self.begin], []), 4: ([self.part1], []), 7: ([self.part2], [self.end])}
        return {0: ([_meet, self.begin], []), 1: ([self.part1], []), steps - 2: ([self.part2], []), steps - 1: ([], [self.end])}


class Chunks:
    def __init__(self, rows, chunks):
        self.rows, self.n = rows, chunks - 2

    def scratch(self):
        n, rows, dma = self.n, self.rows, pltpu.SemaphoreType.DMA
        sems = [dma((n, 2, 4)), dma((n, 2, 4)), dma((n, 2, 2)), dma((n, 2, 2)), dma((n, 2)), dma((n, 2))]
        block = lambda *lead: pltpu.VMEM((*lead, rows, CHUNK), BF16)
        return [*sems, pltpu.VMEM((n, 2, 8 * rows, CHUNK), BF16), block(n, 2, 4), block(n, 2, 2), block(n, 2, 2), block(n, 2), block(n, 2)]

    def bind(self, outs, scratch):
        self.outs = outs
        self.send0, self.recv0, self.send1, self.recv1, self.send2, self.recv2, self.terms, self.came, self.sum1, self.got1, self.sum2, self.got2 = scratch

    def _block(self, j, u, device):
        return self.terms.at[j, u, _slab(device * self.rows, self.rows)]

    def _own(self, j, u, k):
        me, _, *ways = _around(u)
        return self._block(j, u, me + ([0] + ways)[k])[...].astype(F32) + self.came[j, u, k].astype(F32)

    def _across(self, j, u, k):
        me, other, *ways = _around(u)
        return pltpu.make_async_remote_copy(self._block(j, u, me + other + ([0] + ways)[k]), self.came.at[j, u, k], self.send0.at[j, u, k],
                                            self.recv0.at[j, u, k], device_id={"dp": me + other}, device_id_type=MESH)

    def _first(self, j, u, k):
        me, _, first, _, _ = _around(u)
        return pltpu.make_async_remote_copy(self.sum1.at[j, u, k], self.got1.at[j, u, k], self.send1.at[j, u, k], self.recv1.at[j, u, k],
                                            device_id={"dp": me + first}, device_id_type=MESH)

    def _second(self, j, u):
        me, _, _, second, _ = _around(u)
        return pltpu.make_async_remote_copy(self.sum2.at[j, u], self.got2.at[j, u], self.send2.at[j, u], self.recv2.at[j, u],
                                            device_id={"dp": me + second}, device_id_type=MESH)

    def part0(self, j):
        for u in range(2):
            for k in (1, 3, 2, 0):
                self._across(j, u, k).start()

    def part1(self, j):
        for u in range(2):
            for k, at in ((1, 0), (3, 1)):
                self._across(j, u, k).wait_recv()
                self.sum1[j, u, at] = self._own(j, u, k).astype(BF16)

    def part2(self, j):
        for u in range(2):
            for k in range(2):
                self._first(j, u, k).start()

    def part3(self, j):
        for u in range(2):
            self._across(j, u, 2).wait_recv()
            for k in range(2):
                self._first(j, u, k).wait_recv()
            self.sum2[j, u] = (self._own(j, u, 2) + self.got1[j, u, 1].astype(F32)).astype(BF16)

    def part4(self, j):
        for u in range(2):
            self._second(j, u).start()

    def end(self, j):
        for u in range(2):
            self._across(j, u, 0).wait_recv()
            self._second(j, u).wait_recv()
            total = self._own(j, u, 0) + self.got1[j, u, 0].astype(F32) + self.got2[j, u].astype(F32)
            self.outs[u][:, pl.ds(pl.multiple_of(j * CHUNK, CHUNK), CHUNK)] = total.astype(BF16)
        for u in range(2):
            for k in range(4):
                self._across(j, u, k).wait_send()
            for k in range(2):
                self._first(j, u, k).wait_send()
            self._second(j, u).wait_send()


def _call(body, steps, ins, in_specs, outs, out_specs, scratch, rider=None, given=(), number=0, flops=0, name=None, meet=False):
    ni, no, ns = len(in_specs), len(out_specs), len(scratch)
    more_in, more_out, more_specs, more_scratch = ([], [], [], []) if rider is None else (rider.in_specs(), rider.out_shape(), rider.out_specs(), rider.scratch())

    def kernel(*refs):
        cuts = [ni, len(more_in), no, len(more_out), ns, len(more_scratch)]
        parts, at = [], 0
        for n in cuts:
            parts.append(refs[at : at + n])
            at += n
        my_in, its_in, my_out, its_out, mine, its = parts
        step = pl.program_id(0)
        acts = {}
        if rider is not None:
            rider.bind(its_in, its_out, its)
            acts = rider.actions(steps)
        elif meet:
            acts = {0: ([_meet], [])}

        def run(which):
            for s, lists in acts.items():
                if lists[which]:
                    if steps == 1:
                        for act in lists[which]:
                            act()
                    else:

                        @pl.when(step == s)
                        def _(todo=lists[which]):
                            for act in todo:
                                act()

        run(0)
        body(step, my_in, my_out, mine)
        run(1)

    params = dict(dimension_semantics=("arbitrary",), vmem_limit_bytes=VMEM)
    if rider is not None or meet:
        params |= dict(collective_id=number, has_side_effects=True)
    got = pl.pallas_call(
        kernel,
        grid=(steps,),
        in_specs=[*in_specs, *more_in],
        out_specs=[*out_specs, *more_specs],
        out_shape=[*outs, *more_out],
        scratch_shapes=[*scratch, *more_scratch],
        compiler_params=pltpu.CompilerParams(**params),
        cost_estimate=pl.CostEstimate(flops=int(flops) + 1, bytes_accessed=10**6, transcendentals=0),
        name=name,
    )(*ins, *given)
    return list(got[:no]), list(got[no:])


def _whole(a):
    return pl.BlockSpec(a.shape, lambda *_: (0,) * len(a.shape), pipeline_mode=pl.Buffered(1))


def _shape(shape, dtype=BF16):
    return jax.ShapeDtypeStruct(shape, dtype)


def first(tokens, rider, given, number):
    half = HEAD // 2
    speed = jnp.asarray(THETA ** (-np.arange(half) / half), F32)[None]

    def body(step, ins, outs, scratch):
        (speed_ref,) = ins

        def some(t):
            at = pl.ds(pl.multiple_of(t * 256, 256), 256)
            angle = (lax.broadcasted_iota(jnp.int32, (256, half), 0) + t * 256).astype(F32) * speed_ref[...]
            cos_ref, sin_ref = outs
            cos_ref[at, :], sin_ref[at, :] = jnp.cos(angle), jnp.sin(angle)

        _loop(tokens // 256, some)

    outs = [_shape((tokens, half), F32)] * 2
    return _call(body, 1, [speed], [_whole(speed)], outs, [_whole(a) for a in outs], [], rider, given, number, name="first")


def _hidden():
    return lax.broadcasted_iota(jnp.int32, (BLOCK, BLOCK), 0) > lax.broadcasted_iota(jnp.int32, (BLOCK, BLOCK), 1)


def _strip(ref, head, a):
    return ref[a * BLOCK : (a + 1) * BLOCK, head * HEAD : (head + 1) * HEAD]


def _turn(t, cos, sin):
    half, parts = HEAD // 2, []
    for at in range(0, t.shape[1], HEAD):
        a, b = t[:, at : at + half].astype(F32), t[:, at + half : at + HEAD].astype(F32)
        parts += [a * cos - b * sin, b * cos + a * sin]
    return jnp.concatenate(parts, -1).astype(BF16)


def attend(h, w, tables, rider, given, number):
    wq, wk, wv, wo = (w[n] for n in ATT)
    tokens, heads = h.shape[0], wq.shape[1] // HEAD
    blocks, scale = tokens // BLOCK, HEAD**-0.5
    e = scale * LOG2E

    def body(step, ins, outs, scratch):
        h_ref, wq_ref, wk_ref, wv_ref, wo_ref, cos_ref, sin_ref = ins
        mid_ref, q_ref, k_ref, v_ref, o_ref, lse_ref = outs
        top_s, mix_s = scratch

        @pl.when(step < blocks)
        def _():
            at = pl.ds(pl.multiple_of(step * BLOCK, BLOCK), BLOCK)
            wide = h_ref[at, :].astype(F32)
            a = (wide * _scale(wide)).astype(BF16)
            cos, sin = cos_ref[at, :], sin_ref[at, :]
            q_ref[at, :] = _turn(_nn(a, wq_ref[...]).astype(BF16), cos, sin)
            k_ref[at, :] = _turn(_nn(a, wk_ref[...]).astype(BF16), cos, sin)
            v_ref[at, :] = _nn(a, wv_ref[...]).astype(BF16)

        def block(j):
            strips = [(n, a) for a in range(j, blocks) for n in range(heads)]
            here = slice(j * BLOCK, (j + 1) * BLOCK)
            keys = k_ref[here, :]
            values = jnp.concatenate([v_ref[here, :].T, jnp.ones((8, BLOCK), BF16)], axis=0)
            scores = [_nt(keys, _strip(q_ref, n, a)) for n, a in strips]
            weights, keeps = [], []
            for (n, a), s in zip(strips, scores):
                i = a * heads + n
                if a == j:
                    s = jnp.where(_hidden(), HIDDEN, s)
                top = s.max(axis=0, keepdims=True)
                if j:
                    old = top_s[i : i + 1, :]
                    top = jnp.maximum(old, top)
                    keeps.append(jnp.exp2((old - top) * e))
                else:
                    keeps.append(None)
                top_s[i : i + 1, :] = top
                weights.append(jnp.exp2((s - top) * e).astype(BF16))
            done = []
            for (n, a), p, keep in zip(strips, weights, keeps):
                i = a * heads + n
                mix = _nn(values, p)
                if j:
                    mix = mix_s[i] * keep + mix
                if a > j:
                    mix_s[i] = mix
                else:
                    total = mix[HEAD : HEAD + 1, :]
                    done.append((mix[:HEAD, :] * (1 / total)).T.astype(BF16))
                    o_ref[here, n * HEAD : (n + 1) * HEAD] = done[-1]
                    lse_ref[i : i + 1, :] = top_s[i : i + 1, :] * scale + jnp.log(total)
            out = _nn(jnp.concatenate(done, -1), wo_ref[...]).astype(BF16).astype(F32)
            mid_ref[here, :] = (h_ref[here, :].astype(F32) + out).astype(BF16)

        for j in range(blocks):
            pl.when(step == blocks + j)(functools.partial(block, j))

    n = heads * blocks
    ins = [h, wq, wk, wv, wo, *tables]
    outs = [_shape(h.shape), _shape((tokens, heads * HEAD)), _shape((tokens, HEAD)), _shape((tokens, HEAD)), _shape((tokens, heads * HEAD)), _shape((n, BLOCK), F32)]
    flops = 2 * tokens * (h.shape[1] * 1536 + 1.2 * tokens * heads * HEAD)
    return _call(body, 2 * blocks, ins, [_whole(a) for a in ins], outs, [_whole(a) for a in outs],
                 [pltpu.VMEM((n, BLOCK), F32), pltpu.VMEM((n, HEAD + 8, BLOCK), F32)], rider, given, number, flops, "attend")


def attend_bwd(h, w, tables, kept, by_mid, wanted, rider, given, number):
    q, k, v, o, lse = kept
    wq, wk, wv, wo = (w[n] for n in ATT)
    (tokens, d), heads = h.shape, wq.shape[1] // HEAD
    blocks, scale = tokens // BLOCK, HEAD**-0.5
    e = scale * LOG2E

    def body(step, ins, outs, scratch):
        h_ref, wq_ref, wk_ref, wv_ref, wo_ref, cos_ref, sin_ref, q_ref, k_ref, v_ref, o_ref, lse_ref, by_ref = ins
        dwq_ref, dwk_ref, dwv_ref, dwo_ref, *dh_ref = outs
        dq_s, do_s, delta_s, dwq_s, dwk_s, dwv_s, dwo_s = scratch

        def before(t):
            here = slice(t * BLOCK, (t + 1) * BLOCK)
            by, o = by_ref[here, :], o_ref[here, :]
            do = _nt(by, wo_ref[...]).astype(BF16)
            do_s[here, :] = do
            dots = (do.astype(F32) * o.astype(F32)).T
            for n in range(heads):
                i = t * heads + n
                delta_s[i : i + 1, :] = dots[n * HEAD : (n + 1) * HEAD, :].sum(axis=0, keepdims=True)
            term = _nn(o.T, by)
            if t:
                term = dwo_s[...] + term
            if t < blocks - 1:
                dwo_s[...] = term
            else:
                dwo_ref[...] = term.astype(BF16)

        def block(j):
            here = slice(j * BLOCK, (j + 1) * BLOCK)
            strips = [(n, a) for a in range(j, blocks) for n in range(heads)]
            keys, values = k_ref[here, :], v_ref[here, :]
            turned_keys = keys.T
            dk = dv = None
            dq = []
            scores = [_nt(keys, _strip(q_ref, n, a)) for n, a in strips]
            dps = [_nt(values, _strip(do_s, n, a)) for n, a in strips]
            for (n, a), s, dp in zip(strips, scores, dps):
                i = a * heads + n
                p = jnp.exp2(s * e - lse_ref[i : i + 1, :] * LOG2E)
                if a == j:
                    p = jnp.where(_hidden(), 0.0, p)
                ds = (p * (dp - delta_s[i : i + 1, :])).astype(BF16)
                by_v = _nn(p.astype(BF16), _strip(do_s, n, a))
                by_k = _nn(ds, _strip(q_ref, n, a))
                dv, dk = (by_v, by_k) if dv is None else (dv + by_v, dk + by_k)
                by_q = _nn(turned_keys, ds)
                if j:
                    by_q = dq_s[i] + by_q
                if a > j:
                    dq_s[i] = by_q
                else:
                    dq.append((by_q * scale).T.astype(BF16))
            cos, sin = cos_ref[here, :], -sin_ref[here, :]
            dq = _turn(jnp.concatenate(dq, -1), cos, sin)
            dk = _turn((dk * scale).astype(BF16), cos, sin)
            dv = dv.astype(BF16)
            wide = h_ref[here, :].astype(F32)
            size = _scale(wide)
            at = (wide * size).astype(BF16).T
            for by, sum_s, out_ref in ((dq, dwq_s, dwq_ref), (dk, dwk_s, dwk_ref), (dv, dwv_s, dwv_ref)):
                term = _nn(at, by)
                if j:
                    term = sum_s[...] + term
                if j < blocks - 1:
                    sum_s[...] = term
                else:
                    out_ref[...] = term.astype(BF16)
            if wanted:
                by_a = (_nt(dv, wv_ref[...]).astype(BF16).astype(F32) + _nt(dk, wk_ref[...]).astype(BF16).astype(F32)
                        + _nt(dq, wq_ref[...]).astype(BF16).astype(F32)).astype(BF16).astype(F32)
                by_h = by_a * size - wide * (size * size * size) * jnp.mean(by_a * wide, -1, keepdims=True)
                dh_ref[0][here, :] = (by_h.astype(BF16).astype(F32) + by_ref[here, :].astype(F32)).astype(BF16)

        for t in range(blocks):
            pl.when(step == t)(functools.partial(before, t))
            pl.when(step == blocks + t)(functools.partial(block, t))

    ins = [h, wq, wk, wv, wo, *tables, q, k, v, o, lse, by_mid]
    outs = [_shape(a.shape) for a in (wq, wk, wv, wo) + ((h,) if wanted else ())]
    n = heads * blocks
    full = lambda a: pltpu.VMEM(a.shape, F32)
    flops = 4 * tokens * (d * 1536 + 1.5 * tokens * heads * HEAD)
    return _call(body, 2 * blocks, ins, [_whole(a) for a in ins], outs, [_whole(a) for a in outs],
                 [pltpu.VMEM((n, HEAD, BLOCK), F32), pltpu.VMEM(o.shape, BF16), pltpu.VMEM((n, BLOCK), F32), full(wq), full(wk), full(wv), full(wo)],
                 rider, given, number, flops, "attend_bwd")


def _scale(wide):
    return lax.rsqrt(jnp.mean(wide * wide, -1, keepdims=True) + 1e-6)


def _sigmoid(x):
    return 0.5 * jnp.tanh(0.5 * x) + 0.5


def _tokens(n, do):
    _loop(n // ROWS, lambda t: do(pl.ds(pl.multiple_of(t * ROWS, ROWS), ROWS)))


def _chunks(w_gate, w_down):
    across = pl.BlockSpec((w_gate.shape[0], CHUNK), lambda j: (0, j))
    down = pl.BlockSpec((CHUNK, w_down.shape[1]), lambda j: (j, 0))
    return across, down


def gated(h, w_gate, w_up, w_down, rider, given, number):
    tokens, d = h.shape
    steps = w_gate.shape[1] // CHUNK
    across, down = _chunks(w_gate, w_down)

    def body(step, ins, outs, scratch):
        h_ref, g_ref, u_ref, d_ref = ins
        o_ref, gate_ref, up_ref = outs
        b_s, sum_s = scratch

        @pl.when(step == 0)
        def _():
            def norm(at):
                wide = h_ref[at, :].astype(F32)
                b_s[at, :] = (wide * _scale(wide)).astype(BF16)
                sum_s[at, :] = jnp.zeros((ROWS, d), F32)

            _tokens(tokens, norm)

        def some(at):
            b = b_s[at, :]
            gate, up = _nn(b, g_ref[...]), _nn(b, u_ref[...])
            gate_ref[0, at, :], up_ref[0, at, :] = gate, up
            act = (gate * _sigmoid(gate) * up).astype(BF16)
            sum_s[at, :] += _nn(act, d_ref[...])

        _tokens(tokens, some)

        @pl.when(step == steps - 1)
        def _():
            def last(at):
                o_ref[at, :] = (h_ref[at, :].astype(F32) + sum_s[at, :].astype(BF16).astype(F32)).astype(BF16)

            _tokens(tokens, last)

    keep = pl.BlockSpec((1, tokens, CHUNK), lambda j: (j, 0, 0))
    kept = _shape((steps, tokens, CHUNK), F32)
    return _call(body, steps, [h, w_gate, w_up, w_down], [_whole(h), across, across, down], [_shape(h.shape), kept, kept], [_whole(h), keep, keep],
                 [pltpu.VMEM((tokens, d), BF16), pltpu.VMEM((tokens, d), F32)], rider, given, number, 6 * tokens * d * w_gate.shape[1], "gated")


def gated_bwd(h, by_out, w_gate, w_up, w_down, kept=(), rider=None, given=(), number=0):
    tokens, d = h.shape
    steps = w_gate.shape[1] // CHUNK
    across, down = _chunks(w_gate, w_down)
    sums, inner = Chunks(d // 8, steps), tokens // ROWS

    def body(step, ins, outs, scratch):
        h_ref, by_ref, g_ref, u_ref, d_ref, *kept_refs = ins
        dh_ref, dd_ref, lg_ref, lu_ref, *sum_refs = outs
        bt_s, byt_s, sum_s, act_s, gate_s, up_s = scratch[:6]
        sums.bind(sum_refs, scratch[8:])
        if kept:
            tile_s, sem = scratch[6:8]
        else:
            b_s = scratch[6]

        def tiles(i):
            at = pl.ds(pl.multiple_of(lax.rem(i, inner) * ROWS, ROWS), ROWS)
            slot = lax.rem(i, 2)
            return [pltpu.make_async_copy(ref.at[lax.div(i, inner), at], tile_s.at[slot, k], sem.at[slot, k]) for k, ref in enumerate(kept_refs)]

        if kept:

            @pl.when(step == 0)
            def _():
                for copy in tiles(0):
                    copy.start()

        new, old = (step >= 1) & (step <= sums.n), step >= 2
        pl.when(new)(lambda: sums.part0(step - 1))

        @pl.when(step == 0)
        def _():
            def norm(at):
                wide = h_ref[at, :].astype(F32)
                b = (wide * _scale(wide)).astype(BF16)
                if not kept:
                    b_s[at, :] = b
                bt_s[:, at] = b.T
                byt_s[:, at] = by_ref[at, :].T
                sum_s[at, :] = jnp.zeros((ROWS, d), F32)

            _tokens(tokens, norm)

        def some(t):
            @pl.when(t == inner - 2)
            def _():
                pl.when(old)(lambda: sums.part3(step - 2))
                pl.when(new)(lambda: sums.part1(step - 1))

            @pl.when(t == inner - 1)
            def _():
                pl.when(old)(lambda: sums.part4(step - 2))
                pl.when(new)(lambda: sums.part2(step - 1))

            at = pl.ds(pl.multiple_of(t * ROWS, ROWS), ROWS)
            by = by_ref[at, :]
            if kept:
                i = step * inner + t

                @pl.when(i + 1 < steps * inner)
                def _():
                    for copy in tiles(i + 1):
                        copy.start()

                for copy in tiles(i):
                    copy.wait()
                gate, up = tile_s[lax.rem(i, 2), 0], tile_s[lax.rem(i, 2), 1]
            else:
                b = b_s[at, :]
                gate, up = _nn(b, g_ref[...]), _nn(b, u_ref[...])
            by_act = _nt(by, d_ref[...]).astype(BF16).astype(F32)
            open_ = _sigmoid(gate)
            silu = gate * open_
            act_s[at, :] = (silu * up).astype(BF16)
            by_up = (by_act * silu).astype(BF16)
            by_gate = (by_act * up * (open_ + silu * (1 - open_))).astype(BF16)
            gate_s[at, :] = by_gate
            up_s[at, :] = by_up
            sum_s[at, :] += _nt(by_gate, g_ref[...]) + _nt(by_up, u_ref[...])

        _loop(inner, some)
        for u, by_s, last_ref in ((0, gate_s, lg_ref), (1, up_s, lu_ref)):
            term = _nn(bt_s[...], by_s[...]).astype(BF16)

            @pl.when(step < sums.n)
            def _(u=u, term=term):
                sums.terms[step, u] = term

            @pl.when(step >= sums.n)
            def _(last_ref=last_ref, term=term):
                last_ref[:, pl.ds(pl.multiple_of((step - sums.n) * CHUNK, CHUNK), CHUNK)] = term

        dd_ref[...] = _nn(byt_s[...], act_s[...]).astype(BF16).T
        pl.when(old)(lambda: sums.end(step - 2))

        @pl.when(step == steps - 1)
        def _():
            def last(at):
                wide = h_ref[at, :].astype(F32)
                scale = _scale(wide)
                by_b = sum_s[at, :].astype(BF16).astype(F32)
                by = by_b * scale - wide * (scale * scale * scale) * jnp.mean(by_b * wide, -1, keepdims=True)
                dh_ref[at, :] = (by.astype(BF16).astype(F32) + by_ref[at, :].astype(F32)).astype(BF16)

            _tokens(tokens, last)

    half, full = pltpu.VMEM((tokens, d), BF16), pltpu.VMEM((tokens, d), F32)
    chunk, turned_ = pltpu.VMEM((tokens, CHUNK), BF16), pltpu.VMEM((d, tokens), BF16)
    outs = [_shape(h.shape), _shape(w_down.shape), *[_shape((d, (steps - sums.n) * CHUNK))] * 2, *[_shape((d // 8, sums.n * CHUNK))] * 2]
    more = [pltpu.VMEM((2, 2, ROWS, CHUNK), F32), pltpu.SemaphoreType.DMA((2, 2))] if kept else [half, pltpu.SemaphoreType.DMA((1,))]
    return _call(body, steps, [h, by_out, w_gate, w_up, w_down, *kept], [_whole(h), _whole(h), across, across, down, *[ANY] * len(kept)],
                 outs, [_whole(h), down, *(_whole(a) for a in outs[2:])], [turned_, turned_, full, chunk, chunk, chunk, *more, *sums.scratch()],
                 rider, given, number, (12 if kept else 16) * tokens * d * w_gate.shape[1], "gated_bwd", True)


def finish(rider, given, others, number):
    n, ng, distances = len(others), len(given), range(1, 8)

    def squares(ref):
        rows, columns = ref.shape

        def some(t, total):
            g = ref[_some_rows(t), :].astype(F32)
            g = g * g
            g = g[:8, :] + g[8:, :]
            return total + sum(g[:, c : c + 128] for c in range(0, columns, 128))

        return lax.fori_loop(0, rows // 16, some, jnp.zeros((8, 128), F32))

    def kernel(*refs):
        other_refs, given_refs, refs = refs[:n], refs[n : n + ng], refs[n + ng :]
        out_refs, total_ref, refs = refs[:ng], refs[ng], refs[ng + 1 :]
        mine_s, all_s, send, recv = refs[:4]
        rider.bind(given_refs, out_refs, refs[4:])
        me = lax.axis_index("dp")
        barrier = pltpu.get_barrier_semaphore()
        for k in distances:
            pl.semaphore_signal(barrier, inc=1, device_id={"dp": lax.rem(me + k, 8)}, device_id_type=MESH)
        pl.semaphore_wait(barrier, 7)
        rider.begin()
        total = sum(squares(ref) for ref in other_refs)
        for act in (rider.part1, rider.part2, rider.end):
            act()
        mine_s[...] = total + sum(squares(ref) for ref in out_refs)

        def copy(k):
            return pltpu.make_async_remote_copy(mine_s, all_s.at[me], send.at[k], recv.at[k], device_id={"dp": lax.rem(me + k, 8)}, device_id_type=MESH)

        def arrived(k):
            place = all_s.at[lax.rem(me + 8 - k, 8)]
            return pltpu.make_async_remote_copy(place, place, send.at[k], recv.at[k], device_id={"dp": me}, device_id_type=MESH)

        for k in distances:
            copy(k).start()
        all_s[me] = mine_s[...]
        for k in distances:
            arrived(k).wait_recv()
        for k in distances:
            copy(k).wait_send()
        total_ref[...] = sum(all_s[k] for k in range(8))

    outs = [*rider.out_shape(), _shape((8, 128), F32)]
    got = pl.pallas_call(
        kernel,
        grid=(1,),
        in_specs=[*(_whole(a) for a in others), *rider.in_specs()],
        out_specs=[*rider.out_specs(), _whole(outs[-1])],
        out_shape=outs,
        scratch_shapes=[pltpu.VMEM((8, 128), F32), pltpu.VMEM((8, 8, 128), F32), pltpu.SemaphoreType.DMA((8,)), pltpu.SemaphoreType.DMA((8,)), *rider.scratch()],
        compiler_params=pltpu.CompilerParams(dimension_semantics=("arbitrary",), vmem_limit_bytes=VMEM, collective_id=number, has_side_effects=True),
        name="finish",
    )(*others, *given)
    return list(got[:-1]), got[-1]


def adamw(w, m, v, g):
    m = 0.9 * m + 0.1 * g
    v = 0.95 * v + 0.05 * g * g
    step = m * lax.rsqrt(v + 1e-8) + 0.1 * w
    return (w - 0.02 * step).astype(BF16), m, v


def update(weights, m, v, g, squares):
    parts = {"w_gate": ("first_gate", "last_gate"), "w_up": ("first_up", "last_up")}
    pieces = [p for n in NAMES for p in parts.get(n, (n,))]
    seven, layers, count = len(NAMES), weights[0].shape[0], 8 * sum(w.size for w in weights)

    def kernel(*refs):
        refs = list(refs)
        take = lambda n: [refs.pop(0) for _ in range(n)]
        square_ref, w_refs, m_refs, v_refs = refs.pop(0), take(seven), take(seven), take(seven)
        g_refs = [dict(zip(pieces, take(len(pieces)))) for _ in range(layers)]
        outs = take(seven), take(seven), take(seven)
        total = square_ref[...].sum(axis=0, keepdims=True).sum(axis=1, keepdims=True)
        factor = jnp.minimum(1.0, 0.5 * lax.rsqrt(total / count + 1e-30))

        def one(layer):
            for i, name in enumerate(NAMES):
                left = 0
                for piece in parts.get(name, (name,)):
                    g_ref = g_refs[layer][piece]
                    rows, columns = g_ref.shape

                    def some(t):
                        at = _some_rows(t)
                        for c in range(0, columns, 256):
                            wide = min(256, columns - c)
                            there = slice(left + c, left + c + wide)
                            got = adamw(w_refs[i][0, at, there].astype(F32), m_refs[i][0, at, there], v_refs[i][0, at, there],
                                        g_ref[at, c : c + wide].astype(F32) * factor)
                            for out, value in zip(outs, got):
                                out[i][0, at, there] = value

                    _loop(rows // 16, some)
                    left += columns

        for layer in range(layers):
            pl.when(pl.program_id(0) == layer)(functools.partial(one, layer))

    ins = [squares, *weights, *m, *v, *(of[p] for of in g for p in pieces)]
    layer = lambda a: pl.BlockSpec((1, *a.shape[1:]), lambda n: (n, 0, 0))
    outs = [*(_shape(a.shape) for a in weights), *(_shape(a.shape, F32) for a in (*m, *v))]
    return pl.pallas_call(
        kernel,
        grid=(layers,),
        in_specs=[layer(a) if a.ndim == 3 else _whole(a) for a in ins],
        out_specs=[layer(a) for a in outs],
        out_shape=outs,
        compiler_params=pltpu.CompilerParams(dimension_semantics=("arbitrary",), vmem_limit_bytes=VMEM),
        cost_estimate=pl.CostEstimate(flops=10**7, bytes_accessed=32 * 10**6, transcendentals=0),
        name="update",
    )(*ins)


def solution(mesh):
    def step(x, dy, *arrays):
        weights, m, v = (arrays[i : i + 7] for i in (0, 7, 14))
        shards = dict(zip(NAMES, weights, strict=True))
        blocks = {name: w.shape[1:] for name, w in shards.items()}
        given = lambda names: [shards[n] for n in names]
        h0, tokens = x[0], x.shape[1]

        w0, w1 = {}, {}
        tables, got = first(tokens, Gather(ATT, blocks, 0), given(ATT), 0)
        w0 |= zip(ATT, got)
        (mid0, *kept0), got = attend(h0, w0, tables, Gather(MLP, blocks, 0), given(MLP), 1)
        w0 |= zip(MLP, got)
        early = ATT + MLP[:2]
        (h1, *kept_gated), got = gated(mid0, *(w0[n] for n in MLP), Gather(early, blocks, 1), given(early), 2)
        w1 |= zip(early, got)
        (mid1, *kept1), got = attend(h1, w1, tables, Gather(MLP[2:], blocks, 1), given(MLP[2:]), 3)
        w1 |= zip(MLP[2:], got)

        by0, by1, g0, g1 = {}, {}, {}, {}
        early, last = ("first_gate", "first_up"), ("last_gate", "last_up")
        rest = ("w_down", *last)
        blocks |= {n: (blocks["w_up"][0], 2 * CHUNK) for n in last}
        (by_mid1, *got), _ = gated_bwd(mid1, dy[0], *(w1[n] for n in MLP), number=4)
        by1 |= zip(rest, got)
        g1 |= zip(early, got[len(rest) :])
        (*got, by_h1), sums = attend_bwd(h1, w1, tables, kept1, by_mid1, True, Scatter(last, blocks), [by1[n] for n in last], 5)
        by1 |= zip(ATT, got)
        g1 |= zip(last, sums)
        names = ("w_down", *ATT)
        (by_mid0, *got), sums = gated_bwd(mid0, by_h1, *(w0[n] for n in MLP), kept_gated, Scatter(names, blocks), [by1[n] for n in names], 6)
        by0 |= zip(rest, got)
        g0 |= zip(early, got[len(rest) :])
        g1 |= zip(names, sums)
        got, sums = attend_bwd(h0, w0, tables, kept0, by_mid0, False, Scatter(rest, blocks), [by0[n] for n in rest], 7)
        by0 |= zip(ATT, got)
        g0 |= zip(rest, sums)
        sums, squares = finish(Scatter(ATT, blocks), [by0[n] for n in ATT], [*g1.values(), *g0.values()], 8)
        g0 |= zip(ATT, sums)

        return tuple(update(weights, m, v, (g0, g1), squares))

    states, cut = P(("rep", "dp"), None, None), P(None, "dp", None)
    return jax.shard_map(
        step,
        mesh=mesh,
        in_specs=(states, states) + (cut,) * 21,
        out_specs=(P("rep", "dp", None),) * 21,
        check_vma=False,
    )
```
